32 devices in a mesh: shard: 4 (over y, x), ctx: 2 (over core), tp: 4 (over z).
Axes of the slice: x: 2, y: 2, z: 4, core: 2. Of those that a mesh axis runs over, the one named last changes fastest.
Arguments:
- tokens: bfloat16 [4, 2048, 2048], P('shard', 'ctx'), may hold values from -6 to 6
- lengths: int32 [4], P('shard'), may hold values from 512 to 2048, as said below
- cotangent: bfloat16 [4, 2048, 2048], P('shard', 'ctx'), may hold values from -6 to 6
- w_query: float32 [2048, 2048], P(('shard', 'ctx'), 'tp'), may hold values from -0.1875 to 0.1875
- w_key: float32 [2048, 2048], P(('shard', 'ctx'), 'tp'), may hold values from -0.1875 to 0.1875
- w_value: float32 [2048, 2048], P(('shard', 'ctx'), 'tp'), may hold values from -0.125 to 0.125
- w_output: float32 [2048, 2048], P('tp', ('shard', 'ctx')), may hold values from -1 to 1
- w_gate: float32 [2048, 8192], P(('shard', 'ctx'), 'tp'), may hold values from -0.125 to 0.125
- w_up: float32 [2048, 8192], P(('shard', 'ctx'), 'tp'), may hold values from -0.125 to 0.125
- w_down: float32 [8192, 2048], P('tp', ('shard', 'ctx')), may hold values from -0.0625 to 0.0625
Outputs:
- output: bfloat16 [4, 2048, 2048], P('shard', 'ctx')
- grad_tokens: float32 [4, 2048, 2048], P('shard', 'ctx')
- grad_query: float32 [2048, 2048], P(('shard', 'ctx'), 'tp')
- grad_key: float32 [2048, 2048], P(('shard', 'ctx'), 'tp')
- grad_value: float32 [2048, 2048], P(('shard', 'ctx'), 'tp')
- grad_output: float32 [2048, 2048], P('tp', ('shard', 'ctx'))
- grad_gate: float32 [2048, 8192], P(('shard', 'ctx'), 'tp')
- grad_up: float32 [2048, 8192], P(('shard', 'ctx'), 'tp')
- grad_down: float32 [8192, 2048], P('tp', ('shard', 'ctx'))
The draws below stay inside these ranges and needn't reach their ends.
Inputs may be any that keep to these rules, and one draw needn't show every extreme that they name: Slots 0 to lengths[b] - 1 of sequence b are valid, the rest padding; some sequence is full and some has 512 valid slots.
All inputs are finite; a program needn't handle non-finite values.
Results may differ from the reference program's by a relative error of at most 0.014.
The reference program's roundings to bfloat16 on the way count: a program that leaves them out, or rounds other values in their place, can miss the bound.
Values may be sent and summed in bfloat16 or wider, within the bound.
A program may use at most 256 MiB of HBM per device.

```python
import jax
import jax.numpy as jnp
from jax import lax

D = 2048
HEADS = 16
HEAD_DIM = 128
FF = 8192
SEQ_LEN = 2048
BATCH = 4


def draw_lengths(key, part):
    least = SEQ_LEN // 4
    key_base = jax.random.fold_in(key, 11)
    key_long = jax.random.fold_in(key, 23)
    key_offset = jax.random.fold_in(key, 37)
    drawn = jax.random.randint(key_base, (BATCH,), least, SEQ_LEN + 1)
    longest = jax.random.randint(key_long, (), 0, BATCH)
    offset_draw = jax.random.randint(key_offset, (), 1, BATCH)
    shortest = (longest + offset_draw) % BATCH
    positions = jnp.arange(BATCH)
    drawn = jnp.where(positions == longest, SEQ_LEN, drawn)
    drawn = jnp.where(positions == shortest, least, drawn)
    return drawn.astype(jnp.int32)


def steps_of(stream_key, dims, pieces, smallest, high):
    loudness = 1.0
    for dim, parts in pieces:
        draws = jax.random.uniform(jax.random.fold_in(jax.random.fold_in(stream_key, 6), dim), (parts,), jnp.float32, smallest / len(pieces), high / len(pieces))
        loudness = loudness * jnp.repeat(jnp.exp(draws), dims[dim] // parts).reshape((-1,) + (1,) * (len(dims) - 1 - dim))
    return loudness


def bell_draw(key, shape, scale, bound, pieces=(), dtype=jnp.bfloat16):
    loudness = steps_of(key, shape, pieces, -0.22, 0.18) if pieces else 1.0
    array = jax.random.normal(key, shape, jnp.float32) * scale * loudness
    return jnp.minimum(jnp.maximum(array, -bound), bound).astype(dtype)


def setup_inputs(seed: int = 0) -> dict:
    splits = jax.random.split(jax.random.key(seed), 11)
    tokens = bell_draw(splits[0], (BATCH, SEQ_LEN, D), 1.0, 6.0, ((0, 4), (1, 2)))
    lengths = draw_lengths(jax.random.fold_in(splits[10], 71), 0)
    cotangent = bell_draw(splits[2], (BATCH, SEQ_LEN, D), 1.0, 6.0, ((0, 4), (1, 2)))
    w_query = bell_draw(splits[3], (D, HEADS * HEAD_DIM), (D // 2) ** -0.5, 0.1875, ((0, 8), (1, 4)), jnp.float32)
    w_key = bell_draw(splits[4], (D, HEADS * HEAD_DIM), (D // 2) ** -0.5, 0.1875, ((0, 8), (1, 4)), jnp.float32)
    w_value = bell_draw(splits[5], (D, HEADS * HEAD_DIM), D ** -0.5, 0.125, ((0, 8), (1, 4)), jnp.float32)
    w_output = bell_draw(splits[6], (HEADS * HEAD_DIM, D), (max(D // 64, 4)) ** -0.5, 1.0, ((0, 4), (1, 8)), jnp.float32)
    w_gate = bell_draw(splits[7], (D, FF), D ** -0.5, 0.125, ((0, 8), (1, 4)), jnp.float32)
    w_up = bell_draw(splits[8], (D, FF), D ** -0.5, 0.125, ((0, 8), (1, 4)), jnp.float32)
    w_down = bell_draw(splits[9], (FF, D), FF ** -0.5, 0.0625, ((0, 4), (1, 8)), jnp.float32)
    return dict(tokens=tokens, lengths=lengths, cotangent=cotangent, w_query=w_query, w_key=w_key, w_value=w_value, w_output=w_output, w_gate=w_gate, w_up=w_up, w_down=w_down)


@jax.custom_vjp
def low(v):
    return lax.optimization_barrier(v.astype(jnp.bfloat16)).astype(jnp.float32)

@jax.custom_vjp
def low_back(v):
    return v

def low_keep(v):
    return (low(v), None)

def low_pass(kept, grad):
    return (grad,)

def back_keep(v):
    return (v, None)

def back_low(kept, grad):
    return (low(grad),)
low.defvjp(low_keep, low_pass)
low_back.defvjp(back_keep, back_low)

def matmul(left, right):
    return jnp.dot(left, right, precision=lax.Precision.HIGHEST, preferred_element_type=jnp.float32)

def normalize(values):
    center = values - lax.optimization_barrier(jnp.mean(values, axis=-1, keepdims=True))
    spread = lax.optimization_barrier(jnp.mean(center * center, axis=-1, keepdims=True))
    return center * lax.rsqrt(spread + 1e-05)

def rope_tables(row_count, head_size, offset):
    positions = (jnp.arange(row_count) + offset).astype(jnp.float32)
    inverse = 10000.0 ** (-(jnp.arange(head_size // 2).astype(jnp.float32) * 2.0) / head_size)
    angles = positions[:, None] * inverse[None, :]
    angles = jnp.concatenate([angles, angles], axis=-1)
    return (jnp.cos(angles)[:, None, :], jnp.sin(angles)[:, None, :])

def rotate(values, cosine, sine_table):
    half_dim = values.shape[-1] // 2
    front_half = values[..., :half_dim]
    back_half = values[..., half_dim:]
    turned = jnp.concatenate([-back_half, front_half], axis=-1)
    return values * cosine + turned * sine_table

def attend_sequence(queries, keys_all, values_all, length):
    row_count = queries.shape[0]
    block_rows = min(512, row_count)
    block_count = row_count // block_rows
    score_scale = HEAD_DIM ** (-0.5)
    key_pos = jnp.arange(row_count)

    def one_block(query_rows, start):
        row_pos = start + jnp.arange(block_rows)
        scores = jnp.einsum('qhd,khd->hqk', query_rows, keys_all, precision=lax.Precision.HIGHEST, preferred_element_type=jnp.float32) * score_scale
        scores = low_back(scores)
        allowed = (key_pos[None, :] <= row_pos[:, None]) & (key_pos[None, :] < length)
        scores = jnp.where(allowed[None], scores, -1e+30)
        row_peak = lax.optimization_barrier(jnp.max(scores, axis=-1, keepdims=True))
        log_total = jnp.log(lax.optimization_barrier(jnp.sum(jnp.exp(scores - row_peak), axis=-1, keepdims=True))) + row_peak
        probability = low(jnp.exp(scores - log_total))
        return jnp.einsum('hqk,khd->qhd', probability, values_all, precision=lax.Precision.HIGHEST, preferred_element_type=jnp.float32)
    checked = jax.checkpoint(one_block)
    grouped = queries.reshape(block_count, block_rows, HEADS, HEAD_DIM)
    starts = jnp.arange(block_count) * block_rows
    attended = lax.map(lambda paired: checked(paired[0], paired[1]), (grouped, starts))
    return attended.reshape(row_count, HEADS, HEAD_DIM)

def layer(tokens_row, length, matrices):
    w_query, w_key, w_value, w_output, w_gate, w_up, w_down = [low(matrix) for matrix in matrices]
    row_count = tokens_row.shape[0]
    split_heads = (row_count, HEADS, HEAD_DIM)
    normed = low(normalize(tokens_row))
    cosine, sine_table = rope_tables(row_count, HEAD_DIM, 0)
    query_pre = low_back(matmul(normed, w_query)).reshape(split_heads)
    key_pre = low_back(matmul(normed, w_key)).reshape(split_heads)
    queries = low(rotate(query_pre, cosine, sine_table))
    keys_all = low(rotate(key_pre, cosine, sine_table))
    values_all = low(low_back(matmul(normed, w_value))).reshape(split_heads)
    attended = attend_sequence(queries, keys_all, values_all, length)
    attended = low(low_back(attended)).reshape(row_count, HEADS * HEAD_DIM)
    resid = tokens_row + low_back(matmul(attended, w_output))
    normed_two = low(normalize(resid))
    gate_proj = low_back(matmul(normed_two, w_gate))
    up_proj = low_back(matmul(normed_two, w_up))
    hidden = low(jax.nn.silu(gate_proj) * up_proj)
    return resid + low_back(matmul(hidden, w_down))

def reference(tokens, lengths, cotangent, w_query, w_key, w_value, w_output, w_gate, w_up, w_down):
    weights = (w_query, w_key, w_value, w_output, w_gate, w_up, w_down)
    positions = jnp.arange(SEQ_LEN)

    def one_sequence(grads, inputs):
        tokens_row, cot_row, length = inputs
        tokens_wide = tokens_row.astype(jnp.float32)
        valid_mask = (positions < length).astype(jnp.float32)

        def forward(tok_in, matrices):
            return layer(tok_in, length, matrices)
        final_sum, pullback = jax.vjp(forward, tokens_wide, weights)
        cot_wide = cot_row.astype(jnp.float32) * valid_mask[:, None]
        grad_input, grad_weights = pullback(cot_wide)
        new_grads = tuple((summed + piece_grad for summed, piece_grad in zip(grads, grad_weights)))
        return (new_grads, (final_sum.astype(jnp.bfloat16), grad_input))
    start_grads = tuple((jnp.zeros_like(matrix) for matrix in weights))
    grads, stacked = lax.scan(one_sequence, start_grads, (tokens, cotangent, lengths))
    output, grad_tokens = stacked
    return (output, grad_tokens, grads[0], grads[1], grads[2], grads[3], grads[4], grads[5], grads[6])
```

```python
import jax
import jax.numpy as jnp
from jax import lax
from jax.sharding import PartitionSpec as P

HEAD_DIM = 128


EPSILON = 1e-05


def normalize(values):
    center = values - jnp.mean(values, axis=-1, keepdims=True)
    inv_scale = lax.rsqrt(jnp.mean(center * center, axis=-1, keepdims=True) + EPSILON)
    return (center * inv_scale, inv_scale)


def norm_back(normed, inv_scale, upstream):
    first_mean = jnp.mean(upstream, axis=-1, keepdims=True)
    second_mean = jnp.mean(upstream * normed, axis=-1, keepdims=True)
    return inv_scale * (upstream - first_mean - normed * second_mean)


def rope_tables(row_count, head_size, offset):
    positions = (jnp.arange(row_count) + offset).astype(jnp.float32)
    inverse = 10000.0 ** (-(jnp.arange(head_size // 2).astype(jnp.float32) * 2.0) / head_size)
    angles = positions[:, None] * inverse[None, :]
    angles = jnp.concatenate([angles, angles], axis=-1)
    return (jnp.cos(angles)[:, None, :], jnp.sin(angles)[:, None, :])


def turn_half(values):
    half_dim = values.shape[-1] // 2
    return jnp.concatenate([-values[..., half_dim:], values[..., :half_dim]], axis=-1)


def rotate(values, cosine, sine_table):
    return values * cosine + turn_half(values) * sine_table


def rotate_back(values, cosine, sine_table):
    return values * cosine - turn_half(values) * sine_table


def score_block(query_rows, keys_seq, length, row_start):
    block_rows = query_rows.shape[0]
    key_pos = jnp.arange(keys_seq.shape[0])
    row_pos = row_start + jnp.arange(block_rows)
    scores = jnp.einsum(
        "qhd,khd->hqk", query_rows, keys_seq, preferred_element_type=jnp.float32
    ) * HEAD_DIM ** (-0.5)
    allowed = (key_pos[None, :] <= row_pos[:, None]) & (key_pos[None, :] < length)
    return jnp.where(allowed[None], scores, -1e30)


def attend_forward(queries_seq, keys_seq, values_seq, length, offset):
    half_len, head_count, head_size = queries_seq.shape
    block_rows = min(512, half_len)
    block_count = half_len // block_rows
    grouped = queries_seq.reshape(block_count, block_rows, head_count, head_size)

    def one_block(paired):
        query_rows, block_index = paired
        scores = score_block(query_rows, keys_seq, length, offset + block_index * block_rows)
        row_peak = jnp.max(scores, axis=-1, keepdims=True)
        log_total = jnp.log(jnp.sum(jnp.exp(scores - row_peak), axis=-1, keepdims=True)) + row_peak
        probability = jnp.exp(scores - log_total).astype(jnp.bfloat16)
        attended = jnp.einsum(
            "hqk,khd->qhd", probability, values_seq, preferred_element_type=jnp.float32
        )
        return (attended.astype(jnp.bfloat16), log_total[..., 0])

    attended, log_totals = lax.map(one_block, (grouped, jnp.arange(block_count)))
    return (attended.reshape(half_len, head_count, head_size), log_totals)


def attend_backward(queries_seq, keys_seq, values_seq, length, offset, log_totals, grad_seq):
    half_len, head_count, head_size = queries_seq.shape
    block_rows = min(512, half_len)
    block_count = half_len // block_rows
    score_scale = HEAD_DIM ** (-0.5)
    grouped = queries_seq.reshape(block_count, block_rows, head_count, head_size)
    grad_grouped = grad_seq.reshape(block_count, block_rows, head_count, head_size)

    def one_block(carried, paired):
        query_rows, grad_rows, log_rows, block_index = paired
        scores = score_block(query_rows, keys_seq, length, offset + block_index * block_rows)
        probability = jnp.exp(scores - log_rows[..., None])
        prob_low = probability.astype(jnp.bfloat16)
        grad_prob = jnp.einsum(
            "qhd,khd->hqk", grad_rows, values_seq, preferred_element_type=jnp.float32
        )
        inner_sum = jnp.sum(probability * grad_prob, axis=-1, keepdims=True)
        grad_scores = (probability * (grad_prob - inner_sum)).astype(jnp.bfloat16)
        grad_query_rows = (
            jnp.einsum("hqk,khd->qhd", grad_scores, keys_seq, preferred_element_type=jnp.float32)
            * score_scale
        )
        key_part = (
            jnp.einsum("hqk,qhd->khd", grad_scores, query_rows, preferred_element_type=jnp.float32)
            * score_scale
        )
        value_part = jnp.einsum(
            "hqk,qhd->khd", prob_low, grad_rows, preferred_element_type=jnp.float32
        )
        return ((carried[0] + key_part, carried[1] + value_part), grad_query_rows)

    empty = jnp.zeros(keys_seq.shape, jnp.float32)
    sums, grad_queries = lax.scan(
        one_block, (empty, empty), (grouped, grad_grouped, log_totals, jnp.arange(block_count))
    )
    return (grad_queries.reshape(half_len, head_count, head_size), sums[0], sums[1])


def scatter_low(grad, dim):
    summed = lax.psum_scatter(
        grad.astype(jnp.bfloat16), ("shard", "ctx"), scatter_dimension=dim, tiled=True
    )
    return summed.astype(jnp.float32)


def matmul_low(left, right):
    return jnp.dot(left, right, preferred_element_type=jnp.float32)


def body(tokens, lengths, cotangent, w_query, w_key, w_value, w_output, w_gate, w_up, w_down):
    seq_count, half_len, model_width = tokens.shape
    head_cols = w_query.shape[1]
    head_count = head_cols // HEAD_DIM
    row_total = seq_count * half_len
    offset = lax.axis_index("ctx") * half_len
    positions = offset + jnp.arange(half_len)
    valid_mask = (positions[None, :] < lengths[:, None]).astype(jnp.float32)
    bf_type = jnp.bfloat16
    attn_low = (
        w_query.astype(bf_type),
        w_key.astype(bf_type),
        w_value.astype(bf_type),
        w_output.astype(bf_type),
    )
    mlp_low = (w_gate.astype(bf_type), w_up.astype(bf_type), w_down.astype(bf_type))
    query_full, key_full, value_full, output_full = (
        lax.all_gather(attn_low[0], ("shard", "ctx"), axis=0, tiled=True),
        lax.all_gather(attn_low[1], ("shard", "ctx"), axis=0, tiled=True),
        lax.all_gather(attn_low[2], ("shard", "ctx"), axis=0, tiled=True),
        lax.all_gather(attn_low[3], ("shard", "ctx"), axis=1, tiled=True),
    )
    gate_full, up_full, down_full = (
        lax.all_gather(mlp_low[0], ("shard", "ctx"), axis=0, tiled=True),
        lax.all_gather(mlp_low[1], ("shard", "ctx"), axis=0, tiled=True),
        lax.all_gather(mlp_low[2], ("shard", "ctx"), axis=1, tiled=True),
    )
    tokens_wide = tokens.astype(jnp.float32).reshape(row_total, model_width)
    normed_one, scale_one = normalize(tokens_wide)
    input_one = normed_one.astype(bf_type)
    split_heads = (seq_count, half_len, head_count, HEAD_DIM)
    query_pre = matmul_low(input_one, query_full).reshape(split_heads)
    key_pre = matmul_low(input_one, key_full).reshape(split_heads)
    value_pre = matmul_low(input_one, value_full).reshape(split_heads)
    cosine, sine_table = rope_tables(half_len, HEAD_DIM, offset)
    queries = rotate(query_pre, cosine, sine_table).astype(bf_type)
    keys_rot = rotate(key_pre, cosine, sine_table).astype(bf_type)
    values_low = value_pre.astype(bf_type)
    keys_all, values_all = (
        lax.all_gather(keys_rot, "ctx", axis=1, tiled=True),
        lax.all_gather(values_low, "ctx", axis=1, tiled=True),
    )
    seq_index = 0
    attended, log_totals = attend_forward(
        queries[seq_index], keys_all[seq_index], values_all[seq_index], lengths[seq_index], offset
    )
    attended_list = [attended]
    log_list = [log_totals]
    attn_out = jnp.stack(attended_list).reshape(row_total, head_cols)
    branch_part = matmul_low(attn_out, output_full)
    resid = tokens_wide + lax.psum(branch_part.astype(bf_type), "tp").astype(jnp.float32)
    normed_two, scale_two = normalize(resid)
    input_two = normed_two.astype(bf_type)
    gate_proj = matmul_low(input_two, gate_full)
    up_proj = matmul_low(input_two, up_full)
    gate_sigmoid = jax.nn.sigmoid(gate_proj)
    hidden = (gate_proj * gate_sigmoid * up_proj).astype(bf_type)
    branch_two_part = matmul_low(hidden, down_full)
    final_sum = resid + lax.psum(branch_two_part.astype(jnp.bfloat16), "tp").astype(jnp.float32)
    grad_final = cotangent.astype(jnp.float32).reshape(row_total, model_width) * valid_mask.reshape(
        row_total, 1
    )
    grad_branch = grad_final.astype(bf_type)
    grad_down = jnp.einsum("rf,rd->fd", hidden, grad_branch, preferred_element_type=jnp.float32)
    grad_hidden = jnp.einsum(
        "rd,fd->rf", grad_branch, down_full, preferred_element_type=jnp.float32
    )
    grad_gate_act = (
        grad_hidden * up_proj * gate_sigmoid * (1.0 + gate_proj * (1.0 - gate_sigmoid))
    ).astype(bf_type)
    grad_up_act = (grad_hidden * gate_proj * gate_sigmoid).astype(bf_type)
    grad_gate = jnp.einsum(
        "rd,rf->df", input_two, grad_gate_act, preferred_element_type=jnp.float32
    )
    grad_up = jnp.einsum("rd,rf->df", input_two, grad_up_act, preferred_element_type=jnp.float32)
    grad_input_two = jnp.einsum(
        "rf,df->rd", grad_gate_act, gate_full, preferred_element_type=jnp.float32
    ) + jnp.einsum("rf,df->rd", grad_up_act, up_full, preferred_element_type=jnp.float32)
    mlp_grads = (
        scatter_low(grad_gate, 0),
        scatter_low(grad_up, 0),
        scatter_low(grad_down, 1),
    )
    grad_input_two = lax.psum(grad_input_two.astype(bf_type), "tp").astype(jnp.float32)
    grad_resid = grad_final + norm_back(normed_two, scale_two, grad_input_two)
    grad_resid_low = grad_resid.astype(bf_type)
    grad_wout = jnp.einsum(
        "rc,rd->cd", attn_out, grad_resid_low, preferred_element_type=jnp.float32
    )
    grad_attn = jnp.einsum(
        "rd,cd->rc", grad_resid_low, output_full, preferred_element_type=jnp.float32
    )
    grad_attn = grad_attn.astype(bf_type).reshape(split_heads)
    seq_index = 0
    grad_queries, grad_keys_seq, grad_values_seq = attend_backward(
        queries[seq_index],
        keys_all[seq_index],
        values_all[seq_index],
        lengths[seq_index],
        offset,
        log_list[seq_index],
        grad_attn[seq_index],
    )
    query_grads = [grad_queries]
    key_grads = [grad_keys_seq]
    value_grads = [grad_values_seq]
    grad_keys, grad_values = (
        lax.psum_scatter(jnp.stack(key_grads), "ctx", scatter_dimension=1, tiled=True),
        lax.psum_scatter(jnp.stack(value_grads), "ctx", scatter_dimension=1, tiled=True),
    )
    grad_q_pre = (
        rotate_back(jnp.stack(query_grads), cosine, sine_table)
        .astype(bf_type)
        .reshape(row_total, head_cols)
    )
    grad_k_pre = (
        rotate_back(grad_keys, cosine, sine_table).astype(bf_type).reshape(row_total, head_cols)
    )
    grad_v_pre = grad_values.astype(bf_type).reshape(row_total, head_cols)
    grad_wq = jnp.einsum("rd,rc->dc", input_one, grad_q_pre, preferred_element_type=jnp.float32)
    grad_wk = jnp.einsum("rd,rc->dc", input_one, grad_k_pre, preferred_element_type=jnp.float32)
    grad_wv = jnp.einsum("rd,rc->dc", input_one, grad_v_pre, preferred_element_type=jnp.float32)
    grad_input_one = (
        jnp.einsum("rc,dc->rd", grad_q_pre, query_full, preferred_element_type=jnp.float32)
        + jnp.einsum("rc,dc->rd", grad_k_pre, key_full, preferred_element_type=jnp.float32)
        + jnp.einsum("rc,dc->rd", grad_v_pre, value_full, preferred_element_type=jnp.float32)
    )
    attn_grads = (
        scatter_low(grad_wq, 0),
        scatter_low(grad_wk, 0),
        scatter_low(grad_wv, 0),
        scatter_low(grad_wout, 1),
    )
    grad_input_one = lax.psum(grad_input_one.astype(bf_type), "tp").astype(jnp.float32)
    grad_tokens = grad_resid + norm_back(normed_one, scale_one, grad_input_one)
    output = final_sum.astype(bf_type).reshape(seq_count, half_len, model_width)
    grad_tokens = grad_tokens.reshape(seq_count, half_len, model_width)
    return (
        output,
        grad_tokens,
        attn_grads[0],
        attn_grads[1],
        attn_grads[2],
        attn_grads[3],
        mlp_grads[0],
        mlp_grads[1],
        mlp_grads[2],
    )


def solution(mesh):
    return jax.shard_map(
        body,
        mesh=mesh,
        in_specs=(
            P("shard", "ctx", None),
            P("shard"),
            P("shard", "ctx", None),
            P(("shard", "ctx"), "tp"),
            P(("shard", "ctx"), "tp"),
            P(("shard", "ctx"), "tp"),
            P("tp", ("shard", "ctx")),
            P(("shard", "ctx"), "tp"),
            P(("shard", "ctx"), "tp"),
            P("tp", ("shard", "ctx")),
        ),
        out_specs=(
            P("shard", "ctx", None),
            P("shard", "ctx", None),
            P(("shard", "ctx"), "tp"),
            P(("shard", "ctx"), "tp"),
            P(("shard", "ctx"), "tp"),
            P("tp", ("shard", "ctx")),
            P(("shard", "ctx"), "tp"),
            P(("shard", "ctx"), "tp"),
            P("tp", ("shard", "ctx")),
        ),
        check_vma=False,
    )
```

```python
import functools

import jax
import jax.numpy as jnp
from jax import lax
from jax.sharding import PartitionSpec as P

HEAD_DIM = 128


EPSILON = 1e-05


def normalize(values):
    center = values - jnp.mean(values, axis=-1, keepdims=True)
    inv_scale = lax.rsqrt(jnp.mean(center * center, axis=-1, keepdims=True) + EPSILON)
    return (center * inv_scale, inv_scale)


def norm_back(normed, inv_scale, upstream):
    first_mean = jnp.mean(upstream, axis=-1, keepdims=True)
    second_mean = jnp.mean(upstream * normed, axis=-1, keepdims=True)
    return inv_scale * (upstream - first_mean - normed * second_mean)


def rope_tables(row_count, head_size, offset):
    positions = (jnp.arange(row_count) + offset).astype(jnp.float32)
    inverse = 10000.0 ** (-(jnp.arange(head_size // 2).astype(jnp.float32) * 2.0) / head_size)
    angles = positions[:, None] * inverse[None, :]
    angles = jnp.concatenate([angles, angles], axis=-1)
    return (jnp.cos(angles)[:, None, :], jnp.sin(angles)[:, None, :])


def turn_half(values):
    half_dim = values.shape[-1] // 2
    return jnp.concatenate([-values[..., half_dim:], values[..., :half_dim]], axis=-1)


def rotate(values, cosine, sine_table):
    return values * cosine + turn_half(values) * sine_table


def rotate_back(values, cosine, sine_table):
    return values * cosine - turn_half(values) * sine_table


def score_block(query_rows, keys_seq, length, row_start):
    block_rows = query_rows.shape[0]
    key_pos = jnp.arange(keys_seq.shape[0])
    row_pos = row_start + jnp.arange(block_rows)
    scores = jnp.einsum(
        "qhd,khd->hqk", query_rows, keys_seq, preferred_element_type=jnp.float32
    ) * HEAD_DIM ** (-0.5)
    allowed = (key_pos[None, :] <= row_pos[:, None]) & (key_pos[None, :] < length)
    return jnp.where(allowed[None], scores, -1e30)


def attend_forward(queries_seq, keys_seq, values_seq, length, offset):
    half_len, head_count, head_size = queries_seq.shape
    block_rows = min(512, half_len)
    block_count = half_len // block_rows
    grouped = queries_seq.reshape(block_count, block_rows, head_count, head_size)

    def one_block(paired):
        query_rows, block_index = paired
        scores = score_block(query_rows, keys_seq, length, offset + block_index * block_rows)
        row_peak = jnp.max(scores, axis=-1, keepdims=True)
        log_total = jnp.log(jnp.sum(jnp.exp(scores - row_peak), axis=-1, keepdims=True)) + row_peak
        probability = jnp.exp(scores - log_total).astype(jnp.bfloat16)
        attended = jnp.einsum(
            "hqk,khd->qhd", probability, values_seq, preferred_element_type=jnp.float32
        )
        return (attended.astype(jnp.bfloat16), log_total[..., 0])

    attended, log_totals = lax.map(one_block, (grouped, jnp.arange(block_count)))
    return (attended.reshape(half_len, head_count, head_size), log_totals)


def attend_backward(queries_seq, keys_seq, values_seq, length, offset, log_totals, grad_seq):
    half_len, head_count, head_size = queries_seq.shape
    block_rows = min(512, half_len)
    block_count = half_len // block_rows
    score_scale = HEAD_DIM ** (-0.5)
    grouped = queries_seq.reshape(block_count, block_rows, head_count, head_size)
    grad_grouped = grad_seq.reshape(block_count, block_rows, head_count, head_size)

    def one_block(carried, paired):
        query_rows, grad_rows, log_rows, block_index = paired
        scores = score_block(query_rows, keys_seq, length, offset + block_index * block_rows)
        probability = jnp.exp(scores - log_rows[..., None])
        prob_low = probability.astype(jnp.bfloat16)
        grad_prob = jnp.einsum(
            "qhd,khd->hqk", grad_rows, values_seq, preferred_element_type=jnp.float32
        )
        inner_sum = jnp.sum(probability * grad_prob, axis=-1, keepdims=True)
        grad_scores = (probability * (grad_prob - inner_sum)).astype(jnp.bfloat16)
        grad_query_rows = (
            jnp.einsum("hqk,khd->qhd", grad_scores, keys_seq, preferred_element_type=jnp.float32)
            * score_scale
        )
        key_part = (
            jnp.einsum("hqk,qhd->khd", grad_scores, query_rows, preferred_element_type=jnp.float32)
            * score_scale
        )
        value_part = jnp.einsum(
            "hqk,qhd->khd", prob_low, grad_rows, preferred_element_type=jnp.float32
        )
        return ((carried[0] + key_part, carried[1] + value_part), grad_query_rows)

    empty = jnp.zeros(keys_seq.shape, jnp.float32)
    sums, grad_queries = lax.scan(
        one_block, (empty, empty), (grouped, grad_grouped, log_totals, jnp.arange(block_count))
    )
    return (grad_queries.reshape(half_len, head_count, head_size), sums[0], sums[1])


def tp_psum(part, count):
    me = lax.axis_index("tp")
    low_part = part.astype(jnp.bfloat16)
    rows = part.shape[0] // count
    chunks = low_part.reshape((count, rows) + part.shape[1:])
    total = lax.dynamic_index_in_dim(chunks, me, 0, keepdims=False).astype(jnp.float32)
    for shift in range(1, count):
        pairs = [(i, (i + shift) % count) for i in range(count)]
        piece = lax.dynamic_index_in_dim(chunks, (me + shift) % count, 0, keepdims=False)
        total = total + lax.ppermute(piece, "tp", pairs).astype(jnp.float32)
    reduced = total.astype(jnp.bfloat16)
    gathered = jnp.zeros(low_part.shape, jnp.bfloat16)
    gathered = lax.dynamic_update_slice_in_dim(gathered, reduced, me * rows, 0)
    for shift in range(1, count):
        pairs = [(i, (i + shift) % count) for i in range(count)]
        got = lax.ppermute(reduced, "tp", pairs)
        gathered = lax.dynamic_update_slice_in_dim(
            gathered, got, ((me + count - shift) % count) * rows, 0
        )
    return gathered


def scatter_low(grad, dim):
    summed = lax.psum_scatter(
        grad.astype(jnp.bfloat16), ("shard", "ctx"), scatter_dimension=dim, tiled=True
    )
    return summed.astype(jnp.float32)


def matmul_low(left, right):
    return jnp.dot(left, right, preferred_element_type=jnp.float32)


def body(tp_count, tokens, lengths, cotangent, w_query, w_key, w_value, w_output, w_gate, w_up, w_down):
    seq_count, half_len, model_width = tokens.shape
    head_cols = w_query.shape[1]
    head_count = head_cols // HEAD_DIM
    row_total = seq_count * half_len
    offset = lax.axis_index("ctx") * half_len
    positions = offset + jnp.arange(half_len)
    valid_mask = (positions[None, :] < lengths[:, None]).astype(jnp.float32)
    bf_type = jnp.bfloat16
    attn_low = (
        w_query.astype(bf_type),
        w_key.astype(bf_type),
        w_value.astype(bf_type),
        w_output.astype(bf_type),
    )
    mlp_low = (w_gate.astype(bf_type), w_up.astype(bf_type), w_down.astype(bf_type))
    query_full, key_full, value_full, output_full = (
        lax.all_gather(attn_low[0], ("shard", "ctx"), axis=0, tiled=True),
        lax.all_gather(attn_low[1], ("shard", "ctx"), axis=0, tiled=True),
        lax.all_gather(attn_low[2], ("shard", "ctx"), axis=0, tiled=True),
        lax.all_gather(attn_low[3], ("shard", "ctx"), axis=1, tiled=True),
    )
    gate_full, up_full, down_full = (
        lax.all_gather(mlp_low[0], ("shard", "ctx"), axis=0, tiled=True),
        lax.all_gather(mlp_low[1], ("shard", "ctx"), axis=0, tiled=True),
        lax.all_gather(mlp_low[2], ("shard", "ctx"), axis=1, tiled=True),
    )
    tokens_wide = tokens.astype(jnp.float32).reshape(row_total, model_width)
    normed_one, scale_one = normalize(tokens_wide)
    input_one = normed_one.astype(bf_type)
    split_heads = (seq_count, half_len, head_count, HEAD_DIM)
    query_pre = matmul_low(input_one, query_full).reshape(split_heads)
    key_pre = matmul_low(input_one, key_full).reshape(split_heads)
    value_pre = matmul_low(input_one, value_full).reshape(split_heads)
    cosine, sine_table = rope_tables(half_len, HEAD_DIM, offset)
    queries = rotate(query_pre, cosine, sine_table).astype(bf_type)
    keys_rot = rotate(key_pre, cosine, sine_table).astype(bf_type)
    values_low = value_pre.astype(bf_type)
    keys_all, values_all = (
        lax.all_gather(keys_rot, "ctx", axis=1, tiled=True),
        lax.all_gather(values_low, "ctx", axis=1, tiled=True),
    )
    seq_index = 0
    attended, log_totals = attend_forward(
        queries[seq_index], keys_all[seq_index], values_all[seq_index], lengths[seq_index], offset
    )
    attended_list = [attended]
    log_list = [log_totals]
    attn_out = jnp.stack(attended_list).reshape(row_total, head_cols)
    branch_part = matmul_low(attn_out, output_full)
    resid = tokens_wide + tp_psum(branch_part, tp_count).astype(jnp.float32)
    normed_two, scale_two = normalize(resid)
    input_two = normed_two.astype(bf_type)
    gate_proj = matmul_low(input_two, gate_full)
    up_proj = matmul_low(input_two, up_full)
    gate_sigmoid = jax.nn.sigmoid(gate_proj)
    hidden = (gate_proj * gate_sigmoid * up_proj).astype(bf_type)
    branch_two_part = matmul_low(hidden, down_full)
    final_sum = resid + tp_psum(branch_two_part, tp_count).astype(jnp.float32)
    grad_final = cotangent.astype(jnp.float32).reshape(row_total, model_width) * valid_mask.reshape(
        row_total, 1
    )
    grad_branch = grad_final.astype(bf_type)
    grad_down = jnp.einsum("rf,rd->fd", hidden, grad_branch, preferred_element_type=jnp.float32)
    grad_hidden = jnp.einsum(
        "rd,fd->rf", grad_branch, down_full, preferred_element_type=jnp.float32
    )
    grad_gate_act = (
        grad_hidden * up_proj * gate_sigmoid * (1.0 + gate_proj * (1.0 - gate_sigmoid))
    ).astype(bf_type)
    grad_up_act = (grad_hidden * gate_proj * gate_sigmoid).astype(bf_type)
    grad_gate = jnp.einsum(
        "rd,rf->df", input_two, grad_gate_act, preferred_element_type=jnp.float32
    )
    grad_up = jnp.einsum("rd,rf->df", input_two, grad_up_act, preferred_element_type=jnp.float32)
    grad_input_two = jnp.einsum(
        "rf,df->rd", grad_gate_act, gate_full, preferred_element_type=jnp.float32
    ) + jnp.einsum("rf,df->rd", grad_up_act, up_full, preferred_element_type=jnp.float32)
    mlp_grads = (
        scatter_low(grad_gate, 0),
        scatter_low(grad_up, 0),
        scatter_low(grad_down, 1),
    )
    grad_input_two = tp_psum(grad_input_two, tp_count).astype(jnp.float32)
    grad_resid = grad_final + norm_back(normed_two, scale_two, grad_input_two)
    grad_resid_low = grad_resid.astype(bf_type)
    grad_wout = jnp.einsum(
        "rc,rd->cd", attn_out, grad_resid_low, preferred_element_type=jnp.float32
    )
    grad_attn = jnp.einsum(
        "rd,cd->rc", grad_resid_low, output_full, preferred_element_type=jnp.float32
    )
    grad_attn = grad_attn.astype(bf_type).reshape(split_heads)
    seq_index = 0
    grad_queries, grad_keys_seq, grad_values_seq = attend_backward(
        queries[seq_index],
        keys_all[seq_index],
        values_all[seq_index],
        lengths[seq_index],
        offset,
        log_list[seq_index],
        grad_attn[seq_index],
    )
    query_grads = [grad_queries]
    key_grads = [grad_keys_seq]
    value_grads = [grad_values_seq]
    grad_keys, grad_values = (
        lax.psum_scatter(jnp.stack(key_grads), "ctx", scatter_dimension=1, tiled=True),
        lax.psum_scatter(jnp.stack(value_grads), "ctx", scatter_dimension=1, tiled=True),
    )
    grad_q_pre = (
        rotate_back(jnp.stack(query_grads), cosine, sine_table)
        .astype(bf_type)
        .reshape(row_total, head_cols)
    )
    grad_k_pre = (
        rotate_back(grad_keys, cosine, sine_table).astype(bf_type).reshape(row_total, head_cols)
    )
    grad_v_pre = grad_values.astype(bf_type).reshape(row_total, head_cols)
    grad_wq = jnp.einsum("rd,rc->dc", input_one, grad_q_pre, preferred_element_type=jnp.float32)
    grad_wk = jnp.einsum("rd,rc->dc", input_one, grad_k_pre, preferred_element_type=jnp.float32)
    grad_wv = jnp.einsum("rd,rc->dc", input_one, grad_v_pre, preferred_element_type=jnp.float32)
    grad_input_one = (
        jnp.einsum("rc,dc->rd", grad_q_pre, query_full, preferred_element_type=jnp.float32)
        + jnp.einsum("rc,dc->rd", grad_k_pre, key_full, preferred_element_type=jnp.float32)
        + jnp.einsum("rc,dc->rd", grad_v_pre, value_full, preferred_element_type=jnp.float32)
    )
    attn_grads = (
        scatter_low(grad_wq, 0),
        scatter_low(grad_wk, 0),
        scatter_low(grad_wv, 0),
        scatter_low(grad_wout, 1),
    )
    grad_input_one = tp_psum(grad_input_one, tp_count).astype(jnp.float32)
    grad_tokens = grad_resid + norm_back(normed_one, scale_one, grad_input_one)
    output = final_sum.astype(bf_type).reshape(seq_count, half_len, model_width)
    grad_tokens = grad_tokens.reshape(seq_count, half_len, model_width)
    return (
        output,
        grad_tokens,
        attn_grads[0],
        attn_grads[1],
        attn_grads[2],
        attn_grads[3],
        mlp_grads[0],
        mlp_grads[1],
        mlp_grads[2],
    )


def solution(mesh):
    return jax.shard_map(
        functools.partial(body, mesh.shape["tp"]),
        mesh=mesh,
        in_specs=(
            P("shard", "ctx", None),
            P("shard"),
            P("shard", "ctx", None),
            P(("shard", "ctx"), "tp"),
            P(("shard", "ctx"), "tp"),
            P(("shard", "ctx"), "tp"),
            P("tp", ("shard", "ctx")),
            P(("shard", "ctx"), "tp"),
            P(("shard", "ctx"), "tp"),
            P("tp", ("shard", "ctx")),
        ),
        out_specs=(
            P("shard", "ctx", None),
            P("shard", "ctx", None),
            P(("shard", "ctx"), "tp"),
            P(("shard", "ctx"), "tp"),
            P(("shard", "ctx"), "tp"),
            P("tp", ("shard", "ctx")),
            P(("shard", "ctx"), "tp"),
            P(("shard", "ctx"), "tp"),
            P("tp", ("shard", "ctx")),
        ),
        check_vma=False,
    )
```

```python
import functools

import jax
import jax.numpy as jnp
from jax import lax
from jax.sharding import PartitionSpec as P

SHARD, CTX, TP = "shard", "ctx", "tp"

HEAD_DIM = 128


EPSILON = 1e-05


def normalize(values):
    center = values - jnp.mean(values, axis=-1, keepdims=True)
    inv_scale = lax.rsqrt(jnp.mean(center * center, axis=-1, keepdims=True) + EPSILON)
    return (center * inv_scale, inv_scale)


def norm_back(normed, inv_scale, upstream):
    first_mean = jnp.mean(upstream, axis=-1, keepdims=True)
    second_mean = jnp.mean(upstream * normed, axis=-1, keepdims=True)
    return inv_scale * (upstream - first_mean - normed * second_mean)


def rope_tables(row_count, head_size, offset):
    positions = (jnp.arange(row_count) + offset).astype(jnp.float32)
    inverse = 10000.0 ** (-(jnp.arange(head_size // 2).astype(jnp.float32) * 2.0) / head_size)
    angles = positions[:, None] * inverse[None, :]
    angles = jnp.concatenate([angles, angles], axis=-1)
    return (jnp.cos(angles)[:, None, :], jnp.sin(angles)[:, None, :])


def turn_half(values):
    half_dim = values.shape[-1] // 2
    return jnp.concatenate([-values[..., half_dim:], values[..., :half_dim]], axis=-1)


def rotate(values, cosine, sine_table):
    return values * cosine + turn_half(values) * sine_table


def rotate_back(values, cosine, sine_table):
    return values * cosine - turn_half(values) * sine_table


def score_block(query_rows, keys_seq, length, row_start):
    block_rows = query_rows.shape[0]
    key_pos = jnp.arange(keys_seq.shape[0])
    row_pos = row_start + jnp.arange(block_rows)
    scores = jnp.einsum(
        "qhd,khd->hqk", query_rows, keys_seq, preferred_element_type=jnp.float32
    ) * HEAD_DIM ** (-0.5)
    allowed = (key_pos[None, :] <= row_pos[:, None]) & (key_pos[None, :] < length)
    return jnp.where(allowed[None], scores, -1e30)


def attend_forward(queries_seq, keys_seq, values_seq, length, offset):
    half_len, head_count, head_size = queries_seq.shape
    block_rows = min(512, half_len)
    block_count = half_len // block_rows
    grouped = queries_seq.reshape(block_count, block_rows, head_count, head_size)

    def one_block(paired):
        query_rows, block_index = paired
        scores = score_block(query_rows, keys_seq, length, offset + block_index * block_rows)
        row_peak = jnp.max(scores, axis=-1, keepdims=True)
        log_total = jnp.log(jnp.sum(jnp.exp(scores - row_peak), axis=-1, keepdims=True)) + row_peak
        probability = jnp.exp(scores - log_total).astype(jnp.bfloat16)
        attended = jnp.einsum(
            "hqk,khd->qhd", probability, values_seq, preferred_element_type=jnp.float32
        )
        return (attended.astype(jnp.bfloat16), log_total[..., 0])

    attended, log_totals = lax.map(one_block, (grouped, jnp.arange(block_count)))
    return (attended.reshape(half_len, head_count, head_size), log_totals)


def attend_backward(queries_seq, keys_seq, values_seq, length, offset, log_totals, grad_seq):
    half_len, head_count, head_size = queries_seq.shape
    block_rows = min(512, half_len)
    block_count = half_len // block_rows
    score_scale = HEAD_DIM ** (-0.5)
    grouped = queries_seq.reshape(block_count, block_rows, head_count, head_size)
    grad_grouped = grad_seq.reshape(block_count, block_rows, head_count, head_size)

    def one_block(carried, paired):
        query_rows, grad_rows, log_rows, block_index = paired
        scores = score_block(query_rows, keys_seq, length, offset + block_index * block_rows)
        probability = jnp.exp(scores - log_rows[..., None])
        prob_low = probability.astype(jnp.bfloat16)
        grad_prob = jnp.einsum(
            "qhd,khd->hqk", grad_rows, values_seq, preferred_element_type=jnp.float32
        )
        inner_sum = jnp.sum(probability * grad_prob, axis=-1, keepdims=True)
        grad_scores = (probability * (grad_prob - inner_sum)).astype(jnp.bfloat16)
        grad_query_rows = (
            jnp.einsum("hqk,khd->qhd", grad_scores, keys_seq, preferred_element_type=jnp.float32)
            * score_scale
        )
        key_part = (
            jnp.einsum("hqk,qhd->khd", grad_scores, query_rows, preferred_element_type=jnp.float32)
            * score_scale
        )
        value_part = jnp.einsum(
            "hqk,qhd->khd", prob_low, grad_rows, preferred_element_type=jnp.float32
        )
        return ((carried[0] + key_part, carried[1] + value_part), grad_query_rows)

    empty = jnp.zeros(keys_seq.shape, jnp.float32)
    sums, grad_queries = lax.scan(
        one_block, (empty, empty), (grouped, grad_grouped, log_totals, jnp.arange(block_count))
    )
    return (grad_queries.reshape(half_len, head_count, head_size), sums[0], sums[1])


def tp_psum(part, count):
    me = lax.axis_index(TP)
    low_part = part.astype(jnp.bfloat16)
    rows = part.shape[0] // count
    chunks = low_part.reshape((count, rows) + part.shape[1:])
    total = lax.dynamic_index_in_dim(chunks, me, 0, keepdims=False).astype(jnp.float32)
    for shift in range(1, count):
        pairs = [(i, (i + shift) % count) for i in range(count)]
        piece = lax.dynamic_index_in_dim(chunks, (me + shift) % count, 0, keepdims=False)
        total = total + lax.ppermute(piece, TP, pairs).astype(jnp.float32)
    reduced = total.astype(jnp.bfloat16)
    gathered = jnp.zeros(low_part.shape, jnp.bfloat16)
    gathered = lax.dynamic_update_slice_in_dim(gathered, reduced, me * rows, 0)
    for shift in range(1, count):
        pairs = [(i, (i + shift) % count) for i in range(count)]
        got = lax.ppermute(reduced, TP, pairs)
        gathered = lax.dynamic_update_slice_in_dim(
            gathered, got, ((me + count - shift) % count) * rows, 0
        )
    return gathered


def exchange_gather(piece, axis, count):
    me = lax.axis_index(axis)
    gathered = jnp.zeros((count,) + piece.shape, piece.dtype)
    gathered = lax.dynamic_update_index_in_dim(gathered, piece, me, 0)
    for shift in range(1, count):
        pairs = [(i, (i + shift) % count) for i in range(count)]
        got = lax.ppermute(piece, axis, pairs)
        gathered = lax.dynamic_update_index_in_dim(gathered, got, (me + count - shift) % count, 0)
    return gathered


def exchange_scatter(blocks, axis, count):
    me = lax.axis_index(axis)
    total = lax.dynamic_index_in_dim(blocks, me, 0, keepdims=False)
    for shift in range(1, count):
        pairs = [(i, (i + shift) % count) for i in range(count)]
        piece = lax.dynamic_index_in_dim(blocks, (me + shift) % count, 0, keepdims=False)
        total = total + lax.ppermute(piece, axis, pairs)
    return total


def scatter_low(grad, dim):
    summed = lax.psum_scatter(
        grad.astype(jnp.bfloat16), (SHARD, CTX), scatter_dimension=dim, tiled=True
    )
    return summed.astype(jnp.float32)


def matmul_low(left, right):
    return jnp.dot(left, right, preferred_element_type=jnp.float32)


MID_SPLIT = (3, 5)


def middle_rows(attn_rows, tokens_rows, grad_final, output_full, gate_full, up_full, down_full, tp_count):
    bf_type = jnp.bfloat16
    resid = tokens_rows + tp_psum(matmul_low(attn_rows, output_full), tp_count).astype(jnp.float32)
    normed_two, scale_two = normalize(resid)
    input_two = normed_two.astype(bf_type)
    gate_proj = matmul_low(input_two, gate_full)
    up_proj = matmul_low(input_two, up_full)
    gate_sigmoid = jax.nn.sigmoid(gate_proj)
    hidden = (gate_proj * gate_sigmoid * up_proj).astype(bf_type)
    grad_branch = grad_final.astype(bf_type)
    grad_hidden = jnp.einsum(
        "rd,fd->rf", grad_branch, down_full, preferred_element_type=jnp.float32
    )
    grad_gate_act = (
        grad_hidden * up_proj * gate_sigmoid * (1.0 + gate_proj * (1.0 - gate_sigmoid))
    ).astype(bf_type)
    grad_up_act = (grad_hidden * gate_proj * gate_sigmoid).astype(bf_type)
    grad_input_two = jnp.einsum(
        "rf,df->rd", grad_gate_act, gate_full, preferred_element_type=jnp.float32
    ) + jnp.einsum("rf,df->rd", grad_up_act, up_full, preferred_element_type=jnp.float32)
    branch_two = matmul_low(hidden, down_full)
    grad_down = jnp.einsum("rf,rd->fd", hidden, grad_branch, preferred_element_type=jnp.float32)
    grad_gate = jnp.einsum(
        "rd,rf->df", input_two, grad_gate_act, preferred_element_type=jnp.float32
    )
    grad_up = jnp.einsum("rd,rf->df", input_two, grad_up_act, preferred_element_type=jnp.float32)
    grad_input_two = tp_psum(grad_input_two, tp_count)
    return [
        resid, branch_two, normed_two, scale_two, grad_final, grad_input_two,
        grad_gate, grad_up, grad_down,
    ]


def body(tp_count, ctx_count, *args):
    return block(tp_count, ctx_count, *args)


def block(tp_count, ctx_count, tokens, lengths, cotangent, w_query, w_key, w_value, w_output, w_gate, w_up, w_down):
    seq_count, half_len, model_width = tokens.shape
    head_cols = w_query.shape[1]
    head_count = head_cols // HEAD_DIM
    row_total = seq_count * half_len
    offset = lax.axis_index(CTX) * half_len
    positions = offset + jnp.arange(half_len)
    valid_mask = (positions[None, :] < lengths[:, None]).astype(jnp.float32)
    bf_type = jnp.bfloat16
    attn_low = (
        w_query.astype(bf_type),
        w_key.astype(bf_type),
        w_value.astype(bf_type),
        w_output.astype(bf_type),
    )
    mlp_low = (w_gate.astype(bf_type), w_up.astype(bf_type), w_down.astype(bf_type))
    attn_joined = lax.all_gather(
        jnp.concatenate([attn_low[0], attn_low[1], attn_low[2], attn_low[3].T], axis=1),
        (SHARD, CTX),
        axis=0,
        tiled=True,
    )
    query_full, key_full, value_full, output_t = jnp.split(attn_joined, 4, axis=1)
    output_full = output_t.T
    gate_full, up_full, down_full = (
        lax.all_gather(mlp_low[0], (SHARD, CTX), axis=0, tiled=True),
        lax.all_gather(mlp_low[1], (SHARD, CTX), axis=0, tiled=True),
        lax.all_gather(mlp_low[2], (SHARD, CTX), axis=1, tiled=True),
    )
    tokens_wide = tokens.astype(jnp.float32).reshape(row_total, model_width)
    normed_one, scale_one = normalize(tokens_wide)
    input_one = normed_one.astype(bf_type)
    split_heads = (seq_count, half_len, head_count, HEAD_DIM)
    query_pre = matmul_low(input_one, query_full).reshape(split_heads)
    key_pre = matmul_low(input_one, key_full).reshape(split_heads)
    value_pre = matmul_low(input_one, value_full).reshape(split_heads)
    cosine, sine_table = rope_tables(half_len, HEAD_DIM, offset)
    queries = rotate(query_pre, cosine, sine_table).astype(bf_type)
    keys_rot = rotate(key_pre, cosine, sine_table).astype(bf_type)
    values_low = value_pre.astype(bf_type)
    keys_all, values_all = (
        jnp.swapaxes(exchange_gather(keys_rot, CTX, ctx_count), 0, 1).reshape(
            (seq_count, ctx_count * half_len, head_count, HEAD_DIM)
        ),
        jnp.swapaxes(exchange_gather(values_low, CTX, ctx_count), 0, 1).reshape(
            (seq_count, ctx_count * half_len, head_count, HEAD_DIM)
        ),
    )
    seq_index = 0
    attended, log_totals = attend_forward(
        queries[seq_index], keys_all[seq_index], values_all[seq_index], lengths[seq_index], offset
    )
    attended_list = [attended]
    log_list = [log_totals]
    attn_out = jnp.stack(attended_list).reshape(row_total, head_cols)
    grad_final = cotangent.astype(jnp.float32).reshape(row_total, model_width) * valid_mask.reshape(
        row_total, 1
    )
    unit = row_total // sum(MID_SPLIT)
    bounds = [0]
    for share in MID_SPLIT:
        bounds.append(bounds[-1] + share * unit)
    pieces = []
    for index in range(len(MID_SPLIT)):
        rows = slice(bounds[index], bounds[index + 1])
        pieces.append(
            middle_rows(
                attn_out[rows], tokens_wide[rows], grad_final[rows],
                output_full, gate_full, up_full, down_full, tp_count,
            )
        )
    grad_gate = sum(piece[6] for piece in pieces)
    grad_up = sum(piece[7] for piece in pieces)
    grad_down = sum(piece[8] for piece in pieces)
    last_sum = pieces[-1][5]
    (grad_gate, grad_up, grad_down), last_sum = lax.optimization_barrier(
        ((grad_gate, grad_up, grad_down), last_sum)
    )
    pieces[-1][5] = last_sum
    mlp_grads = (
        scatter_low(grad_gate, 0),
        scatter_low(grad_up, 0),
        scatter_low(grad_down, 1),
    )
    resid = jnp.concatenate([piece[0] for piece in pieces], axis=0)
    branch_two_part = jnp.concatenate([piece[1] for piece in pieces], axis=0)
    grad_resid_parts = [
        piece[4]
        + norm_back(piece[2], piece[3], piece[5].astype(jnp.float32))
        for piece in pieces
    ]
    grad_resid = jnp.concatenate(grad_resid_parts, axis=0)
    grad_resid_low = grad_resid.astype(bf_type)
    grad_wout = jnp.einsum(
        "rc,rd->cd", attn_out, grad_resid_low, preferred_element_type=jnp.float32
    )
    grad_attn = jnp.einsum(
        "rd,cd->rc", grad_resid_low, output_full, preferred_element_type=jnp.float32
    )
    grad_attn = grad_attn.astype(bf_type).reshape(split_heads)
    branch_two_part, grad_attn = lax.optimization_barrier((branch_two_part, grad_attn))
    final_sum = resid + tp_psum(branch_two_part, tp_count).astype(jnp.float32)
    seq_index = 0
    grad_queries, grad_keys_seq, grad_values_seq = attend_backward(
        queries[seq_index],
        keys_all[seq_index],
        values_all[seq_index],
        lengths[seq_index],
        offset,
        log_list[seq_index],
        grad_attn[seq_index],
    )
    query_grads = [grad_queries]
    key_grads = [grad_keys_seq]
    value_grads = [grad_values_seq]
    grad_keys, grad_values = (
        exchange_scatter(
            jnp.stack(key_grads).reshape((ctx_count, half_len, head_count, HEAD_DIM)), CTX, ctx_count
        ).reshape(split_heads),
        exchange_scatter(
            jnp.stack(value_grads).reshape((ctx_count, half_len, head_count, HEAD_DIM)), CTX, ctx_count
        ).reshape(split_heads),
    )
    grad_q_pre = (
        rotate_back(jnp.stack(query_grads), cosine, sine_table)
        .astype(bf_type)
        .reshape(row_total, head_cols)
    )
    grad_k_pre = (
        rotate_back(grad_keys, cosine, sine_table).astype(bf_type).reshape(row_total, head_cols)
    )
    grad_v_pre = grad_values.astype(bf_type).reshape(row_total, head_cols)
    grad_wq = jnp.einsum("rd,rc->dc", input_one, grad_q_pre, preferred_element_type=jnp.float32)
    grad_wk = jnp.einsum("rd,rc->dc", input_one, grad_k_pre, preferred_element_type=jnp.float32)
    grad_wv = jnp.einsum("rd,rc->dc", input_one, grad_v_pre, preferred_element_type=jnp.float32)
    grad_input_one = (
        jnp.einsum("rc,dc->rd", grad_q_pre, query_full, preferred_element_type=jnp.float32)
        + jnp.einsum("rc,dc->rd", grad_k_pre, key_full, preferred_element_type=jnp.float32)
        + jnp.einsum("rc,dc->rd", grad_v_pre, value_full, preferred_element_type=jnp.float32)
    )
    qkv_grads = jnp.split(
        scatter_low(jnp.concatenate([grad_wq, grad_wk, grad_wv], axis=1), 0), 3, axis=1
    )
    attn_grads = (qkv_grads[0], qkv_grads[1], qkv_grads[2], scatter_low(grad_wout, 1))
    grad_input_one = tp_psum(grad_input_one, tp_count).astype(jnp.float32)
    grad_tokens = grad_resid + norm_back(normed_one, scale_one, grad_input_one)
    output = final_sum.astype(bf_type).reshape(seq_count, half_len, model_width)
    grad_tokens = grad_tokens.reshape(seq_count, half_len, model_width)
    return (
        output,
        grad_tokens,
        attn_grads[0],
        attn_grads[1],
        attn_grads[2],
        attn_grads[3],
        mlp_grads[0],
        mlp_grads[1],
        mlp_grads[2],
    )


def solution(mesh):
    return jax.shard_map(
        functools.partial(body, mesh.shape[TP], mesh.shape[CTX]),
        mesh=mesh,
        in_specs=(
            P(SHARD, CTX, None),
            P(SHARD),
            P(SHARD, CTX, None),
            P((SHARD, CTX), TP),
            P((SHARD, CTX), TP),
            P((SHARD, CTX), TP),
            P(TP, (SHARD, CTX)),
            P((SHARD, CTX), TP),
            P((SHARD, CTX), TP),
            P(TP, (SHARD, CTX)),
        ),
        out_specs=(
            P(SHARD, CTX, None),
            P(SHARD, CTX, None),
            P((SHARD, CTX), TP),
            P((SHARD, CTX), TP),
            P((SHARD, CTX), TP),
            P(TP, (SHARD, CTX)),
            P((SHARD, CTX), TP),
            P((SHARD, CTX), TP),
            P(TP, (SHARD, CTX)),
        ),
        check_vma=False,
    )
```

```python
import functools

import jax
import jax.numpy as jnp
from jax import lax
from jax.sharding import PartitionSpec as P

SHARD, CTX, TP = "shard", "ctx", "tp"

HEAD_DIM = 128


EPSILON = 1e-05


def normalize(values):
    center = values - jnp.mean(values, axis=-1, keepdims=True)
    inv_scale = lax.rsqrt(jnp.mean(center * center, axis=-1, keepdims=True) + EPSILON)
    return (center * inv_scale, inv_scale)


def norm_back(normed, inv_scale, upstream):
    first_mean = jnp.mean(upstream, axis=-1, keepdims=True)
    second_mean = jnp.mean(upstream * normed, axis=-1, keepdims=True)
    return inv_scale * (upstream - first_mean - normed * second_mean)


def rope_tables(row_count, head_size, offset):
    positions = (jnp.arange(row_count) + offset).astype(jnp.float32)
    inverse = 10000.0 ** (-(jnp.arange(head_size // 2).astype(jnp.float32) * 2.0) / head_size)
    angles = positions[:, None] * inverse[None, :]
    angles = jnp.concatenate([angles, angles], axis=-1)
    return (jnp.cos(angles)[:, None, :], jnp.sin(angles)[:, None, :])


def turn_half(values):
    half_dim = values.shape[-1] // 2
    return jnp.concatenate([-values[..., half_dim:], values[..., :half_dim]], axis=-1)


def rotate(values, cosine, sine_table):
    return values * cosine + turn_half(values) * sine_table


def rotate_back(values, cosine, sine_table):
    return values * cosine - turn_half(values) * sine_table


def score_block(query_rows, keys_seq, length, row_start):
    block_rows = query_rows.shape[0]
    key_pos = jnp.arange(keys_seq.shape[0])
    row_pos = row_start + jnp.arange(block_rows)
    scores = jnp.einsum(
        "qhd,khd->hqk", query_rows, keys_seq, preferred_element_type=jnp.float32
    ) * HEAD_DIM ** (-0.5)
    allowed = (key_pos[None, :] <= row_pos[:, None]) & (key_pos[None, :] < length)
    return jnp.where(allowed[None], scores, -1e30)


def attend_forward(queries_seq, keys_seq, values_seq, length, offset):
    half_len, head_count, head_size = queries_seq.shape
    block_rows = min(512, half_len)
    block_count = half_len // block_rows
    grouped = queries_seq.reshape(block_count, block_rows, head_count, head_size)

    def one_block(paired):
        query_rows, block_index = paired
        scores = score_block(query_rows, keys_seq, length, offset + block_index * block_rows)
        row_peak = jnp.max(scores, axis=-1, keepdims=True)
        log_total = jnp.log(jnp.sum(jnp.exp(scores - row_peak), axis=-1, keepdims=True)) + row_peak
        probability = jnp.exp(scores - log_total).astype(jnp.bfloat16)
        attended = jnp.einsum(
            "hqk,khd->qhd", probability, values_seq, preferred_element_type=jnp.float32
        )
        return (attended.astype(jnp.bfloat16), log_total[..., 0])

    attended, log_totals = lax.map(one_block, (grouped, jnp.arange(block_count)))
    return (attended.reshape(half_len, head_count, head_size), log_totals)


def attend_backward(queries_seq, keys_seq, values_seq, length, offset, log_totals, grad_seq):
    half_len, head_count, head_size = queries_seq.shape
    block_rows = min(512, half_len)
    block_count = half_len // block_rows
    score_scale = HEAD_DIM ** (-0.5)
    grouped = queries_seq.reshape(block_count, block_rows, head_count, head_size)
    grad_grouped = grad_seq.reshape(block_count, block_rows, head_count, head_size)

    def one_block(carried, paired):
        query_rows, grad_rows, log_rows, block_index = paired
        scores = score_block(query_rows, keys_seq, length, offset + block_index * block_rows)
        probability = jnp.exp(scores - log_rows[..., None])
        prob_low = probability.astype(jnp.bfloat16)
        grad_prob = jnp.einsum(
            "qhd,khd->hqk", grad_rows, values_seq, preferred_element_type=jnp.float32
        )
        inner_sum = jnp.sum(probability * grad_prob, axis=-1, keepdims=True)
        grad_scores = (probability * (grad_prob - inner_sum)).astype(jnp.bfloat16)
        grad_query_rows = (
            jnp.einsum("hqk,khd->qhd", grad_scores, keys_seq, preferred_element_type=jnp.float32)
            * score_scale
        )
        key_part = (
            jnp.einsum("hqk,qhd->khd", grad_scores, query_rows, preferred_element_type=jnp.float32)
            * score_scale
        )
        value_part = jnp.einsum(
            "hqk,qhd->khd", prob_low, grad_rows, preferred_element_type=jnp.float32
        )
        return ((carried[0] + key_part, carried[1] + value_part), grad_query_rows)

    empty = jnp.zeros(keys_seq.shape, jnp.float32)
    sums, grad_queries = lax.scan(
        one_block, (empty, empty), (grouped, grad_grouped, log_totals, jnp.arange(block_count))
    )
    return (grad_queries.reshape(half_len, head_count, head_size), sums[0], sums[1])


def tp_psum(part, count):
    me = lax.axis_index(TP)
    low_part = part.astype(jnp.bfloat16)
    rows = part.shape[0] // count
    chunks = low_part.reshape((count, rows) + part.shape[1:])
    total = lax.dynamic_index_in_dim(chunks, me, 0, keepdims=False).astype(jnp.float32)
    for shift in range(1, count):
        pairs = [(i, (i + shift) % count) for i in range(count)]
        piece = lax.dynamic_index_in_dim(chunks, (me + shift) % count, 0, keepdims=False)
        total = total + lax.ppermute(piece, TP, pairs).astype(jnp.float32)
    reduced = total.astype(jnp.bfloat16)
    gathered = jnp.zeros(low_part.shape, jnp.bfloat16)
    gathered = lax.dynamic_update_slice_in_dim(gathered, reduced, me * rows, 0)
    for shift in range(1, count):
        pairs = [(i, (i + shift) % count) for i in range(count)]
        got = lax.ppermute(reduced, TP, pairs)
        gathered = lax.dynamic_update_slice_in_dim(
            gathered, got, ((me + count - shift) % count) * rows, 0
        )
    return gathered


def exchange_gather(piece, axis, count):
    me = lax.axis_index(axis)
    gathered = jnp.zeros((count,) + piece.shape, piece.dtype)
    gathered = lax.dynamic_update_index_in_dim(gathered, piece, me, 0)
    for shift in range(1, count):
        pairs = [(i, (i + shift) % count) for i in range(count)]
        got = lax.ppermute(piece, axis, pairs)
        gathered = lax.dynamic_update_index_in_dim(gathered, got, (me + count - shift) % count, 0)
    return gathered


def exchange_scatter(blocks, axis, count):
    me = lax.axis_index(axis)
    total = lax.dynamic_index_in_dim(blocks, me, 0, keepdims=False)
    for shift in range(1, count):
        pairs = [(i, (i + shift) % count) for i in range(count)]
        piece = lax.dynamic_index_in_dim(blocks, (me + shift) % count, 0, keepdims=False)
        total = total + lax.ppermute(piece, axis, pairs)
    return total


def scatter_low(grad, dim):
    summed = lax.psum_scatter(
        grad.astype(jnp.bfloat16), (SHARD, CTX), scatter_dimension=dim, tiled=True
    )
    return summed.astype(jnp.float32)


def matmul_low(left, right):
    return jnp.dot(left, right, preferred_element_type=jnp.float32)


MID_SPLIT = (3, 5)


def middle_rows(attn_rows, tokens_rows, grad_final, output_full, gate_full, up_full, down_full, tp_count):
    bf_type = jnp.bfloat16
    resid = tokens_rows + tp_psum(matmul_low(attn_rows, output_full), tp_count).astype(jnp.float32)
    normed_two, scale_two = normalize(resid)
    input_two = normed_two.astype(bf_type)
    gate_proj = matmul_low(input_two, gate_full)
    up_proj = matmul_low(input_two, up_full)
    gate_sigmoid = jax.nn.sigmoid(gate_proj)
    hidden = (gate_proj * gate_sigmoid * up_proj).astype(bf_type)
    grad_branch = grad_final.astype(bf_type)
    grad_hidden = jnp.einsum(
        "rd,fd->rf", grad_branch, down_full, preferred_element_type=jnp.float32
    )
    grad_gate_act = (
        grad_hidden * up_proj * gate_sigmoid * (1.0 + gate_proj * (1.0 - gate_sigmoid))
    ).astype(bf_type)
    grad_up_act = (grad_hidden * gate_proj * gate_sigmoid).astype(bf_type)
    grad_input_two = jnp.einsum(
        "rf,df->rd", grad_gate_act, gate_full, preferred_element_type=jnp.float32
    ) + jnp.einsum("rf,df->rd", grad_up_act, up_full, preferred_element_type=jnp.float32)
    branch_two = matmul_low(hidden, down_full)
    grad_down = jnp.einsum("rf,rd->fd", hidden, grad_branch, preferred_element_type=jnp.float32)
    grad_gate = jnp.einsum(
        "rd,rf->df", input_two, grad_gate_act, preferred_element_type=jnp.float32
    )
    grad_up = jnp.einsum("rd,rf->df", input_two, grad_up_act, preferred_element_type=jnp.float32)
    grad_input_two = tp_psum(grad_input_two, tp_count)
    return [
        resid, branch_two, normed_two, scale_two, grad_final, grad_input_two,
        grad_gate, grad_up, grad_down,
    ]


def body(tp_count, ctx_count, *args):
    return block(tp_count, ctx_count, *args)


def block(tp_count, ctx_count, tokens, lengths, cotangent, w_query, w_key, w_value, w_output, w_gate, w_up, w_down):
    seq_count, half_len, model_width = tokens.shape
    head_cols = w_query.shape[1]
    head_count = head_cols // HEAD_DIM
    row_total = seq_count * half_len
    offset = lax.axis_index(CTX) * half_len
    positions = offset + jnp.arange(half_len)
    valid_mask = (positions[None, :] < lengths[:, None]).astype(jnp.float32)
    bf_type = jnp.bfloat16
    attn_low = (
        w_query.astype(bf_type),
        w_key.astype(bf_type),
        w_value.astype(bf_type),
        w_output.astype(bf_type),
    )
    mlp_low = (w_gate.astype(bf_type), w_up.astype(bf_type), w_down.astype(bf_type))
    attn_joined = lax.all_gather(
        jnp.concatenate([attn_low[0], attn_low[1], attn_low[2], attn_low[3].T], axis=1),
        (SHARD, CTX),
        axis=0,
        tiled=True,
    )
    query_full, key_full, value_full, output_t = jnp.split(attn_joined, 4, axis=1)
    output_full = output_t.T
    gate_full, up_full, down_full = (
        lax.all_gather(mlp_low[0], (SHARD, CTX), axis=0, tiled=True),
        lax.all_gather(mlp_low[1], (SHARD, CTX), axis=0, tiled=True),
        lax.all_gather(mlp_low[2], (SHARD, CTX), axis=1, tiled=True),
    )
    tokens_wide = tokens.astype(jnp.float32).reshape(row_total, model_width)
    normed_one, scale_one = normalize(tokens_wide)
    input_one = normed_one.astype(bf_type)
    split_heads = (seq_count, half_len, head_count, HEAD_DIM)
    query_pre = matmul_low(input_one, query_full).reshape(split_heads)
    key_pre = matmul_low(input_one, key_full).reshape(split_heads)
    value_pre = matmul_low(input_one, value_full).reshape(split_heads)
    cosine, sine_table = rope_tables(half_len, HEAD_DIM, offset)
    queries = rotate(query_pre, cosine, sine_table).astype(bf_type)
    keys_rot = rotate(key_pre, cosine, sine_table).astype(bf_type)
    values_low = value_pre.astype(bf_type)
    keys_all, values_all = (
        jnp.swapaxes(exchange_gather(keys_rot, CTX, ctx_count), 0, 1).reshape(
            (seq_count, ctx_count * half_len, head_count, HEAD_DIM)
        ),
        jnp.swapaxes(exchange_gather(values_low, CTX, ctx_count), 0, 1).reshape(
            (seq_count, ctx_count * half_len, head_count, HEAD_DIM)
        ),
    )
    seq_index = 0
    attended, log_totals = attend_forward(
        queries[seq_index], keys_all[seq_index], values_all[seq_index], lengths[seq_index], offset
    )
    attended_list = [attended]
    log_list = [log_totals]
    attn_out = jnp.stack(attended_list).reshape(row_total, head_cols)
    grad_final = cotangent.astype(jnp.float32).reshape(row_total, model_width) * valid_mask.reshape(
        row_total, 1
    )
    unit = row_total // sum(MID_SPLIT)
    bounds = [0]
    for share in MID_SPLIT:
        bounds.append(bounds[-1] + share * unit)
    pieces = []
    for index in range(len(MID_SPLIT)):
        rows = slice(bounds[index], bounds[index + 1])
        pieces.append(
            middle_rows(
                attn_out[rows], tokens_wide[rows], grad_final[rows],
                output_full, gate_full, up_full, down_full, tp_count,
            )
        )
    grad_gate = sum(piece[6] for piece in pieces)
    grad_up = sum(piece[7] for piece in pieces)
    grad_down = sum(piece[8] for piece in pieces)
    last_sum = pieces[-1][5]
    (grad_gate, grad_up, grad_down), last_sum = lax.optimization_barrier(
        ((grad_gate, grad_up, grad_down), last_sum)
    )
    pieces[-1][5] = last_sum
    mlp_grads = (
        scatter_low(grad_gate, 0),
        scatter_low(grad_up, 0),
        scatter_low(grad_down, 1),
    )
    resid = jnp.concatenate([piece[0] for piece in pieces], axis=0)
    branch_two_part = jnp.concatenate([piece[1] for piece in pieces], axis=0)
    grad_resid_parts, grad_attn_parts, grad_wout = [], [], 0.0
    for index, piece in enumerate(pieces):
        grad_resid_part = piece[4] + norm_back(piece[2], piece[3], piece[5].astype(jnp.float32))
        resid_low = grad_resid_part.astype(bf_type)
        grad_wout = grad_wout + jnp.einsum(
            "rc,rd->cd", attn_out[bounds[index]:bounds[index + 1]], resid_low,
            preferred_element_type=jnp.float32,
        )
        grad_attn_parts.append(
            jnp.einsum("rd,cd->rc", resid_low, output_full, preferred_element_type=jnp.float32)
        )
        grad_resid_parts.append(grad_resid_part)
    grad_resid = jnp.concatenate(grad_resid_parts, axis=0)
    grad_attn = jnp.concatenate(grad_attn_parts, axis=0).astype(bf_type).reshape(split_heads)
    branch_two_part, grad_attn = lax.optimization_barrier((branch_two_part, grad_attn))
    final_sum = resid + tp_psum(branch_two_part, tp_count).astype(jnp.float32)
    seq_index = 0
    grad_queries, grad_keys_seq, grad_values_seq = attend_backward(
        queries[seq_index],
        keys_all[seq_index],
        values_all[seq_index],
        lengths[seq_index],
        offset,
        log_list[seq_index],
        grad_attn[seq_index],
    )
    query_grads = [grad_queries]
    key_grads = [grad_keys_seq]
    value_grads = [grad_values_seq]
    grad_keys, grad_values = (
        exchange_scatter(
            jnp.stack(key_grads).reshape((ctx_count, half_len, head_count, HEAD_DIM)), CTX, ctx_count
        ).reshape(split_heads),
        exchange_scatter(
            jnp.stack(value_grads).reshape((ctx_count, half_len, head_count, HEAD_DIM)), CTX, ctx_count
        ).reshape(split_heads),
    )
    grad_q_pre = (
        rotate_back(jnp.stack(query_grads), cosine, sine_table)
        .astype(bf_type)
        .reshape(row_total, head_cols)
    )
    grad_k_pre = (
        rotate_back(grad_keys, cosine, sine_table).astype(bf_type).reshape(row_total, head_cols)
    )
    grad_v_pre = grad_values.astype(bf_type).reshape(row_total, head_cols)
    grad_wq = jnp.einsum("rd,rc->dc", input_one, grad_q_pre, preferred_element_type=jnp.float32)
    grad_wk = jnp.einsum("rd,rc->dc", input_one, grad_k_pre, preferred_element_type=jnp.float32)
    grad_wv = jnp.einsum("rd,rc->dc", input_one, grad_v_pre, preferred_element_type=jnp.float32)
    grad_input_one = (
        jnp.einsum("rc,dc->rd", grad_q_pre, query_full, preferred_element_type=jnp.float32)
        + jnp.einsum("rc,dc->rd", grad_k_pre, key_full, preferred_element_type=jnp.float32)
        + jnp.einsum("rc,dc->rd", grad_v_pre, value_full, preferred_element_type=jnp.float32)
    )
    qkv_grads = jnp.split(
        scatter_low(jnp.concatenate([grad_wq, grad_wk, grad_wv], axis=1), 0), 3, axis=1
    )
    attn_grads = (qkv_grads[0], qkv_grads[1], qkv_grads[2], scatter_low(grad_wout, 1))
    grad_input_one = tp_psum(grad_input_one, tp_count).astype(jnp.float32)
    grad_tokens = grad_resid + norm_back(normed_one, scale_one, grad_input_one)
    output = final_sum.astype(bf_type).reshape(seq_count, half_len, model_width)
    grad_tokens = grad_tokens.reshape(seq_count, half_len, model_width)
    return (
        output,
        grad_tokens,
        attn_grads[0],
        attn_grads[1],
        attn_grads[2],
        attn_grads[3],
        mlp_grads[0],
        mlp_grads[1],
        mlp_grads[2],
    )


def solution(mesh):
    return jax.shard_map(
        functools.partial(body, mesh.shape[TP], mesh.shape[CTX]),
        mesh=mesh,
        in_specs=(
            P(SHARD, CTX, None),
            P(SHARD),
            P(SHARD, CTX, None),
            P((SHARD, CTX), TP),
            P((SHARD, CTX), TP),
            P((SHARD, CTX), TP),
            P(TP, (SHARD, CTX)),
            P((SHARD, CTX), TP),
            P((SHARD, CTX), TP),
            P(TP, (SHARD, CTX)),
        ),
        out_specs=(
            P(SHARD, CTX, None),
            P(SHARD, CTX, None),
            P((SHARD, CTX), TP),
            P((SHARD, CTX), TP),
            P((SHARD, CTX), TP),
            P(TP, (SHARD, CTX)),
            P((SHARD, CTX), TP),
            P((SHARD, CTX), TP),
            P(TP, (SHARD, CTX)),
        ),
        check_vma=False,
    )
```

```python
import functools

import jax
import jax.numpy as jnp
from jax import lax
from jax.sharding import PartitionSpec as P

SHARD, CTX, TP = "shard", "ctx", "tp"

HEAD_DIM = 128


EPSILON = 1e-05


def normalize(values):
    center = values - jnp.mean(values, axis=-1, keepdims=True)
    inv_scale = lax.rsqrt(jnp.mean(center * center, axis=-1, keepdims=True) + EPSILON)
    return (center * inv_scale, inv_scale)


def norm_back(normed, inv_scale, upstream):
    first_mean = jnp.mean(upstream, axis=-1, keepdims=True)
    second_mean = jnp.mean(upstream * normed, axis=-1, keepdims=True)
    return inv_scale * (upstream - first_mean - normed * second_mean)


def rope_tables(row_count, head_size, offset):
    positions = (jnp.arange(row_count) + offset).astype(jnp.float32)
    inverse = 10000.0 ** (-(jnp.arange(head_size // 2).astype(jnp.float32) * 2.0) / head_size)
    angles = positions[:, None] * inverse[None, :]
    angles = jnp.concatenate([angles, angles], axis=-1)
    return (jnp.cos(angles)[:, None, :], jnp.sin(angles)[:, None, :])


def turn_half(values):
    half_dim = values.shape[-1] // 2
    return jnp.concatenate([-values[..., half_dim:], values[..., :half_dim]], axis=-1)


def rotate(values, cosine, sine_table):
    return values * cosine + turn_half(values) * sine_table


def rotate_back(values, cosine, sine_table):
    return values * cosine - turn_half(values) * sine_table


def score_block(query_rows, keys_seq, length, row_start):
    block_rows = query_rows.shape[0]
    key_pos = jnp.arange(keys_seq.shape[0])
    row_pos = row_start + jnp.arange(block_rows)
    scores = jnp.einsum(
        "qhd,khd->hqk", query_rows, keys_seq, preferred_element_type=jnp.float32
    ) * HEAD_DIM ** (-0.5)
    allowed = (key_pos[None, :] <= row_pos[:, None]) & (key_pos[None, :] < length)
    return jnp.where(allowed[None], scores, -1e30)


def attend_forward(queries_seq, keys_seq, values_seq, length, offset):
    half_len, head_count, head_size = queries_seq.shape
    block_rows = min(512, half_len)
    block_count = half_len // block_rows
    grouped = queries_seq.reshape(block_count, block_rows, head_count, head_size)

    def one_block(paired):
        query_rows, block_index = paired
        scores = score_block(query_rows, keys_seq, length, offset + block_index * block_rows)
        row_peak = jnp.max(scores, axis=-1, keepdims=True)
        log_total = jnp.log(jnp.sum(jnp.exp(scores - row_peak), axis=-1, keepdims=True)) + row_peak
        probability = jnp.exp(scores - log_total).astype(jnp.bfloat16)
        attended = jnp.einsum(
            "hqk,khd->qhd", probability, values_seq, preferred_element_type=jnp.float32
        )
        return (attended.astype(jnp.bfloat16), log_total[..., 0])

    attended, log_totals = lax.map(one_block, (grouped, jnp.arange(block_count)))
    return (attended.reshape(half_len, head_count, head_size), log_totals)


def attend_backward(queries_seq, keys_seq, values_seq, length, offset, log_totals, grad_seq):
    half_len, head_count, head_size = queries_seq.shape
    block_rows = min(512, half_len)
    block_count = half_len // block_rows
    score_scale = HEAD_DIM ** (-0.5)
    grouped = queries_seq.reshape(block_count, block_rows, head_count, head_size)
    grad_grouped = grad_seq.reshape(block_count, block_rows, head_count, head_size)

    def one_block(carried, paired):
        query_rows, grad_rows, log_rows, block_index = paired
        scores = score_block(query_rows, keys_seq, length, offset + block_index * block_rows)
        probability = jnp.exp(scores - log_rows[..., None])
        prob_low = probability.astype(jnp.bfloat16)
        grad_prob = jnp.einsum(
            "qhd,khd->hqk", grad_rows, values_seq, preferred_element_type=jnp.float32
        )
        inner_sum = jnp.sum(probability * grad_prob, axis=-1, keepdims=True)
        grad_scores = (probability * (grad_prob - inner_sum)).astype(jnp.bfloat16)
        grad_query_rows = (
            jnp.einsum("hqk,khd->qhd", grad_scores, keys_seq, preferred_element_type=jnp.float32)
            * score_scale
        )
        key_part = (
            jnp.einsum("hqk,qhd->khd", grad_scores, query_rows, preferred_element_type=jnp.float32)
            * score_scale
        )
        value_part = jnp.einsum(
            "hqk,qhd->khd", prob_low, grad_rows, preferred_element_type=jnp.float32
        )
        return ((carried[0] + key_part, carried[1] + value_part), grad_query_rows)

    empty = jnp.zeros(keys_seq.shape, jnp.float32)
    sums, grad_queries = lax.scan(
        one_block, (empty, empty), (grouped, grad_grouped, log_totals, jnp.arange(block_count))
    )
    return (grad_queries.reshape(half_len, head_count, head_size), sums[0], sums[1])


def tp_psum(part, count):
    me = lax.axis_index(TP)
    low_part = part.astype(jnp.bfloat16)
    rows = part.shape[0] // count
    chunks = low_part.reshape((count, rows) + part.shape[1:])
    total = lax.dynamic_index_in_dim(chunks, me, 0, keepdims=False).astype(jnp.float32)
    for shift in range(1, count):
        pairs = [(i, (i + shift) % count) for i in range(count)]
        piece = lax.dynamic_index_in_dim(chunks, (me + shift) % count, 0, keepdims=False)
        total = total + lax.ppermute(piece, TP, pairs).astype(jnp.float32)
    reduced = total.astype(jnp.bfloat16)
    gathered = jnp.zeros(low_part.shape, jnp.bfloat16)
    gathered = lax.dynamic_update_slice_in_dim(gathered, reduced, me * rows, 0)
    for shift in range(1, count):
        pairs = [(i, (i + shift) % count) for i in range(count)]
        got = lax.ppermute(reduced, TP, pairs)
        gathered = lax.dynamic_update_slice_in_dim(
            gathered, got, ((me + count - shift) % count) * rows, 0
        )
    return gathered


def tp_psum_line(part, count, axis="tp"):
    me = lax.axis_index(axis)
    low_part = part.astype(jnp.bfloat16)
    rows = part.shape[0] // count
    chunks = low_part.reshape((count, rows) + part.shape[1:])

    def chunk_at(index):
        return lax.dynamic_index_in_dim(chunks, jnp.clip(index, 0, count - 1), 0, keepdims=False)

    from_left = jnp.zeros(chunks.shape[1:], jnp.bfloat16)
    from_right = jnp.zeros(chunks.shape[1:], jnp.bfloat16)
    for step in range(1, count):
      right_pairs = [(i, i + 1) for i in range(count - 1) if i <= step - 1]
      left_pairs = [(i, i - 1) for i in range(1, count) if i >= count - step]
      send_right = (chunk_at(me + count - step).astype(jnp.float32) + from_left.astype(jnp.float32))
      send_left = (chunk_at(me + step - count).astype(jnp.float32) + from_right.astype(jnp.float32))
      from_left = lax.ppermute(send_right.astype(jnp.bfloat16), axis, right_pairs)
      from_right = lax.ppermute(send_left.astype(jnp.bfloat16), axis, left_pairs)
    total = chunk_at(me).astype(jnp.float32) + from_left.astype(jnp.float32) + from_right.astype(jnp.float32)
    reduced = total.astype(jnp.bfloat16)
    gathered = jnp.zeros(chunks.shape, jnp.bfloat16)
    gathered = lax.dynamic_update_index_in_dim(gathered, reduced, me, 0)
    going_right = reduced
    going_left = reduced
    for step in range(1, count):
      right_pairs = [(i, i + 1) for i in range(count - 1) if i >= step - 1]
      left_pairs = [(i, i - 1) for i in range(1, count) if i <= count - step]
      going_right = lax.ppermute(going_right, axis, right_pairs)
      going_left = lax.ppermute(going_left, axis, left_pairs)
      for got, index in ((going_right, me - step), (going_left, me + step)):
          spot = jnp.clip(index, 0, count - 1)
          held = lax.dynamic_index_in_dim(gathered, spot, 0, keepdims=False)
          gathered = lax.dynamic_update_index_in_dim(gathered, held + got, spot, 0)
    return gathered.reshape(low_part.shape)


def exchange_gather(piece, axis, count):
    me = lax.axis_index(axis)
    gathered = jnp.zeros((count,) + piece.shape, piece.dtype)
    gathered = lax.dynamic_update_index_in_dim(gathered, piece, me, 0)
    for shift in range(1, count):
        pairs = [(i, (i + shift) % count) for i in range(count)]
        got = lax.ppermute(piece, axis, pairs)
        gathered = lax.dynamic_update_index_in_dim(gathered, got, (me + count - shift) % count, 0)
    return gathered


def exchange_scatter(blocks, axis, count):
    me = lax.axis_index(axis)
    total = lax.dynamic_index_in_dim(blocks, me, 0, keepdims=False)
    for shift in range(1, count):
        pairs = [(i, (i + shift) % count) for i in range(count)]
        piece = lax.dynamic_index_in_dim(blocks, (me + shift) % count, 0, keepdims=False)
        total = total + lax.ppermute(piece, axis, pairs)
    return total


def scatter_low(grad, dim):
    summed = lax.psum_scatter(
        grad.astype(jnp.bfloat16), (SHARD, CTX), scatter_dimension=dim, tiled=True
    )
    return summed.astype(jnp.float32)


def matmul_low(left, right):
    return jnp.dot(left, right, preferred_element_type=jnp.float32)


MID_SPLIT = (3, 5)


def middle_rows(attn_rows, tokens_rows, grad_final, output_full, gate_full, up_full, down_full, tp_count):
    bf_type = jnp.bfloat16
    resid = tokens_rows + tp_psum(matmul_low(attn_rows, output_full), tp_count).astype(jnp.float32)
    normed_two, scale_two = normalize(resid)
    input_two = normed_two.astype(bf_type)
    gate_proj = matmul_low(input_two, gate_full)
    up_proj = matmul_low(input_two, up_full)
    gate_sigmoid = jax.nn.sigmoid(gate_proj)
    hidden = (gate_proj * gate_sigmoid * up_proj).astype(bf_type)
    grad_branch = grad_final.astype(bf_type)
    grad_hidden = jnp.einsum(
        "rd,fd->rf", grad_branch, down_full, preferred_element_type=jnp.float32
    )
    grad_gate_act = (grad_hidden * up_proj * gate_sigmoid * (1.0 + gate_proj * (1.0 - gate_sigmoid))).astype(bf_type)
    grad_up_act = (grad_hidden * gate_proj * gate_sigmoid).astype(bf_type)
    grad_input_two = jnp.einsum(
        "rf,df->rd", grad_gate_act, gate_full, preferred_element_type=jnp.float32
    ) + jnp.einsum("rf,df->rd", grad_up_act, up_full, preferred_element_type=jnp.float32)
    branch_two = matmul_low(hidden, down_full)
    grad_down = jnp.einsum("rf,rd->fd", hidden, grad_branch, preferred_element_type=jnp.float32)
    grad_gate = jnp.einsum(
        "rd,rf->df", input_two, grad_gate_act, preferred_element_type=jnp.float32
    )
    grad_up = jnp.einsum("rd,rf->df", input_two, grad_up_act, preferred_element_type=jnp.float32)
    grad_input_two = tp_psum(grad_input_two, tp_count)
    return [
        resid, branch_two, normed_two, scale_two, grad_final, grad_input_two,
        grad_gate, grad_up, grad_down,
    ]


def body(tp_count, ctx_count, *args):
    return block(tp_count, ctx_count, *args)


def block(tp_count, ctx_count, tokens, lengths, cotangent, w_query, w_key, w_value, w_output, w_gate, w_up, w_down):
    seq_count, half_len, model_width = tokens.shape
    head_cols = w_query.shape[1]
    head_count = head_cols // HEAD_DIM
    row_total = seq_count * half_len
    offset = lax.axis_index(CTX) * half_len
    positions = offset + jnp.arange(half_len)
    valid_mask = (positions[None, :] < lengths[:, None]).astype(jnp.float32)
    bf_type = jnp.bfloat16
    attn_low = (
        w_query.astype(bf_type),
        w_key.astype(bf_type),
        w_value.astype(bf_type),
        w_output.astype(bf_type),
    )
    mlp_low = (w_gate.astype(bf_type), w_up.astype(bf_type), w_down.astype(bf_type))
    attn_joined = lax.all_gather(
        jnp.concatenate([attn_low[0], attn_low[1], attn_low[2], attn_low[3].T], axis=1),
        (SHARD, CTX),
        axis=0,
        tiled=True,
    )
    query_full, key_full, value_full, output_t = jnp.split(attn_joined, 4, axis=1)
    output_full = output_t.T
    gate_full, up_full, down_full = (
        lax.all_gather(mlp_low[0], (SHARD, CTX), axis=0, tiled=True),
        lax.all_gather(mlp_low[1], (SHARD, CTX), axis=0, tiled=True),
        lax.all_gather(mlp_low[2], (SHARD, CTX), axis=1, tiled=True),
    )
    tokens_wide = tokens.astype(jnp.float32).reshape(row_total, model_width)
    normed_one, scale_one = normalize(tokens_wide)
    input_one = normed_one.astype(bf_type)
    split_heads = (seq_count, half_len, head_count, HEAD_DIM)
    query_pre = matmul_low(input_one, query_full).reshape(split_heads)
    key_pre = matmul_low(input_one, key_full).reshape(split_heads)
    value_pre = matmul_low(input_one, value_full).reshape(split_heads)
    cosine, sine_table = rope_tables(half_len, HEAD_DIM, offset)
    queries = rotate(query_pre, cosine, sine_table).astype(bf_type)
    keys_rot = rotate(key_pre, cosine, sine_table).astype(bf_type)
    values_low = value_pre.astype(bf_type)
    keys_all, values_all = (
        jnp.swapaxes(exchange_gather(keys_rot, CTX, ctx_count), 0, 1).reshape(
            (seq_count, ctx_count * half_len, head_count, HEAD_DIM)
        ),
        jnp.swapaxes(exchange_gather(values_low, CTX, ctx_count), 0, 1).reshape(
            (seq_count, ctx_count * half_len, head_count, HEAD_DIM)
        ),
    )
    seq_index = 0
    attended, log_totals = attend_forward(
        queries[seq_index], keys_all[seq_index], values_all[seq_index], lengths[seq_index], offset
    )
    attended_list = [attended]
    log_list = [log_totals]
    attn_out = jnp.stack(attended_list).reshape(row_total, head_cols)
    grad_final = cotangent.astype(jnp.float32).reshape(row_total, model_width) * valid_mask.reshape(
        row_total, 1
    )
    unit = row_total // sum(MID_SPLIT)
    bounds = [0]
    for share in MID_SPLIT:
        bounds.append(bounds[-1] + share * unit)
    pieces = []
    for index in range(len(MID_SPLIT)):
        rows = slice(bounds[index], bounds[index + 1])
        pieces.append(
            middle_rows(
                attn_out[rows], tokens_wide[rows], grad_final[rows],
                output_full, gate_full, up_full, down_full, tp_count,
            )
        )
    grad_gate = sum(piece[6] for piece in pieces)
    grad_up = sum(piece[7] for piece in pieces)
    grad_down = sum(piece[8] for piece in pieces)
    last_sum = pieces[-1][5]
    (grad_gate, grad_up, grad_down), last_sum = lax.optimization_barrier(
        ((grad_gate, grad_up, grad_down), last_sum)
    )
    pieces[-1][5] = last_sum
    mlp_grads = (
        scatter_low(grad_gate, 0),
        scatter_low(grad_up, 0),
        scatter_low(grad_down, 1),
    )
    resid = jnp.concatenate([piece[0] for piece in pieces], axis=0)
    branch_two_part = jnp.concatenate([piece[1] for piece in pieces], axis=0)
    grad_resid_parts, grad_attn_parts, grad_wout = [], [], 0.0
    for index, piece in enumerate(pieces):
        grad_resid_part = piece[4] + norm_back(piece[2], piece[3], piece[5].astype(jnp.float32))
        resid_low = grad_resid_part.astype(bf_type)
        grad_wout = grad_wout + jnp.einsum(
            "rc,rd->cd", attn_out[bounds[index]:bounds[index + 1]], resid_low,
            preferred_element_type=jnp.float32,
        )
        grad_attn_parts.append(
            jnp.einsum("rd,cd->rc", resid_low, output_full, preferred_element_type=jnp.float32)
        )
        grad_resid_parts.append(grad_resid_part)
    grad_resid = jnp.concatenate(grad_resid_parts, axis=0)
    grad_attn = jnp.concatenate(grad_attn_parts, axis=0).astype(bf_type).reshape(split_heads)
    branch_two_part, grad_attn = lax.optimization_barrier((branch_two_part, grad_attn))
    final_sum = resid + tp_psum(branch_two_part, tp_count).astype(jnp.float32)
    seq_index = 0
    grad_queries, grad_keys_seq, grad_values_seq = attend_backward(
        queries[seq_index],
        keys_all[seq_index],
        values_all[seq_index],
        lengths[seq_index],
        offset,
        log_list[seq_index],
        grad_attn[seq_index],
    )
    query_grads = [grad_queries]
    key_grads = [grad_keys_seq]
    value_grads = [grad_values_seq]
    grad_keys, grad_values = (
        exchange_scatter(
            jnp.stack(key_grads).reshape((ctx_count, half_len, head_count, HEAD_DIM)), CTX, ctx_count
        ).reshape(split_heads),
        exchange_scatter(
            jnp.stack(value_grads).reshape((ctx_count, half_len, head_count, HEAD_DIM)), CTX, ctx_count
        ).reshape(split_heads),
    )
    grad_q_pre = (
        rotate_back(jnp.stack(query_grads), cosine, sine_table)
        .astype(bf_type)
        .reshape(row_total, head_cols)
    )
    grad_k_pre = (
        rotate_back(grad_keys, cosine, sine_table).astype(bf_type).reshape(row_total, head_cols)
    )
    grad_v_pre = grad_values.astype(bf_type).reshape(row_total, head_cols)
    grad_wq = jnp.einsum("rd,rc->dc", input_one, grad_q_pre, preferred_element_type=jnp.float32)
    grad_wk = jnp.einsum("rd,rc->dc", input_one, grad_k_pre, preferred_element_type=jnp.float32)
    grad_wv = jnp.einsum("rd,rc->dc", input_one, grad_v_pre, preferred_element_type=jnp.float32)
    grad_input_one = (
        jnp.einsum("rc,dc->rd", grad_q_pre, query_full, preferred_element_type=jnp.float32)
        + jnp.einsum("rc,dc->rd", grad_k_pre, key_full, preferred_element_type=jnp.float32)
        + jnp.einsum("rc,dc->rd", grad_v_pre, value_full, preferred_element_type=jnp.float32)
    )
    qkv_grads = jnp.split(
        scatter_low(jnp.concatenate([grad_wq, grad_wk, grad_wv], axis=1), 0), 3, axis=1
    )
    attn_grads = (qkv_grads[0], qkv_grads[1], qkv_grads[2], scatter_low(grad_wout, 1))
    grad_input_one = tp_psum_line(grad_input_one, tp_count).astype(jnp.float32)
    grad_tokens = grad_resid + norm_back(normed_one, scale_one, grad_input_one)
    output = final_sum.astype(bf_type).reshape(seq_count, half_len, model_width)
    grad_tokens = grad_tokens.reshape(seq_count, half_len, model_width)
    return (
        output,
        grad_tokens,
        attn_grads[0],
        attn_grads[1],
        attn_grads[2],
        attn_grads[3],
        mlp_grads[0],
        mlp_grads[1],
        mlp_grads[2],
    )


def solution(mesh):
    return jax.shard_map(
        functools.partial(body, mesh.shape[TP], mesh.shape[CTX]),
        mesh=mesh,
        in_specs=(
            P(SHARD, CTX, None),
            P(SHARD),
            P(SHARD, CTX, None),
            P((SHARD, CTX), TP),
            P((SHARD, CTX), TP),
            P((SHARD, CTX), TP),
            P(TP, (SHARD, CTX)),
            P((SHARD, CTX), TP),
            P((SHARD, CTX), TP),
            P(TP, (SHARD, CTX)),
        ),
        out_specs=(
            P(SHARD, CTX, None),
            P(SHARD, CTX, None),
            P((SHARD, CTX), TP),
            P((SHARD, CTX), TP),
            P((SHARD, CTX), TP),
            P(TP, (SHARD, CTX)),
            P((SHARD, CTX), TP),
            P((SHARD, CTX), TP),
            P(TP, (SHARD, CTX)),
        ),
        check_vma=False,
    )
```

```python
import functools

import jax
import jax.numpy as jnp
from jax import lax
from jax.sharding import PartitionSpec as P

SHARD, CTX, TP = "shard", "ctx", "tp"

HEAD_DIM = 128


EPSILON = 1e-05


def normalize(values):
    center = values - jnp.mean(values, axis=-1, keepdims=True)
    inv_scale = lax.rsqrt(jnp.mean(center * center, axis=-1, keepdims=True) + EPSILON)
    return (center * inv_scale, inv_scale)


def norm_back(normed, inv_scale, upstream):
    first_mean = jnp.mean(upstream, axis=-1, keepdims=True)
    second_mean = jnp.mean(upstream * normed, axis=-1, keepdims=True)
    return inv_scale * (upstream - first_mean - normed * second_mean)


def rope_tables(row_count, head_size, offset):
    positions = (jnp.arange(row_count) + offset).astype(jnp.float32)
    inverse = 10000.0 ** (-(jnp.arange(head_size // 2).astype(jnp.float32) * 2.0) / head_size)
    angles = positions[:, None] * inverse[None, :]
    angles = jnp.concatenate([angles, angles], axis=-1)
    return (jnp.cos(angles)[:, None, :], jnp.sin(angles)[:, None, :])


def turn_half(values):
    half_dim = values.shape[-1] // 2
    return jnp.concatenate([-values[..., half_dim:], values[..., :half_dim]], axis=-1)


def rotate(values, cosine, sine_table):
    return values * cosine + turn_half(values) * sine_table


def rotate_back(values, cosine, sine_table):
    return values * cosine - turn_half(values) * sine_table


def score_block(query_rows, keys_seq, length, row_start):
    block_rows = query_rows.shape[0]
    key_pos = jnp.arange(keys_seq.shape[0])
    row_pos = row_start + jnp.arange(block_rows)
    scores = jnp.einsum(
        "qhd,khd->hqk", query_rows, keys_seq, preferred_element_type=jnp.float32
    ) * HEAD_DIM ** (-0.5)
    allowed = (key_pos[None, :] <= row_pos[:, None]) & (key_pos[None, :] < length)
    return jnp.where(allowed[None], scores, -1e30)


def attend_forward(queries_seq, keys_seq, values_seq, length, offset):
    half_len, head_count, head_size = queries_seq.shape
    block_rows = min(512, half_len)
    block_count = half_len // block_rows
    grouped = queries_seq.reshape(block_count, block_rows, head_count, head_size)

    def one_block(paired):
        query_rows, block_index = paired
        scores = score_block(query_rows, keys_seq, length, offset + block_index * block_rows)
        row_peak = jnp.max(scores, axis=-1, keepdims=True)
        log_total = jnp.log(jnp.sum(jnp.exp(scores - row_peak), axis=-1, keepdims=True)) + row_peak
        probability = jnp.exp(scores - log_total).astype(jnp.bfloat16)
        attended = jnp.einsum(
            "hqk,khd->qhd", probability, values_seq, preferred_element_type=jnp.float32
        )
        return (attended.astype(jnp.bfloat16), log_total[..., 0])

    attended, log_totals = lax.map(one_block, (grouped, jnp.arange(block_count)))
    return (attended.reshape(half_len, head_count, head_size), log_totals)


def attend_backward(queries_seq, keys_seq, values_seq, length, offset, log_totals, grad_seq):
    half_len, head_count, head_size = queries_seq.shape
    block_rows = min(512, half_len)
    block_count = half_len // block_rows
    score_scale = HEAD_DIM ** (-0.5)
    grouped = queries_seq.reshape(block_count, block_rows, head_count, head_size)
    grad_grouped = grad_seq.reshape(block_count, block_rows, head_count, head_size)

    def one_block(carried, paired):
        query_rows, grad_rows, log_rows, block_index = paired
        scores = score_block(query_rows, keys_seq, length, offset + block_index * block_rows)
        probability = jnp.exp(scores - log_rows[..., None])
        prob_low = probability.astype(jnp.bfloat16)
        grad_prob = jnp.einsum(
            "qhd,khd->hqk", grad_rows, values_seq, preferred_element_type=jnp.float32
        )
        inner_sum = jnp.sum(probability * grad_prob, axis=-1, keepdims=True)
        grad_scores = (probability * (grad_prob - inner_sum)).astype(jnp.bfloat16)
        grad_query_rows = (
            jnp.einsum("hqk,khd->qhd", grad_scores, keys_seq, preferred_element_type=jnp.float32)
            * score_scale
        )
        key_part = (
            jnp.einsum("hqk,qhd->khd", grad_scores, query_rows, preferred_element_type=jnp.float32)
            * score_scale
        )
        value_part = jnp.einsum(
            "hqk,qhd->khd", prob_low, grad_rows, preferred_element_type=jnp.float32
        )
        return ((carried[0] + key_part, carried[1] + value_part), grad_query_rows)

    empty = jnp.zeros(keys_seq.shape, jnp.float32)
    sums, grad_queries = lax.scan(
        one_block, (empty, empty), (grouped, grad_grouped, log_totals, jnp.arange(block_count))
    )
    return (grad_queries.reshape(half_len, head_count, head_size), sums[0], sums[1])


def tp_psum(part, count):
    me = lax.axis_index(TP)
    low_part = part.astype(jnp.bfloat16)
    rows = part.shape[0] // count
    chunks = low_part.reshape((count, rows) + part.shape[1:])
    total = lax.dynamic_index_in_dim(chunks, me, 0, keepdims=False).astype(jnp.float32)
    for shift in range(1, count):
        pairs = [(i, (i + shift) % count) for i in range(count)]
        piece = lax.dynamic_index_in_dim(chunks, (me + shift) % count, 0, keepdims=False)
        total = total + lax.ppermute(piece, TP, pairs).astype(jnp.float32)
    reduced = total.astype(jnp.bfloat16)
    gathered = jnp.zeros(low_part.shape, jnp.bfloat16)
    gathered = lax.dynamic_update_slice_in_dim(gathered, reduced, me * rows, 0)
    for shift in range(1, count):
        pairs = [(i, (i + shift) % count) for i in range(count)]
        got = lax.ppermute(reduced, TP, pairs)
        gathered = lax.dynamic_update_slice_in_dim(
            gathered, got, ((me + count - shift) % count) * rows, 0
        )
    return gathered


def exchange_gather(piece, axis, count):
    me = lax.axis_index(axis)
    gathered = jnp.zeros((count,) + piece.shape, piece.dtype)
    gathered = lax.dynamic_update_index_in_dim(gathered, piece, me, 0)
    for shift in range(1, count):
        pairs = [(i, (i + shift) % count) for i in range(count)]
        got = lax.ppermute(piece, axis, pairs)
        gathered = lax.dynamic_update_index_in_dim(gathered, got, (me + count - shift) % count, 0)
    return gathered


def exchange_scatter(blocks, axis, count):
    me = lax.axis_index(axis)
    total = lax.dynamic_index_in_dim(blocks, me, 0, keepdims=False)
    for shift in range(1, count):
        pairs = [(i, (i + shift) % count) for i in range(count)]
        piece = lax.dynamic_index_in_dim(blocks, (me + shift) % count, 0, keepdims=False)
        total = total + lax.ppermute(piece, axis, pairs)
    return total


def scatter_low(grad, dim):
    summed = lax.psum_scatter(
        grad.astype(jnp.bfloat16), (SHARD, CTX), scatter_dimension=dim, tiled=True
    )
    return summed.astype(jnp.float32)


def matmul_low(left, right):
    return jnp.dot(left, right, preferred_element_type=jnp.float32)


MID_SPLIT = (3, 5)


def middle_rows(attn_rows, tokens_rows, grad_final, output_full, gate_full, up_full, down_full, tp_count):
    bf_type = jnp.bfloat16
    resid = tokens_rows + tp_psum(matmul_low(attn_rows, output_full), tp_count).astype(jnp.float32)
    normed_two, scale_two = normalize(resid)
    input_two = normed_two.astype(bf_type)
    gate_proj = matmul_low(input_two, gate_full)
    up_proj = matmul_low(input_two, up_full)
    gate_sigmoid = jax.nn.sigmoid(gate_proj)
    hidden = (gate_proj * gate_sigmoid * up_proj).astype(bf_type)
    grad_branch = grad_final.astype(bf_type)
    grad_hidden = jnp.einsum(
        "rd,fd->rf", grad_branch, down_full, preferred_element_type=jnp.float32
    )
    grad_gate_act = (
        grad_hidden * up_proj * gate_sigmoid * (1.0 + gate_proj * (1.0 - gate_sigmoid))
    ).astype(bf_type)
    grad_up_act = (grad_hidden * gate_proj * gate_sigmoid).astype(bf_type)
    grad_input_two = jnp.einsum(
        "rf,df->rd", grad_gate_act, gate_full, preferred_element_type=jnp.float32
    ) + jnp.einsum("rf,df->rd", grad_up_act, up_full, preferred_element_type=jnp.float32)
    branch_two = matmul_low(hidden, down_full)
    grad_down = jnp.einsum("rf,rd->fd", hidden, grad_branch, preferred_element_type=jnp.float32)
    grad_gate = jnp.einsum(
        "rd,rf->df", input_two, grad_gate_act, preferred_element_type=jnp.float32
    )
    grad_up = jnp.einsum("rd,rf->df", input_two, grad_up_act, preferred_element_type=jnp.float32)
    grad_input_two = tp_psum(grad_input_two, tp_count)
    return [
        resid, branch_two, normed_two, scale_two, grad_final, grad_input_two,
        grad_gate, grad_up, grad_down,
    ]


def body(tp_count, ctx_count, *args):
    return block(tp_count, ctx_count, *args)


def block(tp_count, ctx_count, tokens, lengths, cotangent, w_query, w_key, w_value, w_output, w_gate, w_up, w_down):
    seq_count, half_len, model_width = tokens.shape
    head_cols = w_query.shape[1]
    head_count = head_cols // HEAD_DIM
    row_total = seq_count * half_len
    offset = lax.axis_index(CTX) * half_len
    positions = offset + jnp.arange(half_len)
    valid_mask = (positions[None, :] < lengths[:, None]).astype(jnp.float32)
    bf_type = jnp.bfloat16
    attn_low = (
        w_query.astype(bf_type),
        w_key.astype(bf_type),
        w_value.astype(bf_type),
        w_output.astype(bf_type),
    )
    mlp_low = (w_gate.astype(bf_type), w_up.astype(bf_type), w_down.astype(bf_type))
    attn_joined = lax.all_gather(
        jnp.concatenate([attn_low[0], attn_low[1], attn_low[2], attn_low[3].T], axis=1),
        (SHARD, CTX),
        axis=0,
        tiled=True,
    )
    query_full, key_full, value_full, output_t = jnp.split(attn_joined, 4, axis=1)
    output_full = output_t.T
    gate_full, up_full, down_full = (
        lax.all_gather(mlp_low[0], (SHARD, CTX), axis=0, tiled=True),
        lax.all_gather(mlp_low[1], (SHARD, CTX), axis=0, tiled=True),
        lax.all_gather(mlp_low[2], (SHARD, CTX), axis=1, tiled=True),
    )
    tokens_wide = tokens.astype(jnp.float32).reshape(row_total, model_width)
    normed_one, scale_one = normalize(tokens_wide)
    input_one = normed_one.astype(bf_type)
    split_heads = (seq_count, half_len, head_count, HEAD_DIM)
    query_pre = matmul_low(input_one, query_full).reshape(split_heads)
    key_pre = matmul_low(input_one, key_full).reshape(split_heads)
    value_pre = matmul_low(input_one, value_full).reshape(split_heads)
    cosine, sine_table = rope_tables(half_len, HEAD_DIM, offset)
    queries = rotate(query_pre, cosine, sine_table).astype(bf_type)
    keys_rot = rotate(key_pre, cosine, sine_table).astype(bf_type)
    values_low = value_pre.astype(bf_type)
    keys_all, values_all = (
        jnp.swapaxes(exchange_gather(keys_rot, CTX, ctx_count), 0, 1).reshape(
            (seq_count, ctx_count * half_len, head_count, HEAD_DIM)
        ),
        jnp.swapaxes(exchange_gather(values_low, CTX, ctx_count), 0, 1).reshape(
            (seq_count, ctx_count * half_len, head_count, HEAD_DIM)
        ),
    )
    seq_index = 0
    attended, log_totals = attend_forward(
        queries[seq_index], keys_all[seq_index], values_all[seq_index], lengths[seq_index], offset
    )
    attended_list = [attended]
    log_list = [log_totals]
    attn_out = jnp.stack(attended_list).reshape(row_total, head_cols)
    grad_final = cotangent.astype(jnp.float32).reshape(row_total, model_width) * valid_mask.reshape(
        row_total, 1
    )
    unit = row_total // sum(MID_SPLIT)
    bounds = [0]
    for share in MID_SPLIT:
        bounds.append(bounds[-1] + share * unit)
    pieces = []
    for index in range(len(MID_SPLIT)):
        rows = slice(bounds[index], bounds[index + 1])
        pieces.append(
            middle_rows(
                attn_out[rows], tokens_wide[rows], grad_final[rows],
                output_full, gate_full, up_full, down_full, tp_count,
            )
        )
    grad_gate = sum(piece[6] for piece in pieces)
    grad_up = sum(piece[7] for piece in pieces)
    grad_down = sum(piece[8] for piece in pieces)
    last_sum = pieces[-1][5]
    (grad_gate, grad_up, grad_down), last_sum = lax.optimization_barrier(
        ((grad_gate, grad_up, grad_down), last_sum)
    )
    pieces[-1][5] = last_sum
    mlp_grads = (
        scatter_low(grad_gate, 0),
        scatter_low(grad_up, 0),
        scatter_low(grad_down, 1),
    )
    resid = jnp.concatenate([piece[0] for piece in pieces], axis=0)
    branch_two_part = jnp.concatenate([piece[1] for piece in pieces], axis=0)
    grad_resid_parts, grad_attn_parts, grad_wout = [], [], 0.0
    for index, piece in enumerate(pieces):
        grad_resid_part = piece[4] + norm_back(piece[2], piece[3], piece[5].astype(jnp.float32))
        resid_low = grad_resid_part.astype(bf_type)
        grad_wout = grad_wout + jnp.einsum(
            "rc,rd->cd", attn_out[bounds[index]:bounds[index + 1]], resid_low,
            preferred_element_type=jnp.float32,
        )
        grad_attn_parts.append(
            jnp.einsum("rd,cd->rc", resid_low, output_full, preferred_element_type=jnp.float32)
        )
        grad_resid_parts.append(grad_resid_part)
    grad_resid = jnp.concatenate(grad_resid_parts, axis=0)
    grad_attn = jnp.concatenate(grad_attn_parts, axis=0).astype(bf_type).reshape(split_heads)
    branch_two_part, grad_attn = lax.optimization_barrier((branch_two_part, grad_attn))
    final_sum = resid + tp_psum(branch_two_part, tp_count).astype(jnp.float32)
    seq_index = 0
    grad_queries, grad_keys_seq, grad_values_seq = attend_backward(
        queries[seq_index],
        keys_all[seq_index],
        values_all[seq_index],
        lengths[seq_index],
        offset,
        log_list[seq_index],
        grad_attn[seq_index],
    )
    query_grads = [grad_queries]
    key_grads = [grad_keys_seq]
    value_grads = [grad_values_seq]
    grad_keys, grad_values = (
        exchange_scatter(
            jnp.stack(key_grads).reshape((ctx_count, half_len, head_count, HEAD_DIM)), CTX, ctx_count
        ).reshape(split_heads),
        exchange_scatter(
            jnp.stack(value_grads).reshape((ctx_count, half_len, head_count, HEAD_DIM)), CTX, ctx_count
        ).reshape(split_heads),
    )
    query_grad = jnp.stack(query_grads)
    q_parts, k_parts, v_parts, token_parts = [], [], [], []
    for index in range(len(MID_SPLIT)):
        low_row, high_row = bounds[index], bounds[index + 1]
        count = high_row - low_row
        cos_part, sin_part = cosine[low_row:high_row], sine_table[low_row:high_row]
        q_part = rotate_back(query_grad[:, low_row:high_row], cos_part, sin_part)
        q_part = q_part.astype(bf_type).reshape(count, head_cols)
        k_part = rotate_back(grad_keys[:, low_row:high_row], cos_part, sin_part)
        k_part = k_part.astype(bf_type).reshape(count, head_cols)
        v_part = grad_values[:, low_row:high_row].astype(bf_type).reshape(count, head_cols)
        input_part = (
            jnp.einsum("rc,dc->rd", q_part, query_full, preferred_element_type=jnp.float32)
            + jnp.einsum("rc,dc->rd", k_part, key_full, preferred_element_type=jnp.float32)
            + jnp.einsum("rc,dc->rd", v_part, value_full, preferred_element_type=jnp.float32)
        )
        input_part = tp_psum(input_part, tp_count).astype(jnp.float32)
        token_parts.append(
            grad_resid[low_row:high_row]
            + norm_back(normed_one[low_row:high_row], scale_one[low_row:high_row], input_part)
        )
        q_parts.append(q_part)
        k_parts.append(k_part)
        v_parts.append(v_part)
    grad_q_pre = jnp.concatenate(q_parts, axis=0)
    grad_k_pre = jnp.concatenate(k_parts, axis=0)
    grad_v_pre = jnp.concatenate(v_parts, axis=0)
    grad_wq = jnp.einsum("rd,rc->dc", input_one, grad_q_pre, preferred_element_type=jnp.float32)
    grad_wk = jnp.einsum("rd,rc->dc", input_one, grad_k_pre, preferred_element_type=jnp.float32)
    grad_wv = jnp.einsum("rd,rc->dc", input_one, grad_v_pre, preferred_element_type=jnp.float32)
    qkv_grads = jnp.split(
        scatter_low(jnp.concatenate([grad_wq, grad_wk, grad_wv], axis=1), 0), 3, axis=1
    )
    attn_grads = (qkv_grads[0], qkv_grads[1], qkv_grads[2], scatter_low(grad_wout, 1))
    grad_tokens = jnp.concatenate(token_parts, axis=0)
    output = final_sum.astype(bf_type).reshape(seq_count, half_len, model_width)
    grad_tokens = grad_tokens.reshape(seq_count, half_len, model_width)
    return (
        output,
        grad_tokens,
        attn_grads[0],
        attn_grads[1],
        attn_grads[2],
        attn_grads[3],
        mlp_grads[0],
        mlp_grads[1],
        mlp_grads[2],
    )


def solution(mesh):
    return jax.shard_map(
        functools.partial(body, mesh.shape[TP], mesh.shape[CTX]),
        mesh=mesh,
        in_specs=(
            P(SHARD, CTX, None),
            P(SHARD),
            P(SHARD, CTX, None),
            P((SHARD, CTX), TP),
            P((SHARD, CTX), TP),
            P((SHARD, CTX), TP),
            P(TP, (SHARD, CTX)),
            P((SHARD, CTX), TP),
            P((SHARD, CTX), TP),
            P(TP, (SHARD, CTX)),
        ),
        out_specs=(
            P(SHARD, CTX, None),
            P(SHARD, CTX, None),
            P((SHARD, CTX), TP),
            P((SHARD, CTX), TP),
            P((SHARD, CTX), TP),
            P(TP, (SHARD, CTX)),
            P((SHARD, CTX), TP),
            P((SHARD, CTX), TP),
            P(TP, (SHARD, CTX)),
        ),
        check_vma=False,
    )
```

```python
import functools

import jax
import jax.numpy as jnp
from jax import lax
from jax.sharding import PartitionSpec as P

SHARD, CTX, TP = "shard", "ctx", "tp"

HEAD_DIM = 128


EPSILON = 1e-05


def normalize(values):
    center = values - jnp.mean(values, axis=-1, keepdims=True)
    inv_scale = lax.rsqrt(jnp.mean(center * center, axis=-1, keepdims=True) + EPSILON)
    return (center * inv_scale, inv_scale)


def norm_back(normed, inv_scale, upstream):
    first_mean = jnp.mean(upstream, axis=-1, keepdims=True)
    second_mean = jnp.mean(upstream * normed, axis=-1, keepdims=True)
    return inv_scale * (upstream - first_mean - normed * second_mean)


def rope_tables(row_count, head_size, offset):
    positions = (jnp.arange(row_count) + offset).astype(jnp.float32)
    inverse = 10000.0 ** (-(jnp.arange(head_size // 2).astype(jnp.float32) * 2.0) / head_size)
    angles = positions[:, None] * inverse[None, :]
    angles = jnp.concatenate([angles, angles], axis=-1)
    return (jnp.cos(angles)[:, None, :], jnp.sin(angles)[:, None, :])


def turn_half(values):
    half_dim = values.shape[-1] // 2
    return jnp.concatenate([-values[..., half_dim:], values[..., :half_dim]], axis=-1)


def rotate(values, cosine, sine_table):
    return values * cosine + turn_half(values) * sine_table


def rotate_back(values, cosine, sine_table):
    return values * cosine - turn_half(values) * sine_table


def score_block(query_rows, keys_seq, length, row_start):
    block_rows = query_rows.shape[0]
    key_pos = jnp.arange(keys_seq.shape[0])
    row_pos = row_start + jnp.arange(block_rows)
    scores = jnp.einsum(
        "qhd,khd->hqk", query_rows, keys_seq, preferred_element_type=jnp.float32
    ) * HEAD_DIM ** (-0.5)
    allowed = (key_pos[None, :] <= row_pos[:, None]) & (key_pos[None, :] < length)
    return jnp.where(allowed[None], scores, -1e30)


def attend_forward(queries_seq, keys_seq, values_seq, length, offset):
    half_len, head_count, head_size = queries_seq.shape
    block_rows = min(512, half_len)
    block_count = half_len // block_rows
    grouped = queries_seq.reshape(block_count, block_rows, head_count, head_size)

    def one_block(paired):
        query_rows, block_index = paired
        scores = score_block(query_rows, keys_seq, length, offset + block_index * block_rows)
        row_peak = jnp.max(scores, axis=-1, keepdims=True)
        log_total = jnp.log(jnp.sum(jnp.exp(scores - row_peak), axis=-1, keepdims=True)) + row_peak
        probability = jnp.exp(scores - log_total).astype(jnp.bfloat16)
        attended = jnp.einsum(
            "hqk,khd->qhd", probability, values_seq, preferred_element_type=jnp.float32
        )
        return (attended.astype(jnp.bfloat16), log_total[..., 0])

    attended, log_totals = lax.map(one_block, (grouped, jnp.arange(block_count)))
    return (attended.reshape(half_len, head_count, head_size), log_totals)


def attend_backward(queries_seq, keys_seq, values_seq, length, offset, log_totals, grad_seq):
    half_len, head_count, head_size = queries_seq.shape
    block_rows = min(512, half_len)
    block_count = half_len // block_rows
    score_scale = HEAD_DIM ** (-0.5)
    grouped = queries_seq.reshape(block_count, block_rows, head_count, head_size)
    grad_grouped = grad_seq.reshape(block_count, block_rows, head_count, head_size)

    def one_block(carried, paired):
        query_rows, grad_rows, log_rows, block_index = paired
        scores = score_block(query_rows, keys_seq, length, offset + block_index * block_rows)
        probability = jnp.exp(scores - log_rows[..., None])
        prob_low = probability.astype(jnp.bfloat16)
        grad_prob = jnp.einsum(
            "qhd,khd->hqk", grad_rows, values_seq, preferred_element_type=jnp.float32
        )
        inner_sum = jnp.sum(probability * grad_prob, axis=-1, keepdims=True)
        grad_scores = (probability * (grad_prob - inner_sum)).astype(jnp.bfloat16)
        grad_query_rows = (
            jnp.einsum("hqk,khd->qhd", grad_scores, keys_seq, preferred_element_type=jnp.float32)
            * score_scale
        )
        key_part = (
            jnp.einsum("hqk,qhd->khd", grad_scores, query_rows, preferred_element_type=jnp.float32)
            * score_scale
        )
        value_part = jnp.einsum(
            "hqk,qhd->khd", prob_low, grad_rows, preferred_element_type=jnp.float32
        )
        return ((carried[0] + key_part, carried[1] + value_part), grad_query_rows)

    empty = jnp.zeros(keys_seq.shape, jnp.float32)
    sums, grad_queries = lax.scan(
        one_block, (empty, empty), (grouped, grad_grouped, log_totals, jnp.arange(block_count))
    )
    return (grad_queries.reshape(half_len, head_count, head_size), sums[0], sums[1])


def tp_psum(part, count):
    me = lax.axis_index(TP)
    low_part = part.astype(jnp.bfloat16)
    rows = part.shape[0] // count
    chunks = low_part.reshape((count, rows) + part.shape[1:])
    total = lax.dynamic_index_in_dim(chunks, me, 0, keepdims=False).astype(jnp.float32)
    for shift in range(1, count):
        pairs = [(i, (i + shift) % count) for i in range(count)]
        piece = lax.dynamic_index_in_dim(chunks, (me + shift) % count, 0, keepdims=False)
        total = total + lax.ppermute(piece, TP, pairs).astype(jnp.float32)
    reduced = total.astype(jnp.bfloat16)
    gathered = jnp.zeros(low_part.shape, jnp.bfloat16)
    gathered = lax.dynamic_update_slice_in_dim(gathered, reduced, me * rows, 0)
    for shift in range(1, count):
        pairs = [(i, (i + shift) % count) for i in range(count)]
        got = lax.ppermute(reduced, TP, pairs)
        gathered = lax.dynamic_update_slice_in_dim(
            gathered, got, ((me + count - shift) % count) * rows, 0
        )
    return gathered


def exchange_gather(piece, axis, count):
    me = lax.axis_index(axis)
    gathered = jnp.zeros((count,) + piece.shape, piece.dtype)
    gathered = lax.dynamic_update_index_in_dim(gathered, piece, me, 0)
    for shift in range(1, count):
        pairs = [(i, (i + shift) % count) for i in range(count)]
        got = lax.ppermute(piece, axis, pairs)
        gathered = lax.dynamic_update_index_in_dim(gathered, got, (me + count - shift) % count, 0)
    return gathered


def exchange_scatter(blocks, axis, count):
    me = lax.axis_index(axis)
    total = lax.dynamic_index_in_dim(blocks, me, 0, keepdims=False)
    for shift in range(1, count):
        pairs = [(i, (i + shift) % count) for i in range(count)]
        piece = lax.dynamic_index_in_dim(blocks, (me + shift) % count, 0, keepdims=False)
        total = total + lax.ppermute(piece, axis, pairs)
    return total


def scatter_low(grad, dim):
    summed = lax.psum_scatter(
        grad.astype(jnp.bfloat16), (SHARD, CTX), scatter_dimension=dim, tiled=True
    )
    return summed.astype(jnp.float32)


def matmul_low(left, right):
    return jnp.dot(left, right, preferred_element_type=jnp.float32)


MID_SPLIT = (3, 5)


def middle_rows(attn_rows, tokens_rows, grad_final, output_full, gate_full, up_full, down_full, tp_count):
    bf_type = jnp.bfloat16
    resid = tokens_rows + tp_psum(matmul_low(attn_rows, output_full), tp_count).astype(jnp.float32)
    normed_two, scale_two = normalize(resid)
    input_two = normed_two.astype(bf_type)
    gate_proj = matmul_low(input_two, gate_full)
    up_proj = matmul_low(input_two, up_full)
    gate_sigmoid = jax.nn.sigmoid(gate_proj)
    hidden = (gate_proj * gate_sigmoid * up_proj).astype(bf_type)
    grad_branch = grad_final.astype(bf_type)
    grad_hidden = jnp.einsum(
        "rd,fd->rf", grad_branch, down_full, preferred_element_type=jnp.float32
    )
    grad_gate_act = (
        grad_hidden * up_proj * gate_sigmoid * (1.0 + gate_proj * (1.0 - gate_sigmoid))
    ).astype(bf_type)
    grad_up_act = (grad_hidden * gate_proj * gate_sigmoid).astype(bf_type)
    grad_input_two = jnp.einsum(
        "rf,df->rd", grad_gate_act, gate_full, preferred_element_type=jnp.float32
    ) + jnp.einsum("rf,df->rd", grad_up_act, up_full, preferred_element_type=jnp.float32)
    branch_two = matmul_low(hidden, down_full)
    grad_down = jnp.einsum("rf,rd->fd", hidden, grad_branch, preferred_element_type=jnp.float32)
    grad_gate = jnp.einsum(
        "rd,rf->df", input_two, grad_gate_act, preferred_element_type=jnp.float32
    )
    grad_up = jnp.einsum("rd,rf->df", input_two, grad_up_act, preferred_element_type=jnp.float32)
    grad_input_two = tp_psum(grad_input_two, tp_count)
    return [
        resid, branch_two, normed_two, scale_two, grad_final, grad_input_two,
        grad_gate, grad_up, grad_down,
    ]


def body(tp_count, ctx_count, *args):
    return block(tp_count, ctx_count, *args)


def block(tp_count, ctx_count, tokens, lengths, cotangent, w_query, w_key, w_value, w_output, w_gate, w_up, w_down):
    seq_count, half_len, model_width = tokens.shape
    head_cols = w_query.shape[1]
    head_count = head_cols // HEAD_DIM
    row_total = seq_count * half_len
    offset = lax.axis_index(CTX) * half_len
    positions = offset + jnp.arange(half_len)
    valid_mask = (positions[None, :] < lengths[:, None]).astype(jnp.float32)
    bf_type = jnp.bfloat16
    attn_low = (
        w_query.astype(bf_type),
        w_key.astype(bf_type),
        w_value.astype(bf_type),
        w_output.astype(bf_type),
    )
    mlp_low = (w_gate.astype(bf_type), w_up.astype(bf_type), w_down.astype(bf_type))
    key_value = lax.all_gather(
        jnp.concatenate([attn_low[1], attn_low[2]], axis=1), (SHARD, CTX), axis=0, tiled=True
    )
    query_output = lax.all_gather(
        jnp.concatenate([attn_low[0], attn_low[3].T], axis=1), (SHARD, CTX), axis=0, tiled=True
    )
    key_full, value_full = jnp.split(key_value, 2, axis=1)
    query_full, output_t = jnp.split(query_output, 2, axis=1)
    output_full = output_t.T
    gate_full, up_full, down_full = (
        lax.all_gather(mlp_low[0], (SHARD, CTX), axis=0, tiled=True),
        lax.all_gather(mlp_low[1], (SHARD, CTX), axis=0, tiled=True),
        lax.all_gather(mlp_low[2], (SHARD, CTX), axis=1, tiled=True),
    )
    tokens_wide = tokens.astype(jnp.float32).reshape(row_total, model_width)
    normed_one, scale_one = normalize(tokens_wide)
    input_one = normed_one.astype(bf_type)
    split_heads = (seq_count, half_len, head_count, HEAD_DIM)
    query_pre = matmul_low(input_one, query_full).reshape(split_heads)
    key_pre = matmul_low(input_one, key_full).reshape(split_heads)
    value_pre = matmul_low(input_one, value_full).reshape(split_heads)
    cosine, sine_table = rope_tables(half_len, HEAD_DIM, offset)
    queries = rotate(query_pre, cosine, sine_table).astype(bf_type)
    keys_rot = rotate(key_pre, cosine, sine_table).astype(bf_type)
    values_low = value_pre.astype(bf_type)
    keys_all, values_all = (
        jnp.swapaxes(exchange_gather(keys_rot, CTX, ctx_count), 0, 1).reshape(
            (seq_count, ctx_count * half_len, head_count, HEAD_DIM)
        ),
        jnp.swapaxes(exchange_gather(values_low, CTX, ctx_count), 0, 1).reshape(
            (seq_count, ctx_count * half_len, head_count, HEAD_DIM)
        ),
    )
    seq_index = 0
    attended, log_totals = attend_forward(
        queries[seq_index], keys_all[seq_index], values_all[seq_index], lengths[seq_index], offset
    )
    attended_list = [attended]
    log_list = [log_totals]
    attn_out = jnp.stack(attended_list).reshape(row_total, head_cols)
    grad_final = cotangent.astype(jnp.float32).reshape(row_total, model_width) * valid_mask.reshape(
        row_total, 1
    )
    unit = row_total // sum(MID_SPLIT)
    bounds = [0]
    for share in MID_SPLIT:
        bounds.append(bounds[-1] + share * unit)
    pieces = []
    for index in range(len(MID_SPLIT)):
        rows = slice(bounds[index], bounds[index + 1])
        pieces.append(
            middle_rows(
                attn_out[rows], tokens_wide[rows], grad_final[rows],
                output_full, gate_full, up_full, down_full, tp_count,
            )
        )
    grad_gate = sum(piece[6] for piece in pieces)
    grad_up = sum(piece[7] for piece in pieces)
    grad_down = sum(piece[8] for piece in pieces)
    last_sum = pieces[-1][5]
    (grad_gate, grad_up, grad_down), last_sum = lax.optimization_barrier(
        ((grad_gate, grad_up, grad_down), last_sum)
    )
    pieces[-1][5] = last_sum
    mlp_grads = (
        scatter_low(grad_gate, 0),
        scatter_low(grad_up, 0),
        scatter_low(grad_down, 1),
    )
    resid = jnp.concatenate([piece[0] for piece in pieces], axis=0)
    branch_two_part = jnp.concatenate([piece[1] for piece in pieces], axis=0)
    grad_resid_parts, grad_attn_parts, grad_wout = [], [], 0.0
    for index, piece in enumerate(pieces):
        grad_resid_part = piece[4] + norm_back(piece[2], piece[3], piece[5].astype(jnp.float32))
        resid_low = grad_resid_part.astype(bf_type)
        grad_wout = grad_wout + jnp.einsum(
            "rc,rd->cd", attn_out[bounds[index]:bounds[index + 1]], resid_low,
            preferred_element_type=jnp.float32,
        )
        grad_attn_parts.append(
            jnp.einsum("rd,cd->rc", resid_low, output_full, preferred_element_type=jnp.float32)
        )
        grad_resid_parts.append(grad_resid_part)
    grad_resid = jnp.concatenate(grad_resid_parts, axis=0)
    grad_attn = jnp.concatenate(grad_attn_parts, axis=0).astype(bf_type).reshape(split_heads)
    branch_two_part, grad_attn = lax.optimization_barrier((branch_two_part, grad_attn))
    final_sum = resid + tp_psum(branch_two_part, tp_count).astype(jnp.float32)
    seq_index = 0
    grad_queries, grad_keys_seq, grad_values_seq = attend_backward(
        queries[seq_index],
        keys_all[seq_index],
        values_all[seq_index],
        lengths[seq_index],
        offset,
        log_list[seq_index],
        grad_attn[seq_index],
    )
    query_grads = [grad_queries]
    key_grads = [grad_keys_seq]
    value_grads = [grad_values_seq]
    grad_keys, grad_values = (
        exchange_scatter(
            jnp.stack(key_grads).reshape((ctx_count, half_len, head_count, HEAD_DIM)), CTX, ctx_count
        ).reshape(split_heads),
        exchange_scatter(
            jnp.stack(value_grads).reshape((ctx_count, half_len, head_count, HEAD_DIM)), CTX, ctx_count
        ).reshape(split_heads),
    )
    query_grad = jnp.stack(query_grads)
    q_parts, k_parts, v_parts, token_parts = [], [], [], []
    for index in range(len(MID_SPLIT)):
        low_row, high_row = bounds[index], bounds[index + 1]
        count = high_row - low_row
        cos_part, sin_part = cosine[low_row:high_row], sine_table[low_row:high_row]
        q_part = rotate_back(query_grad[:, low_row:high_row], cos_part, sin_part)
        q_part = q_part.astype(bf_type).reshape(count, head_cols)
        k_part = rotate_back(grad_keys[:, low_row:high_row], cos_part, sin_part)
        k_part = k_part.astype(bf_type).reshape(count, head_cols)
        v_part = grad_values[:, low_row:high_row].astype(bf_type).reshape(count, head_cols)
        input_part = (
            jnp.einsum("rc,dc->rd", q_part, query_full, preferred_element_type=jnp.float32)
            + jnp.einsum("rc,dc->rd", k_part, key_full, preferred_element_type=jnp.float32)
            + jnp.einsum("rc,dc->rd", v_part, value_full, preferred_element_type=jnp.float32)
        )
        input_part = tp_psum(input_part, tp_count).astype(jnp.float32)
        token_parts.append(
            grad_resid[low_row:high_row]
            + norm_back(normed_one[low_row:high_row], scale_one[low_row:high_row], input_part)
        )
        q_parts.append(q_part)
        k_parts.append(k_part)
        v_parts.append(v_part)
    grad_q_pre = jnp.concatenate(q_parts, axis=0)
    grad_k_pre = jnp.concatenate(k_parts, axis=0)
    grad_v_pre = jnp.concatenate(v_parts, axis=0)
    grad_wq = jnp.einsum("rd,rc->dc", input_one, grad_q_pre, preferred_element_type=jnp.float32)
    grad_wk = jnp.einsum("rd,rc->dc", input_one, grad_k_pre, preferred_element_type=jnp.float32)
    grad_wv = jnp.einsum("rd,rc->dc", input_one, grad_v_pre, preferred_element_type=jnp.float32)
    qkv_grads = jnp.split(
        scatter_low(jnp.concatenate([grad_wq, grad_wk, grad_wv], axis=1), 0), 3, axis=1
    )
    attn_grads = (qkv_grads[0], qkv_grads[1], qkv_grads[2], scatter_low(grad_wout, 1))
    grad_tokens = jnp.concatenate(token_parts, axis=0)
    output = final_sum.astype(bf_type).reshape(seq_count, half_len, model_width)
    grad_tokens = grad_tokens.reshape(seq_count, half_len, model_width)
    return (
        output,
        grad_tokens,
        attn_grads[0],
        attn_grads[1],
        attn_grads[2],
        attn_grads[3],
        mlp_grads[0],
        mlp_grads[1],
        mlp_grads[2],
    )


def solution(mesh):
    return jax.shard_map(
        functools.partial(body, mesh.shape[TP], mesh.shape[CTX]),
        mesh=mesh,
        in_specs=(
            P(SHARD, CTX, None),
            P(SHARD),
            P(SHARD, CTX, None),
            P((SHARD, CTX), TP),
            P((SHARD, CTX), TP),
            P((SHARD, CTX), TP),
            P(TP, (SHARD, CTX)),
            P((SHARD, CTX), TP),
            P((SHARD, CTX), TP),
            P(TP, (SHARD, CTX)),
        ),
        out_specs=(
            P(SHARD, CTX, None),
            P(SHARD, CTX, None),
            P((SHARD, CTX), TP),
            P((SHARD, CTX), TP),
            P((SHARD, CTX), TP),
            P(TP, (SHARD, CTX)),
            P((SHARD, CTX), TP),
            P((SHARD, CTX), TP),
            P(TP, (SHARD, CTX)),
        ),
        check_vma=False,
    )
```

```python
import functools

import jax
import jax.numpy as jnp
from jax import lax
from jax.sharding import PartitionSpec as P

SHARD, CTX, TP = "shard", "ctx", "tp"

HEAD_DIM = 128


EPSILON = 1e-05


def normalize(values):
    center = values - jnp.mean(values, axis=-1, keepdims=True)
    inv_scale = lax.rsqrt(jnp.mean(center * center, axis=-1, keepdims=True) + EPSILON)
    return (center * inv_scale, inv_scale)


def norm_back(normed, inv_scale, upstream):
    first_mean = jnp.mean(upstream, axis=-1, keepdims=True)
    second_mean = jnp.mean(upstream * normed, axis=-1, keepdims=True)
    return inv_scale * (upstream - first_mean - normed * second_mean)


def rope_tables(row_count, head_size, offset):
    positions = (jnp.arange(row_count) + offset).astype(jnp.float32)
    inverse = 10000.0 ** (-(jnp.arange(head_size // 2).astype(jnp.float32) * 2.0) / head_size)
    angles = positions[:, None] * inverse[None, :]
    angles = jnp.concatenate([angles, angles], axis=-1)
    return (jnp.cos(angles)[:, None, :], jnp.sin(angles)[:, None, :])


def turn_half(values):
    half_dim = values.shape[-1] // 2
    return jnp.concatenate([-values[..., half_dim:], values[..., :half_dim]], axis=-1)


def rotate(values, cosine, sine_table):
    return values * cosine + turn_half(values) * sine_table


def rotate_back(values, cosine, sine_table):
    return values * cosine - turn_half(values) * sine_table


def score_block(query_rows, keys_seq, length, row_start):
    block_rows = query_rows.shape[0]
    key_pos = jnp.arange(keys_seq.shape[0])
    row_pos = row_start + jnp.arange(block_rows)
    scores = jnp.einsum(
        "qhd,khd->hqk", query_rows, keys_seq, preferred_element_type=jnp.float32
    ) * HEAD_DIM ** (-0.5)
    allowed = (key_pos[None, :] <= row_pos[:, None]) & (key_pos[None, :] < length)
    return jnp.where(allowed[None], scores, -1e30)


def attend_forward(queries_seq, keys_seq, values_seq, length, offset):
    half_len, head_count, head_size = queries_seq.shape
    block_rows = min(512, half_len)
    block_count = half_len // block_rows
    grouped = queries_seq.reshape(block_count, block_rows, head_count, head_size)

    def one_block(paired):
        query_rows, block_index = paired
        scores = score_block(query_rows, keys_seq, length, offset + block_index * block_rows)
        row_peak = jnp.max(scores, axis=-1, keepdims=True)
        log_total = jnp.log(jnp.sum(jnp.exp(scores - row_peak), axis=-1, keepdims=True)) + row_peak
        probability = jnp.exp(scores - log_total).astype(jnp.bfloat16)
        attended = jnp.einsum(
            "hqk,khd->qhd", probability, values_seq, preferred_element_type=jnp.float32
        )
        return (attended.astype(jnp.bfloat16), log_total[..., 0])

    attended, log_totals = lax.map(one_block, (grouped, jnp.arange(block_count)))
    return (attended.reshape(half_len, head_count, head_size), log_totals)


def attend_backward(queries_seq, keys_seq, values_seq, length, offset, log_totals, grad_seq):
    half_len, head_count, head_size = queries_seq.shape
    block_rows = min(512, half_len)
    block_count = half_len // block_rows
    score_scale = HEAD_DIM ** (-0.5)
    grouped = queries_seq.reshape(block_count, block_rows, head_count, head_size)
    grad_grouped = grad_seq.reshape(block_count, block_rows, head_count, head_size)

    def one_block(carried, paired):
        query_rows, grad_rows, log_rows, block_index = paired
        scores = score_block(query_rows, keys_seq, length, offset + block_index * block_rows)
        probability = jnp.exp(scores - log_rows[..., None])
        prob_low = probability.astype(jnp.bfloat16)
        grad_prob = jnp.einsum(
            "qhd,khd->hqk", grad_rows, values_seq, preferred_element_type=jnp.float32
        )
        inner_sum = jnp.sum(probability * grad_prob, axis=-1, keepdims=True)
        grad_scores = (probability * (grad_prob - inner_sum)).astype(jnp.bfloat16)
        grad_query_rows = (
            jnp.einsum("hqk,khd->qhd", grad_scores, keys_seq, preferred_element_type=jnp.float32)
            * score_scale
        )
        key_part = (
            jnp.einsum("hqk,qhd->khd", grad_scores, query_rows, preferred_element_type=jnp.float32)
            * score_scale
        )
        value_part = jnp.einsum(
            "hqk,qhd->khd", prob_low, grad_rows, preferred_element_type=jnp.float32
        )
        return ((carried[0] + key_part, carried[1] + value_part), grad_query_rows)

    empty = jnp.zeros(keys_seq.shape, jnp.float32)
    sums, grad_queries = lax.scan(
        one_block, (empty, empty), (grouped, grad_grouped, log_totals, jnp.arange(block_count))
    )
    return (grad_queries.reshape(half_len, head_count, head_size), sums[0], sums[1])


def tp_psum(part, count):
    me = lax.axis_index(TP)
    low_part = part.astype(jnp.bfloat16)
    rows = part.shape[0] // count
    chunks = low_part.reshape((count, rows) + part.shape[1:])
    total = lax.dynamic_index_in_dim(chunks, me, 0, keepdims=False).astype(jnp.float32)
    for shift in range(1, count):
        pairs = [(i, (i + shift) % count) for i in range(count)]
        piece = lax.dynamic_index_in_dim(chunks, (me + shift) % count, 0, keepdims=False)
        total = total + lax.ppermute(piece, TP, pairs).astype(jnp.float32)
    reduced = total.astype(jnp.bfloat16)
    gathered = jnp.zeros(low_part.shape, jnp.bfloat16)
    gathered = lax.dynamic_update_slice_in_dim(gathered, reduced, me * rows, 0)
    for shift in range(1, count):
        pairs = [(i, (i + shift) % count) for i in range(count)]
        got = lax.ppermute(reduced, TP, pairs)
        gathered = lax.dynamic_update_slice_in_dim(
            gathered, got, ((me + count - shift) % count) * rows, 0
        )
    return gathered


def exchange_scatter(blocks, axis, count):
    me = lax.axis_index(axis)
    total = lax.dynamic_index_in_dim(blocks, me, 0, keepdims=False)
    for shift in range(1, count):
        pairs = [(i, (i + shift) % count) for i in range(count)]
        piece = lax.dynamic_index_in_dim(blocks, (me + shift) % count, 0, keepdims=False)
        total = total + lax.ppermute(piece, axis, pairs)
    return total


def scatter_low(grad, dim):
    summed = lax.psum_scatter(
        grad.astype(jnp.bfloat16), (SHARD, CTX), scatter_dimension=dim, tiled=True
    )
    return summed.astype(jnp.float32)


def matmul_low(left, right):
    return jnp.dot(left, right, preferred_element_type=jnp.float32)


MID_SPLIT = (3, 5)


def middle_rows(attn_rows, tokens_rows, grad_final, output_full, gate_full, up_full, down_full, tp_count):
    bf_type = jnp.bfloat16
    resid = tokens_rows + tp_psum(matmul_low(attn_rows, output_full), tp_count).astype(jnp.float32)
    normed_two, scale_two = normalize(resid)
    input_two = normed_two.astype(bf_type)
    gate_proj = matmul_low(input_two, gate_full)
    up_proj = matmul_low(input_two, up_full)
    gate_sigmoid = jax.nn.sigmoid(gate_proj)
    hidden = (gate_proj * gate_sigmoid * up_proj).astype(bf_type)
    grad_branch = grad_final.astype(bf_type)
    grad_hidden = jnp.einsum(
        "rd,fd->rf", grad_branch, down_full, preferred_element_type=jnp.float32
    )
    grad_gate_act = (
        grad_hidden * up_proj * gate_sigmoid * (1.0 + gate_proj * (1.0 - gate_sigmoid))
    ).astype(bf_type)
    grad_up_act = (grad_hidden * gate_proj * gate_sigmoid).astype(bf_type)
    grad_input_two = jnp.einsum(
        "rf,df->rd", grad_gate_act, gate_full, preferred_element_type=jnp.float32
    ) + jnp.einsum("rf,df->rd", grad_up_act, up_full, preferred_element_type=jnp.float32)
    branch_two = matmul_low(hidden, down_full)
    grad_down = jnp.einsum("rf,rd->fd", hidden, grad_branch, preferred_element_type=jnp.float32)
    grad_gate = jnp.einsum(
        "rd,rf->df", input_two, grad_gate_act, preferred_element_type=jnp.float32
    )
    grad_up = jnp.einsum("rd,rf->df", input_two, grad_up_act, preferred_element_type=jnp.float32)
    grad_input_two = tp_psum(grad_input_two, tp_count)
    return [
        resid, branch_two, normed_two, scale_two, grad_final, grad_input_two,
        grad_gate, grad_up, grad_down,
    ]


def body(tp_count, ctx_count, *args):
    return block(tp_count, ctx_count, *args)


def block(tp_count, ctx_count, tokens, lengths, cotangent, w_query, w_key, w_value, w_output, w_gate, w_up, w_down):
    seq_count, half_len, model_width = tokens.shape
    head_cols = w_query.shape[1]
    head_count = head_cols // HEAD_DIM
    row_total = seq_count * half_len
    offset = lax.axis_index(CTX) * half_len
    positions = offset + jnp.arange(half_len)
    valid_mask = (positions[None, :] < lengths[:, None]).astype(jnp.float32)
    bf_type = jnp.bfloat16
    attn_low = (
        w_query.astype(bf_type),
        w_key.astype(bf_type),
        w_value.astype(bf_type),
        w_output.astype(bf_type),
    )
    mlp_low = (w_gate.astype(bf_type), w_up.astype(bf_type), w_down.astype(bf_type))
    key_value = lax.all_gather(
        jnp.concatenate([attn_low[1], attn_low[2]], axis=1), (SHARD, CTX), axis=0, tiled=True
    )
    query_output = lax.all_gather(
        jnp.concatenate([attn_low[0], attn_low[3].T], axis=1), (SHARD, CTX), axis=0, tiled=True
    )
    key_full, value_full = jnp.split(key_value, 2, axis=1)
    query_full, output_t = jnp.split(query_output, 2, axis=1)
    output_full = output_t.T
    gate_full, up_full, down_full = (
        lax.all_gather(mlp_low[0], (SHARD, CTX), axis=0, tiled=True),
        lax.all_gather(mlp_low[1], (SHARD, CTX), axis=0, tiled=True),
        lax.all_gather(mlp_low[2], (SHARD, CTX), axis=1, tiled=True),
    )
    tokens_wide = tokens.astype(jnp.float32).reshape(row_total, model_width)
    normed_one, scale_one = normalize(tokens_wide)
    input_one = normed_one.astype(bf_type)
    split_heads = (seq_count, half_len, head_count, HEAD_DIM)
    query_pre = matmul_low(input_one, query_full).reshape(split_heads)
    key_pre = matmul_low(input_one, key_full).reshape(split_heads)
    value_pre = matmul_low(input_one, value_full).reshape(split_heads)
    cosine, sine_table = rope_tables(half_len, HEAD_DIM, offset)
    queries = rotate(query_pre, cosine, sine_table).astype(bf_type)
    keys_rot = rotate(key_pre, cosine, sine_table).astype(bf_type)
    values_low = value_pre.astype(bf_type)
    keys_all, values_all = (
        lax.all_gather(keys_rot, CTX, axis=1, tiled=True),
        lax.all_gather(values_low, CTX, axis=1, tiled=True),
    )
    seq_index = 0
    attended, log_totals = attend_forward(
        queries[seq_index], keys_all[seq_index], values_all[seq_index], lengths[seq_index], offset
    )
    attended_list = [attended]
    log_list = [log_totals]
    attn_out = jnp.stack(attended_list).reshape(row_total, head_cols)
    grad_final = cotangent.astype(jnp.float32).reshape(row_total, model_width) * valid_mask.reshape(
        row_total, 1
    )
    unit = row_total // sum(MID_SPLIT)
    bounds = [0]
    for share in MID_SPLIT:
        bounds.append(bounds[-1] + share * unit)
    pieces = []
    for index in range(len(MID_SPLIT)):
        rows = slice(bounds[index], bounds[index + 1])
        pieces.append(
            middle_rows(
                attn_out[rows], tokens_wide[rows], grad_final[rows],
                output_full, gate_full, up_full, down_full, tp_count,
            )
        )
    grad_gate = sum(piece[6] for piece in pieces)
    grad_up = sum(piece[7] for piece in pieces)
    grad_down = sum(piece[8] for piece in pieces)
    last_sum = pieces[-1][5]
    (grad_gate, grad_up, grad_down), last_sum = lax.optimization_barrier(
        ((grad_gate, grad_up, grad_down), last_sum)
    )
    pieces[-1][5] = last_sum
    mlp_grads = (
        scatter_low(grad_gate, 0),
        scatter_low(grad_up, 0),
        scatter_low(grad_down, 1),
    )
    resid = jnp.concatenate([piece[0] for piece in pieces], axis=0)
    branch_two_part = jnp.concatenate([piece[1] for piece in pieces], axis=0)
    grad_resid_parts, grad_attn_parts, grad_wout = [], [], 0.0
    for index, piece in enumerate(pieces):
        grad_resid_part = piece[4] + norm_back(piece[2], piece[3], piece[5].astype(jnp.float32))
        resid_low = grad_resid_part.astype(bf_type)
        grad_wout = grad_wout + jnp.einsum(
            "rc,rd->cd", attn_out[bounds[index]:bounds[index + 1]], resid_low,
            preferred_element_type=jnp.float32,
        )
        grad_attn_parts.append(
            jnp.einsum("rd,cd->rc", resid_low, output_full, preferred_element_type=jnp.float32)
        )
        grad_resid_parts.append(grad_resid_part)
    grad_resid = jnp.concatenate(grad_resid_parts, axis=0)
    grad_attn = jnp.concatenate(grad_attn_parts, axis=0).astype(bf_type).reshape(split_heads)
    branch_two_part, grad_attn = lax.optimization_barrier((branch_two_part, grad_attn))
    final_sum = resid + tp_psum(branch_two_part, tp_count).astype(jnp.float32)
    seq_index = 0
    grad_queries, grad_keys_seq, grad_values_seq = attend_backward(
        queries[seq_index],
        keys_all[seq_index],
        values_all[seq_index],
        lengths[seq_index],
        offset,
        log_list[seq_index],
        grad_attn[seq_index],
    )
    query_grads = [grad_queries]
    key_grads = [grad_keys_seq]
    value_grads = [grad_values_seq]
    grad_keys, grad_values = (
        exchange_scatter(
            jnp.stack(key_grads).reshape((ctx_count, half_len, head_count, HEAD_DIM)), CTX, ctx_count
        ).reshape(split_heads),
        exchange_scatter(
            jnp.stack(value_grads).reshape((ctx_count, half_len, head_count, HEAD_DIM)), CTX, ctx_count
        ).reshape(split_heads),
    )
    query_grad = jnp.stack(query_grads)
    q_parts, k_parts, v_parts, token_parts = [], [], [], []
    for index in range(len(MID_SPLIT)):
        low_row, high_row = bounds[index], bounds[index + 1]
        count = high_row - low_row
        cos_part, sin_part = cosine[low_row:high_row], sine_table[low_row:high_row]
        q_part = rotate_back(query_grad[:, low_row:high_row], cos_part, sin_part)
        q_part = q_part.astype(bf_type).reshape(count, head_cols)
        k_part = rotate_back(grad_keys[:, low_row:high_row], cos_part, sin_part)
        k_part = k_part.astype(bf_type).reshape(count, head_cols)
        v_part = grad_values[:, low_row:high_row].astype(bf_type).reshape(count, head_cols)
        input_part = (
            jnp.einsum("rc,dc->rd", q_part, query_full, preferred_element_type=jnp.float32)
            + jnp.einsum("rc,dc->rd", k_part, key_full, preferred_element_type=jnp.float32)
            + jnp.einsum("rc,dc->rd", v_part, value_full, preferred_element_type=jnp.float32)
        )
        input_part = tp_psum(input_part, tp_count).astype(jnp.float32)
        token_parts.append(
            grad_resid[low_row:high_row]
            + norm_back(normed_one[low_row:high_row], scale_one[low_row:high_row], input_part)
        )
        q_parts.append(q_part)
        k_parts.append(k_part)
        v_parts.append(v_part)
    grad_q_pre = jnp.concatenate(q_parts, axis=0)
    grad_k_pre = jnp.concatenate(k_parts, axis=0)
    grad_v_pre = jnp.concatenate(v_parts, axis=0)
    grad_wq = jnp.einsum("rd,rc->dc", input_one, grad_q_pre, preferred_element_type=jnp.float32)
    grad_wk = jnp.einsum("rd,rc->dc", input_one, grad_k_pre, preferred_element_type=jnp.float32)
    grad_wv = jnp.einsum("rd,rc->dc", input_one, grad_v_pre, preferred_element_type=jnp.float32)
    qkv_grads = jnp.split(
        scatter_low(jnp.concatenate([grad_wq, grad_wk, grad_wv], axis=1), 0), 3, axis=1
    )
    attn_grads = (qkv_grads[0], qkv_grads[1], qkv_grads[2], scatter_low(grad_wout, 1))
    grad_tokens = jnp.concatenate(token_parts, axis=0)
    output = final_sum.astype(bf_type).reshape(seq_count, half_len, model_width)
    grad_tokens = grad_tokens.reshape(seq_count, half_len, model_width)
    return (
        output,
        grad_tokens,
        attn_grads[0],
        attn_grads[1],
        attn_grads[2],
        attn_grads[3],
        mlp_grads[0],
        mlp_grads[1],
        mlp_grads[2],
    )


def solution(mesh):
    return jax.shard_map(
        functools.partial(body, mesh.shape[TP], mesh.shape[CTX]),
        mesh=mesh,
        in_specs=(
            P(SHARD, CTX, None),
            P(SHARD),
            P(SHARD, CTX, None),
            P((SHARD, CTX), TP),
            P((SHARD, CTX), TP),
            P((SHARD, CTX), TP),
            P(TP, (SHARD, CTX)),
            P((SHARD, CTX), TP),
            P((SHARD, CTX), TP),
            P(TP, (SHARD, CTX)),
        ),
        out_specs=(
            P(SHARD, CTX, None),
            P(SHARD, CTX, None),
            P((SHARD, CTX), TP),
            P((SHARD, CTX), TP),
            P((SHARD, CTX), TP),
            P(TP, (SHARD, CTX)),
            P((SHARD, CTX), TP),
            P((SHARD, CTX), TP),
            P(TP, (SHARD, CTX)),
        ),
        check_vma=False,
    )
```

```python
import functools

import jax
import jax.numpy as jnp
from jax import lax
from jax.sharding import PartitionSpec as P

SHARD, CTX, TP = "shard", "ctx", "tp"

HEAD_DIM = 128


EPSILON = 1e-05


def normalize(values):
    center = values - jnp.mean(values, axis=-1, keepdims=True)
    inv_scale = lax.rsqrt(jnp.mean(center * center, axis=-1, keepdims=True) + EPSILON)
    return (center * inv_scale, inv_scale)


def norm_back(normed, inv_scale, upstream):
    first_mean = jnp.mean(upstream, axis=-1, keepdims=True)
    second_mean = jnp.mean(upstream * normed, axis=-1, keepdims=True)
    return inv_scale * (upstream - first_mean - normed * second_mean)


def rope_tables(row_count, head_size, offset):
    positions = (jnp.arange(row_count) + offset).astype(jnp.float32)
    inverse = 10000.0 ** (-(jnp.arange(head_size // 2).astype(jnp.float32) * 2.0) / head_size)
    angles = positions[:, None] * inverse[None, :]
    angles = jnp.concatenate([angles, angles], axis=-1)
    return (jnp.cos(angles)[:, None, :], jnp.sin(angles)[:, None, :])


def turn_half(values):
    half_dim = values.shape[-1] // 2
    return jnp.concatenate([-values[..., half_dim:], values[..., :half_dim]], axis=-1)


def rotate(values, cosine, sine_table):
    return values * cosine + turn_half(values) * sine_table


def rotate_back(values, cosine, sine_table):
    return values * cosine - turn_half(values) * sine_table


def score_block(query_rows, keys_seq, length, row_start):
    block_rows = query_rows.shape[0]
    key_pos = jnp.arange(keys_seq.shape[0])
    row_pos = row_start + jnp.arange(block_rows)
    scores = jnp.einsum(
        "qhd,khd->hqk", query_rows, keys_seq, preferred_element_type=jnp.float32
    ) * HEAD_DIM ** (-0.5)
    allowed = (key_pos[None, :] <= row_pos[:, None]) & (key_pos[None, :] < length)
    return jnp.where(allowed[None], scores, -1e30)


def attend_forward(queries_seq, keys_seq, values_seq, length, offset):
    half_len, head_count, head_size = queries_seq.shape
    block_rows = min(512, half_len)
    block_count = half_len // block_rows
    grouped = queries_seq.reshape(block_count, block_rows, head_count, head_size)

    def one_block(paired):
        query_rows, block_index = paired
        scores = score_block(query_rows, keys_seq, length, offset + block_index * block_rows)
        row_peak = jnp.max(scores, axis=-1, keepdims=True)
        log_total = jnp.log(jnp.sum(jnp.exp(scores - row_peak), axis=-1, keepdims=True)) + row_peak
        probability = jnp.exp(scores - log_total).astype(jnp.bfloat16)
        attended = jnp.einsum(
            "hqk,khd->qhd", probability, values_seq, preferred_element_type=jnp.float32
        )
        return (attended.astype(jnp.bfloat16), log_total[..., 0])

    attended, log_totals = lax.map(one_block, (grouped, jnp.arange(block_count)))
    return (attended.reshape(half_len, head_count, head_size), log_totals)


def attend_backward(queries_seq, keys_seq, values_seq, length, offset, log_totals, grad_seq):
    half_len, head_count, head_size = queries_seq.shape
    block_rows = min(512, half_len)
    block_count = half_len // block_rows
    score_scale = HEAD_DIM ** (-0.5)
    grouped = queries_seq.reshape(block_count, block_rows, head_count, head_size)
    grad_grouped = grad_seq.reshape(block_count, block_rows, head_count, head_size)

    def one_block(carried, paired):
        query_rows, grad_rows, log_rows, block_index = paired
        scores = score_block(query_rows, keys_seq, length, offset + block_index * block_rows)
        probability = jnp.exp(scores - log_rows[..., None])
        prob_low = probability.astype(jnp.bfloat16)
        grad_prob = jnp.einsum(
            "qhd,khd->hqk", grad_rows, values_seq, preferred_element_type=jnp.float32
        )
        inner_sum = jnp.sum(probability * grad_prob, axis=-1, keepdims=True)
        grad_scores = (probability * (grad_prob - inner_sum)).astype(jnp.bfloat16)
        grad_query_rows = (
            jnp.einsum("hqk,khd->qhd", grad_scores, keys_seq, preferred_element_type=jnp.float32)
            * score_scale
        )
        key_part = (
            jnp.einsum("hqk,qhd->khd", grad_scores, query_rows, preferred_element_type=jnp.float32)
            * score_scale
        )
        value_part = jnp.einsum(
            "hqk,qhd->khd", prob_low, grad_rows, preferred_element_type=jnp.float32
        )
        return ((carried[0] + key_part, carried[1] + value_part), grad_query_rows)

    empty = jnp.zeros(keys_seq.shape, jnp.float32)
    sums, grad_queries = lax.scan(
        one_block, (empty, empty), (grouped, grad_grouped, log_totals, jnp.arange(block_count))
    )
    return (grad_queries.reshape(half_len, head_count, head_size), sums[0], sums[1])


def tp_psum(part, count):
    me = lax.axis_index(TP)
    low_part = part.astype(jnp.bfloat16)
    rows = part.shape[0] // count
    chunks = low_part.reshape((count, rows) + part.shape[1:])
    total = lax.dynamic_index_in_dim(chunks, me, 0, keepdims=False).astype(jnp.float32)
    for shift in range(1, count):
        pairs = [(i, (i + shift) % count) for i in range(count)]
        piece = lax.dynamic_index_in_dim(chunks, (me + shift) % count, 0, keepdims=False)
        total = total + lax.ppermute(piece, TP, pairs).astype(jnp.float32)
    reduced = total.astype(jnp.bfloat16)
    gathered = jnp.zeros(low_part.shape, jnp.bfloat16)
    gathered = lax.dynamic_update_slice_in_dim(gathered, reduced, me * rows, 0)
    for shift in range(1, count):
        pairs = [(i, (i + shift) % count) for i in range(count)]
        got = lax.ppermute(reduced, TP, pairs)
        gathered = lax.dynamic_update_slice_in_dim(
            gathered, got, ((me + count - shift) % count) * rows, 0
        )
    return gathered


def exchange_scatter(blocks, axis, count):
    me = lax.axis_index(axis)
    total = lax.dynamic_index_in_dim(blocks, me, 0, keepdims=False)
    for shift in range(1, count):
        pairs = [(i, (i + shift) % count) for i in range(count)]
        piece = lax.dynamic_index_in_dim(blocks, (me + shift) % count, 0, keepdims=False)
        total = total + lax.ppermute(piece, axis, pairs)
    return total


def scatter_low(grad, dim):
    summed = lax.psum_scatter(
        grad.astype(jnp.bfloat16), (SHARD, CTX), scatter_dimension=dim, tiled=True
    )
    return summed.astype(jnp.float32)


def matmul_low(left, right):
    return jnp.dot(left, right, preferred_element_type=jnp.float32)


MID_SPLIT = (3, 5)


def middle_rows(attn_rows, tokens_rows, grad_final, output_full, gate_full, up_full, down_full, tp_count, before):
    bf_type = jnp.bfloat16
    resid = tokens_rows + tp_psum(matmul_low(attn_rows, output_full), tp_count).astype(jnp.float32)
    normed_two, scale_two = normalize(resid)
    input_two = normed_two.astype(bf_type)
    gate_proj = matmul_low(input_two, gate_full)
    up_proj = matmul_low(input_two, up_full)
    gate_sigmoid = jax.nn.sigmoid(gate_proj)
    hidden = (gate_proj * gate_sigmoid * up_proj).astype(bf_type)
    grad_branch = grad_final.astype(bf_type)
    grad_hidden = jnp.einsum(
        "rd,fd->rf", grad_branch, down_full, preferred_element_type=jnp.float32
    )
    grad_gate_act = (
        grad_hidden * up_proj * gate_sigmoid * (1.0 + gate_proj * (1.0 - gate_sigmoid))
    ).astype(bf_type)
    grad_up_act = (grad_hidden * gate_proj * gate_sigmoid).astype(bf_type)
    grad_input_two = jnp.einsum(
        "rf,df->rd", grad_gate_act, gate_full, preferred_element_type=jnp.float32
    ) + jnp.einsum("rf,df->rd", grad_up_act, up_full, preferred_element_type=jnp.float32)
    branch_two = matmul_low(hidden, down_full)
    grad_down = jnp.einsum("rf,rd->fd", hidden, grad_branch, preferred_element_type=jnp.float32)
    grad_gate = jnp.einsum(
        "rd,rf->df", input_two, grad_gate_act, preferred_element_type=jnp.float32
    )
    grad_up = jnp.einsum("rd,rf->df", input_two, grad_up_act, preferred_element_type=jnp.float32)
    if before is not None:
        grad_input_two, _ = lax.optimization_barrier((grad_input_two, before))
    grad_input_two = lax.psum(grad_input_two.astype(bf_type), TP)
    return [
        resid, branch_two, normed_two, scale_two, grad_final, grad_input_two,
        grad_gate, grad_up, grad_down,
    ]


def body(tp_count, ctx_count, *args):
    return block(tp_count, ctx_count, *args)


def block(tp_count, ctx_count, tokens, lengths, cotangent, w_query, w_key, w_value, w_output, w_gate, w_up, w_down):
    seq_count, half_len, model_width = tokens.shape
    head_cols = w_query.shape[1]
    head_count = head_cols // HEAD_DIM
    row_total = seq_count * half_len
    offset = lax.axis_index(CTX) * half_len
    positions = offset + jnp.arange(half_len)
    valid_mask = (positions[None, :] < lengths[:, None]).astype(jnp.float32)
    bf_type = jnp.bfloat16
    attn_low = (
        w_query.astype(bf_type),
        w_key.astype(bf_type),
        w_value.astype(bf_type),
        w_output.astype(bf_type),
    )
    mlp_low = (w_gate.astype(bf_type), w_up.astype(bf_type), w_down.astype(bf_type))
    key_value = lax.all_gather(
        jnp.concatenate([attn_low[1], attn_low[2]], axis=1), (SHARD, CTX), axis=0, tiled=True
    )
    query_output = lax.all_gather(
        jnp.concatenate([attn_low[0], attn_low[3].T], axis=1), (SHARD, CTX), axis=0, tiled=True
    )
    key_full, value_full = jnp.split(key_value, 2, axis=1)
    query_full, output_t = jnp.split(query_output, 2, axis=1)
    output_full = output_t.T
    gate_full, up_full, down_full = (
        lax.all_gather(mlp_low[0], (SHARD, CTX), axis=0, tiled=True),
        lax.all_gather(mlp_low[1], (SHARD, CTX), axis=0, tiled=True),
        lax.all_gather(mlp_low[2], (SHARD, CTX), axis=1, tiled=True),
    )
    tokens_wide = tokens.astype(jnp.float32).reshape(row_total, model_width)
    normed_one, scale_one = normalize(tokens_wide)
    input_one = normed_one.astype(bf_type)
    split_heads = (seq_count, half_len, head_count, HEAD_DIM)
    query_pre = matmul_low(input_one, query_full).reshape(split_heads)
    key_pre = matmul_low(input_one, key_full).reshape(split_heads)
    value_pre = matmul_low(input_one, value_full).reshape(split_heads)
    cosine, sine_table = rope_tables(half_len, HEAD_DIM, offset)
    queries = rotate(query_pre, cosine, sine_table).astype(bf_type)
    keys_rot = rotate(key_pre, cosine, sine_table).astype(bf_type)
    values_low = value_pre.astype(bf_type)
    keys_all, values_all = (
        lax.all_gather(keys_rot, CTX, axis=1, tiled=True),
        lax.all_gather(values_low, CTX, axis=1, tiled=True),
    )
    seq_index = 0
    attended, log_totals = attend_forward(
        queries[seq_index], keys_all[seq_index], values_all[seq_index], lengths[seq_index], offset
    )
    attended_list = [attended]
    log_list = [log_totals]
    attn_out = jnp.stack(attended_list).reshape(row_total, head_cols)
    grad_final = cotangent.astype(jnp.float32).reshape(row_total, model_width) * valid_mask.reshape(
        row_total, 1
    )
    unit = row_total // sum(MID_SPLIT)
    bounds = [0]
    for share in MID_SPLIT:
        bounds.append(bounds[-1] + share * unit)
    pieces = []
    for index in range(len(MID_SPLIT)):
        rows = slice(bounds[index], bounds[index + 1])
        pieces.append(
            middle_rows(
                attn_out[rows], tokens_wide[rows], grad_final[rows],
                output_full, gate_full, up_full, down_full, tp_count,
                pieces[-1][5] if pieces else None,
            )
        )
    grad_gate = sum(piece[6] for piece in pieces)
    grad_up = sum(piece[7] for piece in pieces)
    grad_down = sum(piece[8] for piece in pieces)
    last_sum = pieces[-1][5]
    (grad_gate, grad_up, grad_down), last_sum = lax.optimization_barrier(
        ((grad_gate, grad_up, grad_down), last_sum)
    )
    pieces[-1][5] = last_sum
    mlp_grads = (
        scatter_low(grad_gate, 0),
        scatter_low(grad_up, 0),
        scatter_low(grad_down, 1),
    )
    resid = jnp.concatenate([piece[0] for piece in pieces], axis=0)
    branch_two_part = jnp.concatenate([piece[1] for piece in pieces], axis=0)
    grad_resid_parts, grad_attn_parts, grad_wout = [], [], 0.0
    for index, piece in enumerate(pieces):
        grad_resid_part = piece[4] + norm_back(piece[2], piece[3], piece[5].astype(jnp.float32))
        resid_low = grad_resid_part.astype(bf_type)
        grad_wout = grad_wout + jnp.einsum(
            "rc,rd->cd", attn_out[bounds[index]:bounds[index + 1]], resid_low,
            preferred_element_type=jnp.float32,
        )
        grad_attn_parts.append(
            jnp.einsum("rd,cd->rc", resid_low, output_full, preferred_element_type=jnp.float32)
        )
        grad_resid_parts.append(grad_resid_part)
    grad_resid = jnp.concatenate(grad_resid_parts, axis=0)
    grad_attn = jnp.concatenate(grad_attn_parts, axis=0).astype(bf_type).reshape(split_heads)
    branch_two_part, grad_attn = lax.optimization_barrier((branch_two_part, grad_attn))
    final_sum = resid + lax.psum(branch_two_part.astype(bf_type), TP).astype(jnp.float32)
    seq_index = 0
    grad_queries, grad_keys_seq, grad_values_seq = attend_backward(
        queries[seq_index],
        keys_all[seq_index],
        values_all[seq_index],
        lengths[seq_index],
        offset,
        log_list[seq_index],
        grad_attn[seq_index],
    )
    query_grads = [grad_queries]
    key_grads = [grad_keys_seq]
    value_grads = [grad_values_seq]
    grad_keys, grad_values = (
        exchange_scatter(
            jnp.stack(key_grads).reshape((ctx_count, half_len, head_count, HEAD_DIM)), CTX, ctx_count
        ).reshape(split_heads),
        exchange_scatter(
            jnp.stack(value_grads).reshape((ctx_count, half_len, head_count, HEAD_DIM)), CTX, ctx_count
        ).reshape(split_heads),
    )
    query_grad = jnp.stack(query_grads)
    q_parts, k_parts, v_parts, token_parts = [], [], [], []
    for index in range(len(MID_SPLIT)):
        low_row, high_row = bounds[index], bounds[index + 1]
        count = high_row - low_row
        cos_part, sin_part = cosine[low_row:high_row], sine_table[low_row:high_row]
        q_part = rotate_back(query_grad[:, low_row:high_row], cos_part, sin_part)
        q_part = q_part.astype(bf_type).reshape(count, head_cols)
        k_part = rotate_back(grad_keys[:, low_row:high_row], cos_part, sin_part)
        k_part = k_part.astype(bf_type).reshape(count, head_cols)
        v_part = grad_values[:, low_row:high_row].astype(bf_type).reshape(count, head_cols)
        input_part = (
            jnp.einsum("rc,dc->rd", q_part, query_full, preferred_element_type=jnp.float32)
            + jnp.einsum("rc,dc->rd", k_part, key_full, preferred_element_type=jnp.float32)
            + jnp.einsum("rc,dc->rd", v_part, value_full, preferred_element_type=jnp.float32)
        )
        input_part = tp_psum(input_part, tp_count).astype(jnp.float32)
        token_parts.append(
            grad_resid[low_row:high_row]
            + norm_back(normed_one[low_row:high_row], scale_one[low_row:high_row], input_part)
        )
        q_parts.append(q_part)
        k_parts.append(k_part)
        v_parts.append(v_part)
    grad_q_pre = jnp.concatenate(q_parts, axis=0)
    grad_k_pre = jnp.concatenate(k_parts, axis=0)
    grad_v_pre = jnp.concatenate(v_parts, axis=0)
    grad_wq = jnp.einsum("rd,rc->dc", input_one, grad_q_pre, preferred_element_type=jnp.float32)
    grad_wk = jnp.einsum("rd,rc->dc", input_one, grad_k_pre, preferred_element_type=jnp.float32)
    grad_wv = jnp.einsum("rd,rc->dc", input_one, grad_v_pre, preferred_element_type=jnp.float32)
    qkv_grads = jnp.split(
        scatter_low(jnp.concatenate([grad_wq, grad_wk, grad_wv], axis=1), 0), 3, axis=1
    )
    attn_grads = (qkv_grads[0], qkv_grads[1], qkv_grads[2], scatter_low(grad_wout, 1))
    grad_tokens = jnp.concatenate(token_parts, axis=0)
    output = final_sum.astype(bf_type).reshape(seq_count, half_len, model_width)
    grad_tokens = grad_tokens.reshape(seq_count, half_len, model_width)
    return (
        output,
        grad_tokens,
        attn_grads[0],
        attn_grads[1],
        attn_grads[2],
        attn_grads[3],
        mlp_grads[0],
        mlp_grads[1],
        mlp_grads[2],
    )


def solution(mesh):
    return jax.shard_map(
        functools.partial(body, mesh.shape[TP], mesh.shape[CTX]),
        mesh=mesh,
        in_specs=(
            P(SHARD, CTX, None),
            P(SHARD),
            P(SHARD, CTX, None),
            P((SHARD, CTX), TP),
            P((SHARD, CTX), TP),
            P((SHARD, CTX), TP),
            P(TP, (SHARD, CTX)),
            P((SHARD, CTX), TP),
            P((SHARD, CTX), TP),
            P(TP, (SHARD, CTX)),
        ),
        out_specs=(
            P(SHARD, CTX, None),
            P(SHARD, CTX, None),
            P((SHARD, CTX), TP),
            P((SHARD, CTX), TP),
            P((SHARD, CTX), TP),
            P(TP, (SHARD, CTX)),
            P((SHARD, CTX), TP),
            P((SHARD, CTX), TP),
            P(TP, (SHARD, CTX)),
        ),
        check_vma=False,
    )
```

```python
import functools

import jax
import jax.numpy as jnp
from jax import lax
from jax.sharding import PartitionSpec as P

SHARD, CTX, TP = "shard", "ctx", "tp"

HEAD_DIM = 128


EPSILON = 1e-05


def normalize(values):
    center = values - jnp.mean(values, axis=-1, keepdims=True)
    inv_scale = lax.rsqrt(jnp.mean(center * center, axis=-1, keepdims=True) + EPSILON)
    return (center * inv_scale, inv_scale)


def norm_back(normed, inv_scale, upstream):
    first_mean = jnp.mean(upstream, axis=-1, keepdims=True)
    second_mean = jnp.mean(upstream * normed, axis=-1, keepdims=True)
    return inv_scale * (upstream - first_mean - normed * second_mean)


def rope_tables(row_count, head_size, offset):
    positions = (jnp.arange(row_count) + offset).astype(jnp.float32)
    inverse = 10000.0 ** (-(jnp.arange(head_size // 2).astype(jnp.float32) * 2.0) / head_size)
    angles = positions[:, None] * inverse[None, :]
    angles = jnp.concatenate([angles, angles], axis=-1)
    return (jnp.cos(angles)[:, None, :], jnp.sin(angles)[:, None, :])


def turn_half(values):
    half_dim = values.shape[-1] // 2
    return jnp.concatenate([-values[..., half_dim:], values[..., :half_dim]], axis=-1)


def rotate(values, cosine, sine_table):
    return values * cosine + turn_half(values) * sine_table


def rotate_back(values, cosine, sine_table):
    return values * cosine - turn_half(values) * sine_table


def score_block(query_rows, keys_seq, length, row_start):
    block_rows = query_rows.shape[0]
    key_pos = jnp.arange(keys_seq.shape[0])
    row_pos = row_start + jnp.arange(block_rows)
    scores = jnp.einsum(
        "qhd,khd->hqk", query_rows, keys_seq, preferred_element_type=jnp.float32
    ) * HEAD_DIM ** (-0.5)
    allowed = (key_pos[None, :] <= row_pos[:, None]) & (key_pos[None, :] < length)
    return jnp.where(allowed[None], scores, -1e30)


def attend_forward(queries_seq, keys_seq, values_seq, length, offset):
    half_len, head_count, head_size = queries_seq.shape
    block_rows = min(512, half_len)
    block_count = half_len // block_rows
    grouped = queries_seq.reshape(block_count, block_rows, head_count, head_size)

    def one_block(paired):
        query_rows, block_index = paired
        scores = score_block(query_rows, keys_seq, length, offset + block_index * block_rows)
        row_peak = jnp.max(scores, axis=-1, keepdims=True)
        log_total = jnp.log(jnp.sum(jnp.exp(scores - row_peak), axis=-1, keepdims=True)) + row_peak
        probability = jnp.exp(scores - log_total).astype(jnp.bfloat16)
        attended = jnp.einsum(
            "hqk,khd->qhd", probability, values_seq, preferred_element_type=jnp.float32
        )
        return (attended.astype(jnp.bfloat16), log_total[..., 0])

    attended, log_totals = lax.map(one_block, (grouped, jnp.arange(block_count)))
    return (attended.reshape(half_len, head_count, head_size), log_totals)


def attend_backward(queries_seq, keys_seq, values_seq, length, offset, log_totals, grad_seq):
    half_len, head_count, head_size = queries_seq.shape
    block_rows = min(512, half_len)
    block_count = half_len // block_rows
    score_scale = HEAD_DIM ** (-0.5)
    grouped = queries_seq.reshape(block_count, block_rows, head_count, head_size)
    grad_grouped = grad_seq.reshape(block_count, block_rows, head_count, head_size)

    def one_block(carried, paired):
        query_rows, grad_rows, log_rows, block_index = paired
        scores = score_block(query_rows, keys_seq, length, offset + block_index * block_rows)
        probability = jnp.exp(scores - log_rows[..., None])
        prob_low = probability.astype(jnp.bfloat16)
        grad_prob = jnp.einsum(
            "qhd,khd->hqk", grad_rows, values_seq, preferred_element_type=jnp.float32
        )
        inner_sum = jnp.sum(probability * grad_prob, axis=-1, keepdims=True)
        grad_scores = (probability * (grad_prob - inner_sum)).astype(jnp.bfloat16)
        grad_query_rows = (
            jnp.einsum("hqk,khd->qhd", grad_scores, keys_seq, preferred_element_type=jnp.float32)
            * score_scale
        )
        key_part = (
            jnp.einsum("hqk,qhd->khd", grad_scores, query_rows, preferred_element_type=jnp.float32)
            * score_scale
        )
        value_part = jnp.einsum(
            "hqk,qhd->khd", prob_low, grad_rows, preferred_element_type=jnp.float32
        )
        return ((carried[0] + key_part, carried[1] + value_part), grad_query_rows)

    empty = jnp.zeros(keys_seq.shape, jnp.float32)
    sums, grad_queries = lax.scan(
        one_block, (empty, empty), (grouped, grad_grouped, log_totals, jnp.arange(block_count))
    )
    return (grad_queries.reshape(half_len, head_count, head_size), sums[0], sums[1])


def tp_psum(part, count):
    me = lax.axis_index(TP)
    low_part = part.astype(jnp.bfloat16)
    rows = part.shape[0] // count
    chunks = low_part.reshape((count, rows) + part.shape[1:])
    total = lax.dynamic_index_in_dim(chunks, me, 0, keepdims=False).astype(jnp.float32)
    for shift in range(1, count):
        pairs = [(i, (i + shift) % count) for i in range(count)]
        piece = lax.dynamic_index_in_dim(chunks, (me + shift) % count, 0, keepdims=False)
        total = total + lax.ppermute(piece, TP, pairs).astype(jnp.float32)
    reduced = total.astype(jnp.bfloat16)
    gathered = jnp.zeros(low_part.shape, jnp.bfloat16)
    gathered = lax.dynamic_update_slice_in_dim(gathered, reduced, me * rows, 0)
    for shift in range(1, count):
        pairs = [(i, (i + shift) % count) for i in range(count)]
        got = lax.ppermute(reduced, TP, pairs)
        gathered = lax.dynamic_update_slice_in_dim(
            gathered, got, ((me + count - shift) % count) * rows, 0
        )
    return gathered


def exchange_scatter(blocks, axis, count):
    me = lax.axis_index(axis)
    total = lax.dynamic_index_in_dim(blocks, me, 0, keepdims=False)
    for shift in range(1, count):
        pairs = [(i, (i + shift) % count) for i in range(count)]
        piece = lax.dynamic_index_in_dim(blocks, (me + shift) % count, 0, keepdims=False)
        total = total + lax.ppermute(piece, axis, pairs)
    return total


def scatter_low(grad, dim):
    summed = lax.psum_scatter(
        grad.astype(jnp.bfloat16), (SHARD, CTX), scatter_dimension=dim, tiled=True
    )
    return summed.astype(jnp.float32)


def matmul_low(left, right):
    return jnp.dot(left, right, preferred_element_type=jnp.float32)


MID_SPLIT = (3, 5)


def middle_rows(attn_rows, tokens_rows, grad_final, output_full, gate_full, up_full, down_full, tp_count, before):
    bf_type = jnp.bfloat16
    resid = tokens_rows + tp_psum(matmul_low(attn_rows, output_full), tp_count).astype(jnp.float32)
    normed_two, scale_two = normalize(resid)
    input_two = normed_two.astype(bf_type)
    gate_proj = matmul_low(input_two, gate_full)
    up_proj = matmul_low(input_two, up_full)
    gate_sigmoid = jax.nn.sigmoid(gate_proj)
    hidden = (gate_proj * gate_sigmoid * up_proj).astype(bf_type)
    grad_branch = grad_final.astype(bf_type)
    grad_hidden = jnp.einsum(
        "rd,fd->rf", grad_branch, down_full, preferred_element_type=jnp.float32
    )
    grad_gate_act = (
        grad_hidden * up_proj * gate_sigmoid * (1.0 + gate_proj * (1.0 - gate_sigmoid))
    ).astype(bf_type)
    grad_up_act = (grad_hidden * gate_proj * gate_sigmoid).astype(bf_type)
    grad_input_two = jnp.einsum(
        "rf,df->rd", grad_gate_act, gate_full, preferred_element_type=jnp.float32
    ) + jnp.einsum("rf,df->rd", grad_up_act, up_full, preferred_element_type=jnp.float32)
    branch_two = matmul_low(hidden, down_full)
    grad_down = jnp.einsum("rd,rf->df", grad_branch, hidden, preferred_element_type=jnp.float32)
    grad_gate = jnp.einsum(
        "rd,rf->df", input_two, grad_gate_act, preferred_element_type=jnp.float32
    )
    grad_up = jnp.einsum("rd,rf->df", input_two, grad_up_act, preferred_element_type=jnp.float32)
    if before is not None:
        grad_input_two, _ = lax.optimization_barrier((grad_input_two, before))
    grad_input_two = lax.psum(grad_input_two.astype(bf_type), TP)
    return [
        resid, branch_two, normed_two, scale_two, grad_final, grad_input_two,
        grad_gate, grad_up, grad_down,
    ]


def body(tp_count, ctx_count, *args):
    return block(tp_count, ctx_count, *args)


def block(tp_count, ctx_count, tokens, lengths, cotangent, w_query, w_key, w_value, w_output, w_gate, w_up, w_down):
    seq_count, half_len, model_width = tokens.shape
    head_cols = w_query.shape[1]
    head_count = head_cols // HEAD_DIM
    row_total = seq_count * half_len
    offset = lax.axis_index(CTX) * half_len
    positions = offset + jnp.arange(half_len)
    valid_mask = (positions[None, :] < lengths[:, None]).astype(jnp.float32)
    bf_type = jnp.bfloat16
    attn_low = (
        w_query.astype(bf_type),
        w_key.astype(bf_type),
        w_value.astype(bf_type),
        w_output.astype(bf_type),
    )
    mlp_low = (w_gate.astype(bf_type), w_up.astype(bf_type), w_down.astype(bf_type))
    key_value = lax.all_gather(
        jnp.concatenate([attn_low[1], attn_low[2]], axis=1), (SHARD, CTX), axis=0, tiled=True
    )
    query_output = lax.all_gather(
        jnp.concatenate([attn_low[0], attn_low[3].T], axis=1), (SHARD, CTX), axis=0, tiled=True
    )
    key_full, value_full = jnp.split(key_value, 2, axis=1)
    query_full, output_t = jnp.split(query_output, 2, axis=1)
    output_full = output_t.T
    gate_full, up_full, down_full = (
        lax.all_gather(mlp_low[0], (SHARD, CTX), axis=0, tiled=True),
        lax.all_gather(mlp_low[1], (SHARD, CTX), axis=0, tiled=True),
        lax.all_gather(mlp_low[2], (SHARD, CTX), axis=1, tiled=True),
    )
    tokens_wide = tokens.astype(jnp.float32).reshape(row_total, model_width)
    normed_one, scale_one = normalize(tokens_wide)
    input_one = normed_one.astype(bf_type)
    split_heads = (seq_count, half_len, head_count, HEAD_DIM)
    query_pre = matmul_low(input_one, query_full).reshape(split_heads)
    key_pre = matmul_low(input_one, key_full).reshape(split_heads)
    value_pre = matmul_low(input_one, value_full).reshape(split_heads)
    cosine, sine_table = rope_tables(half_len, HEAD_DIM, offset)
    queries = rotate(query_pre, cosine, sine_table).astype(bf_type)
    keys_rot = rotate(key_pre, cosine, sine_table).astype(bf_type)
    values_low = value_pre.astype(bf_type)
    keys_all, values_all = (
        lax.all_gather(keys_rot, CTX, axis=1, tiled=True),
        lax.all_gather(values_low, CTX, axis=1, tiled=True),
    )
    seq_index = 0
    attended, log_totals = attend_forward(
        queries[seq_index], keys_all[seq_index], values_all[seq_index], lengths[seq_index], offset
    )
    attended_list = [attended]
    log_list = [log_totals]
    attn_out = jnp.stack(attended_list).reshape(row_total, head_cols)
    grad_final = cotangent.astype(jnp.float32).reshape(row_total, model_width) * valid_mask.reshape(
        row_total, 1
    )
    unit = row_total // sum(MID_SPLIT)
    bounds = [0]
    for share in MID_SPLIT:
        bounds.append(bounds[-1] + share * unit)
    pieces = []
    for index in range(len(MID_SPLIT)):
        rows = slice(bounds[index], bounds[index + 1])
        pieces.append(
            middle_rows(
                attn_out[rows], tokens_wide[rows], grad_final[rows],
                output_full, gate_full, up_full, down_full, tp_count,
                pieces[-1][5] if pieces else None,
            )
        )
    grad_gate = sum(piece[6] for piece in pieces)
    grad_up = sum(piece[7] for piece in pieces)
    grad_down = sum(piece[8] for piece in pieces)
    last_sum = pieces[-1][5]
    (grad_gate, grad_up, grad_down), last_sum = lax.optimization_barrier(
        ((grad_gate, grad_up, grad_down), last_sum)
    )
    pieces[-1][5] = last_sum
    mlp_grads = (
        scatter_low(grad_gate, 0),
        scatter_low(grad_up, 0),
    )
    resid = jnp.concatenate([piece[0] for piece in pieces], axis=0)
    branch_two_part = jnp.concatenate([piece[1] for piece in pieces], axis=0)
    grad_resid_parts, grad_attn_parts, grad_wout = [], [], 0.0
    for index, piece in enumerate(pieces):
        grad_resid_part = piece[4] + norm_back(piece[2], piece[3], piece[5].astype(jnp.float32))
        resid_low = grad_resid_part.astype(bf_type)
        grad_wout = grad_wout + jnp.einsum(
            "rc,rd->cd", attn_out[bounds[index]:bounds[index + 1]], resid_low,
            preferred_element_type=jnp.float32,
        )
        grad_attn_parts.append(
            jnp.einsum("rd,cd->rc", resid_low, output_full, preferred_element_type=jnp.float32)
        )
        grad_resid_parts.append(grad_resid_part)
    grad_resid = jnp.concatenate(grad_resid_parts, axis=0)
    grad_attn = jnp.concatenate(grad_attn_parts, axis=0).astype(bf_type).reshape(split_heads)
    branch_two_part, grad_attn = lax.optimization_barrier((branch_two_part, grad_attn))
    final_sum = resid + lax.psum(branch_two_part.astype(bf_type), TP).astype(jnp.float32)
    seq_index = 0
    grad_queries, grad_keys_seq, grad_values_seq = attend_backward(
        queries[seq_index],
        keys_all[seq_index],
        values_all[seq_index],
        lengths[seq_index],
        offset,
        log_list[seq_index],
        grad_attn[seq_index],
    )
    query_grads = [grad_queries]
    key_grads = [grad_keys_seq]
    value_grads = [grad_values_seq]
    grad_keys, grad_values = (
        exchange_scatter(
            jnp.stack(key_grads).reshape((ctx_count, half_len, head_count, HEAD_DIM)), CTX, ctx_count
        ).reshape(split_heads),
        exchange_scatter(
            jnp.stack(value_grads).reshape((ctx_count, half_len, head_count, HEAD_DIM)), CTX, ctx_count
        ).reshape(split_heads),
    )
    query_grad = jnp.stack(query_grads)
    q_parts, k_parts, v_parts, token_parts = [], [], [], []
    for index in range(len(MID_SPLIT)):
        low_row, high_row = bounds[index], bounds[index + 1]
        count = high_row - low_row
        cos_part, sin_part = cosine[low_row:high_row], sine_table[low_row:high_row]
        q_part = rotate_back(query_grad[:, low_row:high_row], cos_part, sin_part)
        q_part = q_part.astype(bf_type).reshape(count, head_cols)
        k_part = rotate_back(grad_keys[:, low_row:high_row], cos_part, sin_part)
        k_part = k_part.astype(bf_type).reshape(count, head_cols)
        v_part = grad_values[:, low_row:high_row].astype(bf_type).reshape(count, head_cols)
        input_part = (
            jnp.einsum("rc,dc->rd", q_part, query_full, preferred_element_type=jnp.float32)
            + jnp.einsum("rc,dc->rd", k_part, key_full, preferred_element_type=jnp.float32)
            + jnp.einsum("rc,dc->rd", v_part, value_full, preferred_element_type=jnp.float32)
        )
        input_part = tp_psum(input_part, tp_count).astype(jnp.float32)
        token_parts.append(
            grad_resid[low_row:high_row]
            + norm_back(normed_one[low_row:high_row], scale_one[low_row:high_row], input_part)
        )
        q_parts.append(q_part)
        k_parts.append(k_part)
        v_parts.append(v_part)
    grad_q_pre = jnp.concatenate(q_parts, axis=0)
    grad_k_pre = jnp.concatenate(k_parts, axis=0)
    grad_v_pre = jnp.concatenate(v_parts, axis=0)
    grad_wq = jnp.einsum("rd,rc->dc", input_one, grad_q_pre, preferred_element_type=jnp.float32)
    grad_wk = jnp.einsum("rd,rc->dc", input_one, grad_k_pre, preferred_element_type=jnp.float32)
    grad_wv = jnp.einsum("rd,rc->dc", input_one, grad_v_pre, preferred_element_type=jnp.float32)
    down_cols = grad_down.shape[1]
    joined = scatter_low(jnp.concatenate([grad_down, grad_wq, grad_wk, grad_wv], axis=1), 0)
    mlp_grads = mlp_grads + (joined[:, :down_cols].T,)
    qkv_grads = jnp.split(joined[:, down_cols:], 3, axis=1)
    attn_grads = (qkv_grads[0], qkv_grads[1], qkv_grads[2], scatter_low(grad_wout, 1))
    grad_tokens = jnp.concatenate(token_parts, axis=0)
    output = final_sum.astype(bf_type).reshape(seq_count, half_len, model_width)
    grad_tokens = grad_tokens.reshape(seq_count, half_len, model_width)
    return (
        output,
        grad_tokens,
        attn_grads[0],
        attn_grads[1],
        attn_grads[2],
        attn_grads[3],
        mlp_grads[0],
        mlp_grads[1],
        mlp_grads[2],
    )


def solution(mesh):
    return jax.shard_map(
        functools.partial(body, mesh.shape[TP], mesh.shape[CTX]),
        mesh=mesh,
        in_specs=(
            P(SHARD, CTX, None),
            P(SHARD),
            P(SHARD, CTX, None),
            P((SHARD, CTX), TP),
            P((SHARD, CTX), TP),
            P((SHARD, CTX), TP),
            P(TP, (SHARD, CTX)),
            P((SHARD, CTX), TP),
            P((SHARD, CTX), TP),
            P(TP, (SHARD, CTX)),
        ),
        out_specs=(
            P(SHARD, CTX, None),
            P(SHARD, CTX, None),
            P((SHARD, CTX), TP),
            P((SHARD, CTX), TP),
            P((SHARD, CTX), TP),
            P(TP, (SHARD, CTX)),
            P((SHARD, CTX), TP),
            P((SHARD, CTX), TP),
            P(TP, (SHARD, CTX)),
        ),
        check_vma=False,
    )
```

```python
import functools

import jax
import jax.numpy as jnp
from jax import lax
from jax.sharding import PartitionSpec as P

SHARD, CTX, TP = "shard", "ctx", "tp"

HEAD_DIM = 128


EPSILON = 1e-05


def normalize(values):
    center = values - jnp.mean(values, axis=-1, keepdims=True)
    inv_scale = lax.rsqrt(jnp.mean(center * center, axis=-1, keepdims=True) + EPSILON)
    return (center * inv_scale, inv_scale)


def norm_back(normed, inv_scale, upstream):
    first_mean = jnp.mean(upstream, axis=-1, keepdims=True)
    second_mean = jnp.mean(upstream * normed, axis=-1, keepdims=True)
    return inv_scale * (upstream - first_mean - normed * second_mean)


def rope_tables(row_count, head_size, offset):
    positions = (jnp.arange(row_count) + offset).astype(jnp.float32)
    inverse = 10000.0 ** (-(jnp.arange(head_size // 2).astype(jnp.float32) * 2.0) / head_size)
    angles = positions[:, None] * inverse[None, :]
    angles = jnp.concatenate([angles, angles], axis=-1)
    return (jnp.cos(angles)[:, None, :], jnp.sin(angles)[:, None, :])


def turn_half(values):
    half_dim = values.shape[-1] // 2
    return jnp.concatenate([-values[..., half_dim:], values[..., :half_dim]], axis=-1)


def rotate(values, cosine, sine_table):
    return values * cosine + turn_half(values) * sine_table


def rotate_back(values, cosine, sine_table):
    return values * cosine - turn_half(values) * sine_table


def score_block(query_rows, keys_seq, length, row_start):
    block_rows = query_rows.shape[0]
    key_pos = jnp.arange(keys_seq.shape[0])
    row_pos = row_start + jnp.arange(block_rows)
    scores = jnp.einsum(
        "qhd,khd->hqk", query_rows, keys_seq, preferred_element_type=jnp.float32
    ) * HEAD_DIM ** (-0.5)
    allowed = (key_pos[None, :] <= row_pos[:, None]) & (key_pos[None, :] < length)
    return jnp.where(allowed[None], scores, -1e30)


def attend_forward(queries_seq, keys_seq, values_seq, length, offset):
    half_len, head_count, head_size = queries_seq.shape
    block_rows = min(512, half_len)
    block_count = half_len // block_rows
    grouped = queries_seq.reshape(block_count, block_rows, head_count, head_size)

    def one_block(paired):
        query_rows, block_index = paired
        scores = score_block(query_rows, keys_seq, length, offset + block_index * block_rows)
        row_peak = jnp.max(scores, axis=-1, keepdims=True)
        log_total = jnp.log(jnp.sum(jnp.exp(scores - row_peak), axis=-1, keepdims=True)) + row_peak
        probability = jnp.exp(scores - log_total).astype(jnp.bfloat16)
        attended = jnp.einsum(
            "hqk,khd->qhd", probability, values_seq, preferred_element_type=jnp.float32
        )
        return (attended.astype(jnp.bfloat16), log_total[..., 0])

    attended, log_totals = lax.map(one_block, (grouped, jnp.arange(block_count)))
    return (attended.reshape(half_len, head_count, head_size), log_totals)


def attend_backward(queries_seq, keys_seq, values_seq, length, offset, log_totals, grad_seq):
    half_len, head_count, head_size = queries_seq.shape
    block_rows = min(512, half_len)
    block_count = half_len // block_rows
    score_scale = HEAD_DIM ** (-0.5)
    grouped = queries_seq.reshape(block_count, block_rows, head_count, head_size)
    grad_grouped = grad_seq.reshape(block_count, block_rows, head_count, head_size)

    def one_block(carried, paired):
        query_rows, grad_rows, log_rows, block_index = paired
        scores = score_block(query_rows, keys_seq, length, offset + block_index * block_rows)
        probability = jnp.exp(scores - log_rows[..., None])
        prob_low = probability.astype(jnp.bfloat16)
        grad_prob = jnp.einsum(
            "qhd,khd->hqk", grad_rows, values_seq, preferred_element_type=jnp.float32
        )
        inner_sum = jnp.sum(probability * grad_prob, axis=-1, keepdims=True)
        grad_scores = (probability * (grad_prob - inner_sum)).astype(jnp.bfloat16)
        grad_query_rows = (
            jnp.einsum("hqk,khd->qhd", grad_scores, keys_seq, preferred_element_type=jnp.float32)
            * score_scale
        )
        key_part = (
            jnp.einsum("hqk,qhd->khd", grad_scores, query_rows, preferred_element_type=jnp.float32)
            * score_scale
        )
        value_part = jnp.einsum(
            "hqk,qhd->khd", prob_low, grad_rows, preferred_element_type=jnp.float32
        )
        return ((carried[0] + key_part, carried[1] + value_part), grad_query_rows)

    empty = jnp.zeros(keys_seq.shape, jnp.float32)
    sums, grad_queries = lax.scan(
        one_block, (empty, empty), (grouped, grad_grouped, log_totals, jnp.arange(block_count))
    )
    return (grad_queries.reshape(half_len, head_count, head_size), sums[0], sums[1])


def tp_psum(part, count):
    me = lax.axis_index(TP)
    low_part = part.astype(jnp.bfloat16)
    rows = part.shape[0] // count
    chunks = low_part.reshape((count, rows) + part.shape[1:])
    total = lax.dynamic_index_in_dim(chunks, me, 0, keepdims=False).astype(jnp.float32)
    for shift in range(1, count):
        pairs = [(i, (i + shift) % count) for i in range(count)]
        piece = lax.dynamic_index_in_dim(chunks, (me + shift) % count, 0, keepdims=False)
        total = total + lax.ppermute(piece, TP, pairs).astype(jnp.float32)
    reduced = total.astype(jnp.bfloat16)
    gathered = jnp.zeros(low_part.shape, jnp.bfloat16)
    gathered = lax.dynamic_update_slice_in_dim(gathered, reduced, me * rows, 0)
    for shift in range(1, count):
        pairs = [(i, (i + shift) % count) for i in range(count)]
        got = lax.ppermute(reduced, TP, pairs)
        gathered = lax.dynamic_update_slice_in_dim(
            gathered, got, ((me + count - shift) % count) * rows, 0
        )
    return gathered


def exchange_scatter(blocks, axis, count):
    me = lax.axis_index(axis)
    total = lax.dynamic_index_in_dim(blocks, me, 0, keepdims=False)
    for shift in range(1, count):
        pairs = [(i, (i + shift) % count) for i in range(count)]
        piece = lax.dynamic_index_in_dim(blocks, (me + shift) % count, 0, keepdims=False)
        total = total + lax.ppermute(piece, axis, pairs)
    return total


def scatter_low(grad, dim):
    summed = lax.psum_scatter(
        grad.astype(jnp.bfloat16), (SHARD, CTX), scatter_dimension=dim, tiled=True
    )
    return summed.astype(jnp.float32)


def matmul_low(left, right):
    return jnp.dot(left, right, preferred_element_type=jnp.float32)


MID_SPLIT = (3, 5)


def middle_rows(attn_rows, tokens_rows, grad_final, output_full, gate_full, up_full, down_full, tp_count, before):
    bf_type = jnp.bfloat16
    resid = tokens_rows + tp_psum(matmul_low(attn_rows, output_full), tp_count).astype(jnp.float32)
    normed_two, scale_two = normalize(resid)
    input_two = normed_two.astype(bf_type)
    gate_proj = matmul_low(input_two, gate_full)
    up_proj = matmul_low(input_two, up_full)
    gate_sigmoid = jax.nn.sigmoid(gate_proj)
    hidden = (gate_proj * gate_sigmoid * up_proj).astype(bf_type)
    grad_branch = grad_final.astype(bf_type)
    grad_hidden = jnp.einsum(
        "rd,fd->rf", grad_branch, down_full, preferred_element_type=jnp.float32
    )
    grad_gate_act = (
        grad_hidden * up_proj * gate_sigmoid * (1.0 + gate_proj * (1.0 - gate_sigmoid))
    ).astype(bf_type)
    grad_up_act = (grad_hidden * gate_proj * gate_sigmoid).astype(bf_type)
    grad_input_two = jnp.einsum(
        "rf,df->rd", grad_gate_act, gate_full, preferred_element_type=jnp.float32
    ) + jnp.einsum("rf,df->rd", grad_up_act, up_full, preferred_element_type=jnp.float32)
    branch_two = matmul_low(hidden, down_full)
    grad_down = jnp.einsum("rd,rf->df", grad_branch, hidden, preferred_element_type=jnp.float32)
    grad_gate = jnp.einsum(
        "rd,rf->df", input_two, grad_gate_act, preferred_element_type=jnp.float32
    )
    grad_up = jnp.einsum("rd,rf->df", input_two, grad_up_act, preferred_element_type=jnp.float32)
    if before is not None:
        grad_input_two, _ = lax.optimization_barrier((grad_input_two, before))
    grad_input_two = lax.psum(grad_input_two.astype(bf_type), TP)
    return [
        resid, branch_two, normed_two, scale_two, grad_final, grad_input_two,
        grad_gate, grad_up, grad_down,
    ]


def body(tp_count, ctx_count, *args):
    return block(tp_count, ctx_count, *args)


def block(tp_count, ctx_count, tokens, lengths, cotangent, w_query, w_key, w_value, w_output, w_gate, w_up, w_down):
    seq_count, half_len, model_width = tokens.shape
    head_cols = w_query.shape[1]
    head_count = head_cols // HEAD_DIM
    row_total = seq_count * half_len
    offset = lax.axis_index(CTX) * half_len
    positions = offset + jnp.arange(half_len)
    valid_mask = (positions[None, :] < lengths[:, None]).astype(jnp.float32)
    bf_type = jnp.bfloat16
    attn_low = (
        w_query.astype(bf_type),
        w_key.astype(bf_type),
        w_value.astype(bf_type),
        w_output.astype(bf_type),
    )
    mlp_low = (w_gate.astype(bf_type), w_up.astype(bf_type), w_down.astype(bf_type))
    key_value = lax.all_gather(
        jnp.concatenate([attn_low[1], attn_low[2]], axis=1), (SHARD, CTX), axis=0, tiled=True
    )
    query_output = lax.all_gather(
        jnp.concatenate([attn_low[0], attn_low[3].T], axis=1), (SHARD, CTX), axis=0, tiled=True
    )
    key_full, value_full = jnp.split(key_value, 2, axis=1)
    query_full, output_t = jnp.split(query_output, 2, axis=1)
    output_full = output_t.T
    gate_full, up_full, down_full = (
        lax.all_gather(mlp_low[0], (SHARD, CTX), axis=0, tiled=True),
        lax.all_gather(mlp_low[1], (SHARD, CTX), axis=0, tiled=True),
        lax.all_gather(mlp_low[2], (SHARD, CTX), axis=1, tiled=True),
    )
    tokens_wide = tokens.astype(jnp.float32).reshape(row_total, model_width)
    normed_one, scale_one = normalize(tokens_wide)
    input_one = normed_one.astype(bf_type)
    split_heads = (seq_count, half_len, head_count, HEAD_DIM)
    query_pre = matmul_low(input_one, query_full).reshape(split_heads)
    key_pre = matmul_low(input_one, key_full).reshape(split_heads)
    value_pre = matmul_low(input_one, value_full).reshape(split_heads)
    cosine, sine_table = rope_tables(half_len, HEAD_DIM, offset)
    queries = rotate(query_pre, cosine, sine_table).astype(bf_type)
    keys_rot = rotate(key_pre, cosine, sine_table).astype(bf_type)
    values_low = value_pre.astype(bf_type)
    keys_all, values_all = (
        lax.all_gather(keys_rot, CTX, axis=1, tiled=True),
        lax.all_gather(values_low, CTX, axis=1, tiled=True),
    )
    seq_index = 0
    attended, log_totals = attend_forward(
        queries[seq_index], keys_all[seq_index], values_all[seq_index], lengths[seq_index], offset
    )
    attended_list = [attended]
    log_list = [log_totals]
    attn_out = jnp.stack(attended_list).reshape(row_total, head_cols)
    grad_final = cotangent.astype(jnp.float32).reshape(row_total, model_width) * valid_mask.reshape(
        row_total, 1
    )
    unit = row_total // sum(MID_SPLIT)
    bounds = [0]
    for share in MID_SPLIT:
        bounds.append(bounds[-1] + share * unit)
    pieces = []
    for index in range(len(MID_SPLIT)):
        rows = slice(bounds[index], bounds[index + 1])
        pieces.append(
            middle_rows(
                attn_out[rows], tokens_wide[rows], grad_final[rows],
                output_full, gate_full, up_full, down_full, tp_count,
                pieces[-1][5] if pieces else None,
            )
        )
    grad_gate = sum(piece[6] for piece in pieces)
    grad_up = sum(piece[7] for piece in pieces)
    grad_down = sum(piece[8] for piece in pieces)
    last_sum = pieces[-1][5]
    (grad_gate, grad_up, grad_down), last_sum = lax.optimization_barrier(
        ((grad_gate, grad_up, grad_down), last_sum)
    )
    pieces[-1][5] = last_sum
    resid = jnp.concatenate([piece[0] for piece in pieces], axis=0)
    branch_two_part = jnp.concatenate([piece[1] for piece in pieces], axis=0)
    grad_resid_parts, grad_attn_parts, grad_wout = [], [], 0.0
    for index, piece in enumerate(pieces):
        grad_resid_part = piece[4] + norm_back(piece[2], piece[3], piece[5].astype(jnp.float32))
        resid_low = grad_resid_part.astype(bf_type)
        grad_wout = grad_wout + jnp.einsum(
            "rd,rc->dc", resid_low, attn_out[bounds[index]:bounds[index + 1]],
            preferred_element_type=jnp.float32,
        )
        grad_attn_parts.append(
            jnp.einsum("rd,cd->rc", resid_low, output_full, preferred_element_type=jnp.float32)
        )
        grad_resid_parts.append(grad_resid_part)
    grad_resid = jnp.concatenate(grad_resid_parts, axis=0)
    gate_cols = grad_gate.shape[1]
    front = scatter_low(jnp.concatenate([grad_gate, grad_up, grad_wout], axis=1), 0)
    mlp_grads = (front[:, :gate_cols], front[:, gate_cols:2 * gate_cols])
    wout_grad = front[:, 2 * gate_cols:].T
    grad_attn = jnp.concatenate(grad_attn_parts, axis=0).astype(bf_type).reshape(split_heads)
    branch_two_part, grad_attn = lax.optimization_barrier((branch_two_part, grad_attn))
    final_sum = resid + lax.psum(branch_two_part.astype(bf_type), TP).astype(jnp.float32)
    seq_index = 0
    grad_queries, grad_keys_seq, grad_values_seq = attend_backward(
        queries[seq_index],
        keys_all[seq_index],
        values_all[seq_index],
        lengths[seq_index],
        offset,
        log_list[seq_index],
        grad_attn[seq_index],
    )
    query_grads = [grad_queries]
    key_grads = [grad_keys_seq]
    value_grads = [grad_values_seq]
    grad_keys, grad_values = (
        exchange_scatter(
            jnp.stack(key_grads).reshape((ctx_count, half_len, head_count, HEAD_DIM)), CTX, ctx_count
        ).reshape(split_heads),
        exchange_scatter(
            jnp.stack(value_grads).reshape((ctx_count, half_len, head_count, HEAD_DIM)), CTX, ctx_count
        ).reshape(split_heads),
    )
    query_grad = jnp.stack(query_grads)
    q_parts, k_parts, v_parts, token_parts = [], [], [], []
    for index in range(len(MID_SPLIT)):
        low_row, high_row = bounds[index], bounds[index + 1]
        count = high_row - low_row
        cos_part, sin_part = cosine[low_row:high_row], sine_table[low_row:high_row]
        q_part = rotate_back(query_grad[:, low_row:high_row], cos_part, sin_part)
        q_part = q_part.astype(bf_type).reshape(count, head_cols)
        k_part = rotate_back(grad_keys[:, low_row:high_row], cos_part, sin_part)
        k_part = k_part.astype(bf_type).reshape(count, head_cols)
        v_part = grad_values[:, low_row:high_row].astype(bf_type).reshape(count, head_cols)
        input_part = (
            jnp.einsum("rc,dc->rd", q_part, query_full, preferred_element_type=jnp.float32)
            + jnp.einsum("rc,dc->rd", k_part, key_full, preferred_element_type=jnp.float32)
            + jnp.einsum("rc,dc->rd", v_part, value_full, preferred_element_type=jnp.float32)
        )
        input_part = tp_psum(input_part, tp_count).astype(jnp.float32)
        token_parts.append(
            grad_resid[low_row:high_row]
            + norm_back(normed_one[low_row:high_row], scale_one[low_row:high_row], input_part)
        )
        q_parts.append(q_part)
        k_parts.append(k_part)
        v_parts.append(v_part)
    grad_q_pre = jnp.concatenate(q_parts, axis=0)
    grad_k_pre = jnp.concatenate(k_parts, axis=0)
    grad_v_pre = jnp.concatenate(v_parts, axis=0)
    grad_wq = jnp.einsum("rd,rc->dc", input_one, grad_q_pre, preferred_element_type=jnp.float32)
    grad_wk = jnp.einsum("rd,rc->dc", input_one, grad_k_pre, preferred_element_type=jnp.float32)
    grad_wv = jnp.einsum("rd,rc->dc", input_one, grad_v_pre, preferred_element_type=jnp.float32)
    down_cols = grad_down.shape[1]
    joined = scatter_low(jnp.concatenate([grad_down, grad_wq, grad_wk, grad_wv], axis=1), 0)
    mlp_grads = mlp_grads + (joined[:, :down_cols].T,)
    qkv_grads = jnp.split(joined[:, down_cols:], 3, axis=1)
    attn_grads = (qkv_grads[0], qkv_grads[1], qkv_grads[2], wout_grad)
    grad_tokens = jnp.concatenate(token_parts, axis=0)
    output = final_sum.astype(bf_type).reshape(seq_count, half_len, model_width)
    grad_tokens = grad_tokens.reshape(seq_count, half_len, model_width)
    return (
        output,
        grad_tokens,
        attn_grads[0],
        attn_grads[1],
        attn_grads[2],
        attn_grads[3],
        mlp_grads[0],
        mlp_grads[1],
        mlp_grads[2],
    )


def solution(mesh):
    return jax.shard_map(
        functools.partial(body, mesh.shape[TP], mesh.shape[CTX]),
        mesh=mesh,
        in_specs=(
            P(SHARD, CTX, None),
            P(SHARD),
            P(SHARD, CTX, None),
            P((SHARD, CTX), TP),
            P((SHARD, CTX), TP),
            P((SHARD, CTX), TP),
            P(TP, (SHARD, CTX)),
            P((SHARD, CTX), TP),
            P((SHARD, CTX), TP),
            P(TP, (SHARD, CTX)),
        ),
        out_specs=(
            P(SHARD, CTX, None),
            P(SHARD, CTX, None),
            P((SHARD, CTX), TP),
            P((SHARD, CTX), TP),
            P((SHARD, CTX), TP),
            P(TP, (SHARD, CTX)),
            P((SHARD, CTX), TP),
            P((SHARD, CTX), TP),
            P(TP, (SHARD, CTX)),
        ),
        check_vma=False,
    )
```
